32 devices in a mesh: fsdp: 8 (over z, y), seq: 4 (over x, core).
Axes of the slice: x: 2, y: 2, z: 4, core: 2. Of those that a mesh axis runs over, the one named last changes fastest.
Arguments:
- tokens: bfloat16 [8, 512, 4096], P('fsdp'), may hold values from -7 to 7
- norm_gain: float32 [4096], replicated, may hold values from 0.1 to 1.9
- curvature: bfloat16 [8, 512, 4096], P('fsdp'), may hold values from 0.19921875 to 2
- weight_slots: bfloat16 [4, 400, 128, 128], P('seq', 'fsdp'), may hold values from -1 to 1
- probe_slots: bfloat16 [4, 400, 128, 128], P('seq', 'fsdp'), may hold values from -0.09375 to 0.09375
- block_counts: int32 [4, 8], P('seq'), may hold values from 1 to 50, 320 in all within a row
Outputs:
- hvp_slots: float32 [4, 400, 128, 128], P('seq', 'fsdp')
The draws below stay inside these ranges and needn't reach their ends.
Inputs may be any that keep to these rules, and one draw needn't show every extreme that they name: `block_counts`: in each row, device d along fsdp owns the n_d blocks that follow the earlier devices' blocks, in its first n_d slots; a row sums to 320, and 50 is reached in every row.
All inputs are finite; a program needn't handle non-finite values.
Results may differ from the reference program's by a relative error of at most 0.018.
Values may be sent and summed in bfloat16 or wider, within the bound.
A program may use at most 128 MiB of HBM per device.

```python
import math
import jax
import jax.numpy as jnp
import numpy as np
from jax import lax

D = 4096
HQ = 16
HK = 4
HD = 128
BLK = 128
LEN = 512
NB = 320
SLOTS = 50
N_FSDP = 8
N_SEQ = 4


def draw_tokens(key, part):
    own_key = jax.random.fold_in(key, 11)
    noise = jax.random.normal(own_key, (N_FSDP, LEN, D), jnp.float32)
    result = jnp.clip(noise, -6.0, 6.0)
    return result.astype(jnp.bfloat16)


def draw_weight_slots(key, part):
    own_key = jax.random.fold_in(key, 12)
    result = jnp.clip(jax.random.normal(own_key, (N_SEQ, N_FSDP * SLOTS, BLK, BLK), jnp.float32), -6.0, 6.0) * D ** (-0.5)
    return result.astype(jnp.bfloat16)


def block_scale(key, extent, shards, least, largest):
    def one(axis_at, blocks):
        heights = jax.random.uniform(jax.random.fold_in(jax.random.fold_in(key, 6), axis_at), (blocks,), jnp.float32, least / len(shards), largest / len(shards))
        return jnp.repeat(jnp.exp(heights), extent[axis_at] // blocks).reshape((-1,) + (1,) * (len(extent) - axis_at - 1))

    gain = one(*shards[0])
    for cut in shards[1:]:
        gain = gain * one(*cut)
    return gain


def length_profile(number_of, total, reach, skew):
    weights = [(1 << 20) // math.isqrt(grade ** skew) + 1 for grade in range(2, number_of + 1)]
    surplus, holding = total - reach - (number_of - 1), [1] * (number_of - 1)
    while surplus > 0:
        candidates = [i for i in range(number_of - 1) if holding[i] < reach]
        whole, left = sum([weights[i] for i in candidates]), surplus
        for i in candidates:
            more = min(reach - holding[i], max(1, left * weights[i] // whole), surplus)
            holding[i] = holding[i] + more
            surplus = surplus - more
    return np.array([reach] + holding)


def ragged_sizes(key, count, total, bound, slope):
    if count == 2:
        one = jax.random.randint(key, (), max(1, total - bound), min(bound, total - 1) + 1)
        return jnp.stack([one, total - one])
    lengths = jnp.asarray(length_profile(count, total, bound, slope), jnp.int32)
    couples = (count - 1) // 2
    giver, receiver = lengths[1:1 + 2 * couples:2], lengths[2:2 + 2 * couples:2]
    margin = jnp.minimum(giver - 1, bound - receiver)
    moved = jax.random.randint(jax.random.fold_in(key, 1), (couples,), 0, 1 << 20) % (margin + 1)
    lengths = lengths.at[1:1 + 2 * couples:2].set(giver - moved).at[2:2 + 2 * couples:2].set(receiver + moved)
    return lengths[jax.random.permutation(jax.random.fold_in(key, 2), count)]


def centred(rng, dims, deviation, bound, cuts=(), kind=jnp.bfloat16):
    loudness = block_scale(rng, dims, cuts, -0.22, 0.18) if cuts else 1.0
    values = jax.random.normal(rng, dims, jnp.float32) * deviation * loudness
    return jnp.minimum(jnp.maximum(values, -bound), bound).astype(kind)


def setup_inputs(seed: int = 0) -> dict:
    streams_of = jax.random.split(jax.random.key(seed), 7)
    tokens = draw_tokens(jax.random.fold_in(streams_of[6], 71), 0)
    norm_gain = jnp.clip(1.0 + 0.18 * jax.random.normal(streams_of[1], (D,), jnp.float32), 0.1, 1.9)
    curvature = jnp.clip(jnp.exp(math.log(2.0) - 2.306499 * jax.random.uniform(streams_of[2], (N_FSDP, LEN, D), jnp.float32) ** block_scale(streams_of[2], (N_FSDP, LEN, D), ((0, 8),), -0.2, 0.2)), 0.19921875, 2.0).astype(jnp.bfloat16)
    weight_slots = draw_weight_slots(jax.random.fold_in(streams_of[6], 71), 0)
    probe_slots = centred(streams_of[4], (N_SEQ, N_FSDP * SLOTS, BLK, BLK), D ** -0.5, 0.09375, ((0, 4), (1, 8)))
    block_counts = jax.vmap(lambda own: ragged_sizes(own, N_FSDP, NB, SLOTS, 2))(jax.random.split(streams_of[5], N_SEQ)).reshape((N_SEQ, N_FSDP)).astype(jnp.int32)
    return dict(tokens=tokens, norm_gain=norm_gain, curvature=curvature, weight_slots=weight_slots, probe_slots=probe_slots, block_counts=block_counts)


THETA = 500000.0
EPS = 1e-05
NEGATIVE = -1e+30

def rotary(length, head_dim):
    half_dim = head_dim // 2
    frequency = jnp.exp(-jnp.log(THETA) * 2.0 * jnp.arange(half_dim, dtype=jnp.float32) / head_dim)
    angles = jnp.arange(length, dtype=jnp.float32)[:, None] * frequency[None, :]
    return (jnp.cos(angles)[:, None, :], jnp.sin(angles)[:, None, :])

def rotate(field_in, cosine, sine):
    half_dim = field_in.shape[-1] // 2
    first_half = field_in[..., :half_dim]
    second = field_in[..., half_dim:]
    return jnp.concatenate([first_half * cosine - second * sine, second * cosine + first_half * sine], axis=-1)

def normalize(tokens, norm_gain):
    values = tokens.astype(jnp.float32)
    factor = lax.rsqrt(lax.optimization_barrier(jnp.mean(values * values, axis=-1, keepdims=True)) + EPS)
    return (values * factor * norm_gain).astype(jnp.bfloat16)

def attention_branch(w_qkv, w_out, normed, cosine, sine, q_heads, kv_heads):
    length = normed.shape[0]
    head_dim = w_out.shape[0] // q_heads
    projected = jnp.dot(normed, w_qkv, preferred_element_type=jnp.float32)
    q_end = q_heads * head_dim
    k_end = q_end + kv_heads * head_dim
    queries = rotate(projected[:, :q_end].reshape(length, q_heads, head_dim), cosine, sine).astype(jnp.bfloat16)
    key_rows = rotate(projected[:, q_end:k_end].reshape(length, kv_heads, head_dim), cosine, sine).astype(jnp.bfloat16)
    values = projected[:, k_end:].reshape(length, kv_heads, head_dim).astype(jnp.bfloat16)
    queries, key_rows, values = lax.optimization_barrier((queries, key_rows, values))
    queries = queries.reshape(length, kv_heads, q_heads // kv_heads, head_dim)
    scores = jnp.einsum('qkgd,skd->kgqs', queries.astype(jnp.float32), key_rows.astype(jnp.float32)) * head_dim ** (-0.5)
    causal = jnp.arange(length)[:, None] >= jnp.arange(length)[None, :]
    scores = jnp.where(causal, scores, NEGATIVE)
    attn_probs = jax.nn.softmax(scores, axis=-1).astype(jnp.bfloat16)
    attn_probs = lax.optimization_barrier(attn_probs)
    mixed_heads = jnp.einsum('kgqs,skd->qkgd', attn_probs.astype(jnp.float32), values.astype(jnp.float32))
    mixed_heads = mixed_heads.reshape(length, q_heads * head_dim).astype(jnp.bfloat16)
    return jnp.dot(mixed_heads, w_out, preferred_element_type=jnp.float32)

def owner_slots(counts, blocks, slots):
    range_ends = jnp.cumsum(counts).astype(jnp.int32)
    starts = (range_ends - counts).astype(jnp.int32)
    block_ids = jnp.arange(blocks, dtype=jnp.int32)
    owners = lax.optimization_barrier(jnp.sum((range_ends[None, :] <= block_ids[:, None]).astype(jnp.int32), axis=1)).astype(jnp.int32)
    owner_hot = owners[:, None] == jnp.arange(counts.shape[0], dtype=jnp.int32)[None, :]
    first_block = lax.optimization_barrier(jnp.sum(jnp.where(owner_hot, starts[None, :], 0), axis=1)).astype(jnp.int32)
    return (owners * slots + block_ids - first_block).astype(jnp.int32)

def to_matrix(blocks, row_blocks, col_blocks):
    blk_edge = blocks.shape[-1]
    return blocks.reshape(row_blocks, col_blocks, blk_edge, blk_edge).transpose(0, 2, 1, 3).reshape(row_blocks * blk_edge, col_blocks * blk_edge)

def to_blocks(matrix, blk_edge):
    row_blocks = matrix.shape[0] // blk_edge
    col_blocks = matrix.shape[1] // blk_edge
    return matrix.reshape(row_blocks, blk_edge, col_blocks, blk_edge).transpose(0, 2, 1, 3).reshape(row_blocks * col_blocks, blk_edge, blk_edge)

def reference(tokens, norm_gain, curvature, weight_slots, probe_slots, block_counts):
    n_columns = weight_slots.shape[0]
    q_heads = HQ // n_columns
    kv_heads = HK // n_columns
    row_blocks = D // BLK
    qkv_cols = (q_heads + 2 * kv_heads) * HD // BLK
    out_rows = q_heads * HD // BLK
    qkv_split = row_blocks * qkv_cols
    cosine, sine = rotary(LEN, HD)
    normed = jax.vmap(normalize, in_axes=(0, None))(tokens, norm_gain)
    tangent_sum = jnp.zeros((N_FSDP, LEN, D), jnp.float32)
    unpacked = []
    for column in range(n_columns):
        slot_of = owner_slots(block_counts[column], NB, SLOTS)
        w_blocks = weight_slots[column][slot_of]
        p_blocks = probe_slots[column][slot_of]
        w_qkv = to_matrix(w_blocks[:qkv_split], row_blocks, qkv_cols)
        w_out = to_matrix(w_blocks[qkv_split:], out_rows, row_blocks)
        p_qkv = to_matrix(p_blocks[:qkv_split], row_blocks, qkv_cols)
        p_out = to_matrix(p_blocks[qkv_split:], out_rows, row_blocks)

        def tangent_one(seq_normed, w_qkv=w_qkv, w_out=w_out, p_qkv=p_qkv, p_out=p_out):

            def inner(first_w, second_w):
                return attention_branch(first_w, second_w, seq_normed, cosine, sine, q_heads, kv_heads)
            return jax.jvp(inner, (w_qkv, w_out), (p_qkv, p_out))[1]
        tangent_sum = tangent_sum + lax.map(tangent_one, normed)
        unpacked.append((slot_of, w_qkv, w_out))
    weighted = (curvature.astype(jnp.float32) * tangent_sum).astype(jnp.bfloat16)
    factor = 1.0 / jnp.sqrt(jnp.float32(LEN * N_FSDP))
    results = []
    for column in range(n_columns):
        slot_of, w_qkv, w_out = unpacked[column]

        def accumulate(grad_total, seq_pair, w_qkv=w_qkv, w_out=w_out):
            seq_normed, seq_weighted = seq_pair

            def inner(first_w, second_w):
                return attention_branch(first_w, second_w, seq_normed, cosine, sine, q_heads, kv_heads)
            _, pullback = jax.vjp(inner, w_qkv, w_out)
            g_qkv, g_out = pullback(seq_weighted.astype(jnp.float32))
            grad_blocks = jnp.concatenate([to_blocks(g_qkv, BLK), to_blocks(g_out, BLK)], axis=0)
            return (grad_total + grad_blocks.astype(jnp.float32), None)
        grad_total, _ = lax.scan(accumulate, jnp.zeros((NB, BLK, BLK), jnp.float32), (normed, weighted))
        packed = jnp.zeros((N_FSDP * SLOTS, BLK, BLK), jnp.float32).at[slot_of].set(grad_total * factor)
        results.append(packed)
    return jnp.stack(results)
```

```python
import functools

import jax
import jax.numpy as jnp
from jax import lax
from jax.experimental import pallas as pl
from jax.experimental.pallas import tpu as pltpu
from jax.sharding import PartitionSpec as P

D = 4096
HQ = 16
HK = 4
HD = 128
BLK = 128


THETA = 500000.0
EPS = 1e-05
NEGATIVE = -1e30


def rotary(length, head_dim):
    half_dim = head_dim // 2
    frequency = jnp.exp(-jnp.log(THETA) * 2.0 * jnp.arange(half_dim, dtype=jnp.float32) / head_dim)
    angles = jnp.arange(length, dtype=jnp.float32)[:, None] * frequency[None, :]
    return (jnp.cos(angles)[:, None, :], jnp.sin(angles)[:, None, :])


def rotate(field_in, cosine, sine):
    half_dim = field_in.shape[-1] // 2
    first_half = field_in[..., :half_dim]
    second = field_in[..., half_dim:]
    return jnp.concatenate(
        [first_half * cosine - second * sine, second * cosine + first_half * sine], axis=-1
    )


VMEM_BYTES = 62 * 1024 * 1024
GRID_VMEM_BYTES = 67043328


def attention(projected, cosine, sine, q_heads, kv_heads):
    length = projected.shape[0]
    head_dim = projected.shape[1] // (q_heads + 2 * kv_heads)
    q_end = q_heads * head_dim
    k_end = q_end + kv_heads * head_dim
    queries = rotate(projected[:, :q_end].reshape(length, q_heads, head_dim), cosine, sine).astype(
        jnp.bfloat16
    )
    key_rows = rotate(
        projected[:, q_end:k_end].reshape(length, kv_heads, head_dim), cosine, sine
    ).astype(jnp.bfloat16)
    values = projected[:, k_end:].reshape(length, kv_heads, head_dim).astype(jnp.bfloat16)
    queries = queries.reshape(length, kv_heads, q_heads // kv_heads, head_dim)
    scores = jnp.einsum(
        "qkgd,skd->kgqs", queries, key_rows, preferred_element_type=jnp.float32
    ) * head_dim ** (-0.5)
    causal = jnp.arange(length)[:, None] >= jnp.arange(length)[None, :]
    scores = jnp.where(causal, scores, NEGATIVE)
    attn_probs = jax.nn.softmax(scores, axis=-1).astype(jnp.bfloat16)
    mixed_heads = jnp.einsum(
        "kgqs,skd->qkgd", attn_probs, values, preferred_element_type=jnp.float32
    )
    return mixed_heads.reshape(length, q_heads * head_dim).astype(jnp.bfloat16)


def ring_position(index, n):
    odd = lax.rem(index, 2)
    half = lax.div(index, 2)
    return (1 - odd) * half + odd * (n - 1 - half)


def ring_index(position, n):
    back = lax.div(position, n // 2)
    return (1 - back) * 2 * position + back * (2 * (n - 1 - position) + 1)


def pieces(slots):
    half = slots // 2
    out = []
    for direction, first, count in ((0, 0, half), (1, half, slots - half)):
        cuts = 5 if count % 5 == 0 else 1
        size = count // cuts
        out.append([(first + i * size, size) for i in range(cuts)])
    return out


def enter(neighbours, axis="fsdp"):
    barrier = pltpu.get_barrier_semaphore()
    for neighbour in neighbours:
        pl.semaphore_signal(
            barrier, inc=1, device_id={axis: neighbour}, device_id_type=pl.DeviceIdType.MESH
        )
    pl.semaphore_wait(barrier, len(neighbours))


def gather_kernel(n, slots, grid_qkv, grid_out, slot_ref, w_ref, p_ref, tokens_ref, gain_ref,
                  proj_ref, d_proj_ref, wo_ref, po_ref, normed_t_ref, held_w, held_p, matrix,
                  normed, send_sem, recv_sem):
    me = lax.axis_index("fsdp")
    pos = ring_position(me, n)
    right = ring_index(lax.rem(pos + 1, n), n)
    left = ring_index(lax.rem(pos + n - 1, n), n)
    towards = (right, left)
    enter((left, right))
    parts = pieces(slots)
    arrays = ((w_ref, held_w), (p_ref, held_p))

    def copy(which, step, direction, j):
        own, held = arrays[which]
        first, size = parts[direction][j]
        shift = n - step if direction == 0 else step
        origin = ring_index(lax.rem(pos + shift, n), n)
        there = held.at[pl.ds(origin * slots + first, size)]
        here = own.at[pl.ds(first, size)] if step == 0 else there
        return pltpu.make_async_remote_copy(
            src_ref=here,
            dst_ref=there,
            send_sem=send_sem.at[which, step, direction, j],
            recv_sem=recv_sem.at[which, step, direction, j],
            device_id={"fsdp": towards[direction]},
            device_id_type=pl.DeviceIdType.MESH,
        )

    def arrival(which, step, direction, j):
        first, size = parts[direction][j]
        own, held = arrays[which]
        shift = n - step - 1 if direction == 0 else step + 1
        origin = ring_index(lax.rem(pos + shift, n), n)
        there = held.at[pl.ds(origin * slots + first, size)]
        pltpu.make_async_remote_copy(
            src_ref=there,
            dst_ref=there,
            send_sem=send_sem.at[which, step, direction, j],
            recv_sem=recv_sem.at[which, step, direction, j],
            device_id={"fsdp": towards[direction]},
            device_id_type=pl.DeviceIdType.MESH,
        ).wait_recv()

    def each():
        for j in range(max(len(parts[0]), len(parts[1]))):
            for direction in range(2):
                if j < len(parts[direction]):
                    yield direction, j

    def normalize():
        rows = 32

        def some(i, carry):
            here = pl.ds(pl.multiple_of(i * rows, rows), rows)
            values = tokens_ref[here, :].astype(jnp.float32)
            factor = lax.rsqrt(jnp.mean(values * values, axis=-1, keepdims=True) + EPS)
            normed[here, :] = (values * factor * gain_ref[...]).astype(jnp.bfloat16)
            return carry

        lax.fori_loop(0, normed.shape[0] // rows, some, 0)

    def transpose():
        edge = held_w.shape[-1]

        def some(i, carry):
            here = pl.ds(pl.multiple_of(i * edge, edge), edge)
            normed_t_ref[here, :] = normed[:, here].T
            return carry

        lax.fori_loop(0, normed.shape[1] // edge, some, 0)

    def project(result_ref):
        rows = 256

        def some(i, carry):
            here = pl.ds(pl.multiple_of(i * rows, rows), rows)
            result_ref[here, :] = jnp.dot(
                normed[here, :], matrix[...], preferred_element_type=jnp.float32
            )
            return carry

        lax.fori_loop(0, normed.shape[0] // rows, some, 0)

    def unpack(which, qkv_ref, out_ref):
        own, held = arrays[which]
        rows, cols = grid_qkv
        edge = held.shape[-1]

        def qkv_row(i, carry):
            for c in range(cols):
                qkv_ref[pl.ds(pl.multiple_of(i * edge, edge), edge), c * edge:(c + 1) * edge] = (
                    held[slot_ref[i * cols + c]]
                )
            return carry

        lax.fori_loop(0, rows, qkv_row, 0)
        out_rows, out_cols = grid_out

        def out_col(i, carry):
            for r in range(out_rows):
                out_ref[r * edge:(r + 1) * edge, pl.ds(pl.multiple_of(i * edge, edge), edge)] = (
                    held[slot_ref[rows * cols + r * out_cols + i]]
                )
            return carry

        lax.fori_loop(0, out_cols, out_col, 0)

    def finish(which, qkv_ref, out_ref):
        own, held = arrays[which]
        for direction, j in each():
            arrival(which, n - 2, direction, j)
        held[pl.ds(me * slots, slots)] = own[...]
        unpack(which, qkv_ref, out_ref)

    sent = []
    for which in range(2):
        for step in range(n - 1):
            for direction, j in each():
                if step > 0:
                    arrival(which, step - 1, direction, j)
                one = copy(which, step, direction, j)
                one.start()
                sent.append(one)
            if which == 0 and step == 0:
                normalize()
            if which == 0 and step == 1:
                transpose()
            if which == 1 and step == 0:
                finish(0, matrix, wo_ref)
            if which == 1 and step == 1:
                project(proj_ref)
    finish(1, matrix, po_ref)
    project(d_proj_ref)
    for one in sent:
        one.wait_send()


def gather_weights(slot_of, weights, probes, tokens, gain, n, grid_qkv, grid_out):
    slots, edge, _ = weights.shape
    cuts = max(len(part) for part in pieces(slots))
    length, width = tokens.shape
    proj = jax.ShapeDtypeStruct((length, grid_qkv[1] * edge), jnp.float32)
    turned = jax.ShapeDtypeStruct((width, length), jnp.bfloat16)
    out = jax.ShapeDtypeStruct((grid_out[0] * edge, grid_out[1] * edge), jnp.bfloat16)
    vmem = pl.BlockSpec(memory_space=pltpu.VMEM)
    return pl.pallas_call(
        functools.partial(gather_kernel, n, slots, grid_qkv, grid_out),
        out_shape=(proj, proj, out, out, turned),
        in_specs=[pl.BlockSpec(memory_space=pltpu.SMEM)] + [vmem] * 4,
        out_specs=(vmem,) * 5,
        scratch_shapes=[
            pltpu.VMEM((n * slots, edge, edge), jnp.bfloat16),
            pltpu.VMEM((n * slots, edge, edge), jnp.bfloat16),
            pltpu.VMEM((grid_qkv[0] * edge, grid_qkv[1] * edge), jnp.bfloat16),
            pltpu.VMEM((length, width), jnp.bfloat16),
            pltpu.SemaphoreType.DMA((2, n - 1, 2, cuts)),
            pltpu.SemaphoreType.DMA((2, n - 1, 2, cuts)),
        ],
        compiler_params=pltpu.CompilerParams(
            collective_id=0, has_side_effects=True, vmem_limit_bytes=VMEM_BYTES
        ),
    )(slot_of, weights, probes, tokens, gain)


def gradient_blocks(grid_qkv, grid_out, normed_t_ref, d_proj_ref, mixed_t_ref, weighted_ref,
                    out_ref):
    edge = out_ref.shape[-1]
    rows, cols = grid_qkv
    out_rows, out_cols = grid_out
    group = 2

    out_ref[rows * cols + out_rows * out_cols] = jnp.zeros((edge, edge), out_ref.dtype)

    def qkv_rows(i, carry):
        width = group * edge
        left = normed_t_ref[pl.ds(pl.multiple_of(i * width, width), width), :]
        block = jnp.dot(
            left, d_proj_ref[...], preferred_element_type=jnp.float32
        ).astype(jnp.bfloat16)
        for r in range(group):
            for c in range(cols):
                out_ref[(i * group + r) * cols + c] = block[
                    r * edge:(r + 1) * edge, c * edge:(c + 1) * edge
                ]
        return carry

    lax.fori_loop(0, rows // group, qkv_rows, 0)

    def out_columns(i, carry):
        width = group * edge
        right = weighted_ref[:, pl.ds(pl.multiple_of(i * width, width), width)]
        block = jnp.dot(
            mixed_t_ref[...], right, preferred_element_type=jnp.float32
        ).astype(jnp.bfloat16)
        for r in range(out_rows):
            for c in range(group):
                out_ref[rows * cols + r * out_cols + i * group + c] = block[
                    r * edge:(r + 1) * edge, c * edge:(c + 1) * edge
                ]
        return carry

    lax.fori_loop(0, out_cols // group, out_columns, 0)


def reduce_kernel(n, slots, scale, grid_qkv, grid_out, pick_ref, normed_t_ref, d_proj_ref,
                  mixed_t_ref, weighted_ref, out_ref, grads, begin, held, send_sem, recv_sem):
    me = lax.axis_index("fsdp")
    pos = ring_position(me, n)
    right = ring_index(lax.rem(pos + 1, n), n)
    left = ring_index(lax.rem(pos + n - 1, n), n)
    towards = (right, left)
    enter((left, right))
    parts = pieces(slots)
    gradient_blocks(
        grid_qkv, grid_out, normed_t_ref, d_proj_ref, mixed_t_ref, weighted_ref, grads
    )

    def own(step, direction, j):
        shift = n - 1 - step if direction == 0 else 1 + step
        target = ring_index(lax.rem(pos + shift, n), n)
        return target * slots

    def each_block(direction, j, body):
        first, size = parts[direction][j]

        def some(i, carry):
            body(first + i)
            return carry

        lax.fori_loop(0, size, some, 0)

    def copy(step, direction, j):
        first, size = parts[direction][j]
        here = begin.at[pl.ds(first, size)] if step == 0 else held.at[step - 1, pl.ds(first, size)]
        return pltpu.make_async_remote_copy(
            src_ref=here,
            dst_ref=held.at[step, pl.ds(first, size)],
            send_sem=send_sem.at[step, direction, j],
            recv_sem=recv_sem.at[step, direction, j],
            device_id={"fsdp": towards[direction]},
            device_id_type=pl.DeviceIdType.MESH,
        )

    def each():
        for j in range(max(len(parts[0]), len(parts[1]))):
            for direction in range(2):
                if j < len(parts[direction]):
                    yield direction, j

    sent = {}
    for step in range(n - 1):
        for direction, j in each():
            first, size = parts[direction][j]
            base = own(step, direction, j)
            if step > 0:
                sent[step - 1, direction, j].wait_recv()

                def add(t, step=step, base=base):
                    held[step - 1, t] = (
                        held[step - 1, t].astype(jnp.float32)
                        + grads[pick_ref[base + t]].astype(jnp.float32)
                    ).astype(jnp.bfloat16)

                each_block(direction, j, add)
            else:

                def fill(t, base=base):
                    begin[t] = grads[pick_ref[base + t]]

                each_block(direction, j, fill)
            one = copy(step, direction, j)
            one.start()
            sent[step, direction, j] = one
    for direction, j in each():
        first, size = parts[direction][j]
        sent[n - 2, direction, j].wait_recv()
        base = own(n - 1, direction, j)

        def last(t, base=base):
            out_ref[t] = (
                held[n - 2, t].astype(jnp.float32) + grads[pick_ref[base + t]].astype(jnp.float32)
            ) * scale

        each_block(direction, j, last)
    for one in sent.values():
        one.wait_send()


def reduce_slots(picked, normed_t, d_proj, mixed_t, weighted, n, scale, grid_qkv, grid_out):
    slots = picked.shape[0] // n
    edge = BLK
    total_blocks = grid_qkv[0] * grid_qkv[1] + grid_out[0] * grid_out[1]
    cuts = max(len(part) for part in pieces(slots))
    vmem = pl.BlockSpec(memory_space=pltpu.VMEM)
    return pl.pallas_call(
        functools.partial(reduce_kernel, n, slots, scale, grid_qkv, grid_out),
        out_shape=jax.ShapeDtypeStruct((slots, edge, edge), jnp.float32),
        in_specs=[pl.BlockSpec(memory_space=pltpu.SMEM)] + [vmem] * 4,
        out_specs=vmem,
        scratch_shapes=[
            pltpu.VMEM((total_blocks + 1, edge, edge), jnp.bfloat16),
            pltpu.VMEM((slots, edge, edge), jnp.bfloat16),
            pltpu.VMEM((n - 1, slots, edge, edge), jnp.bfloat16),
            pltpu.SemaphoreType.DMA((n - 1, 2, cuts)),
            pltpu.SemaphoreType.DMA((n - 1, 2, cuts)),
        ],
        compiler_params=pltpu.CompilerParams(
            collective_id=1, has_side_effects=True, vmem_limit_bytes=VMEM_BYTES
        ),
    )(picked, normed_t, d_proj, mixed_t, weighted)


def exchange_kernel(mixed_ref, d_mixed_ref, w_ref, p_ref, curv_ref, weighted_ref, back_ref,
                    terms, near, pair, far, share, rest, send_sem, recv_sem):
    me = lax.axis_index("seq")
    side = lax.rem(me, 2)
    core = me + 1 - 2 * side
    across = me + 2 - 4 * lax.rem(lax.div(me, 2), 2)
    enter((core, across), "seq")
    length, width = terms.shape
    half = width // 2
    chunks = recv_sem.shape[1]
    rows = length // chunks
    mine = pl.ds(pl.multiple_of(side * half, half), half)
    other = pl.ds(pl.multiple_of((1 - side) * half, half), half)

    def block(i):
        return pl.ds(i * rows, rows)

    def copy(stage, i, here, there, target):
        return pltpu.make_async_remote_copy(
            src_ref=here,
            dst_ref=there,
            send_sem=send_sem.at[stage, i],
            recv_sem=recv_sem.at[stage, i],
            device_id={"seq": target},
            device_id_type=pl.DeviceIdType.MESH,
        )

    def terms_of(i):
        tile = width // 4

        def columns(j, carry):
            cols = pl.ds(pl.multiple_of(j * tile, tile), tile)
            terms[block(i), cols] = (
                jnp.dot(d_mixed_ref[block(i), :], w_ref[:, cols], preferred_element_type=jnp.float32)
                + jnp.dot(mixed_ref[block(i), :], p_ref[:, cols], preferred_element_type=jnp.float32)
            ).astype(jnp.bfloat16)
            return carry

        lax.fori_loop(0, 4, columns, 0)

    first = [copy(0, i, terms.at[block(i), other], near.at[block(i)], core) for i in range(chunks)]
    second = [copy(1, i, pair.at[block(i)], far.at[block(i)], across) for i in range(chunks)]
    third = [copy(2, i, share.at[block(i)], rest.at[block(i)], core) for i in range(chunks)]

    def send_pair(i):
        first[i].wait_recv()
        pair[block(i)] = (
            terms[block(i), mine].astype(jnp.float32) + near[block(i)].astype(jnp.float32)
        ).astype(jnp.bfloat16)
        second[i].start()

    def send_share(i):
        second[i].wait_recv()
        total = pair[block(i)].astype(jnp.float32) + far[block(i)].astype(jnp.float32)
        share[block(i)] = (curv_ref[block(i), mine].astype(jnp.float32) * total).astype(
            jnp.bfloat16
        )
        third[i].start()

    def finish(i):
        weighted_ref[block(i), mine] = share[block(i)]
        third[i].wait_recv()
        weighted_ref[block(i), other] = rest[block(i)]
        back_ref[block(i), :] = lax.dot_general(
            weighted_ref[block(i), :],
            w_ref[...],
            (((1,), (1,)), ((), ())),
            preferred_element_type=jnp.float32,
        ).astype(jnp.bfloat16)

    for i in range(chunks):
        terms_of(i)
        first[i].start()
        if i > 0:
            send_pair(i - 1)
    send_pair(chunks - 1)
    for i in range(chunks):
        send_share(i)
        if i > 0:
            finish(i - 1)
    finish(chunks - 1)
    for one in first + second + third:
        one.wait_send()


def exchange(mixed, d_mixed, w_out, p_out, curvature):
    length, width = curvature.shape
    chunks = 4
    vmem = pl.BlockSpec(memory_space=pltpu.VMEM)
    half = pltpu.VMEM((length, width // 2), jnp.bfloat16)
    return pl.pallas_call(
        exchange_kernel,
        out_shape=(
            jax.ShapeDtypeStruct((length, width), jnp.bfloat16),
            jax.ShapeDtypeStruct(mixed.shape, jnp.bfloat16),
        ),
        in_specs=[vmem] * 5,
        out_specs=(vmem, vmem),
        scratch_shapes=[
            pltpu.VMEM((length, width), jnp.bfloat16),
            half,
            half,
            half,
            half,
            half,
            pltpu.SemaphoreType.DMA((3, chunks)),
            pltpu.SemaphoreType.DMA((3, chunks)),
        ],
        compiler_params=pltpu.CompilerParams(
            collective_id=2, has_side_effects=True, vmem_limit_bytes=VMEM_BYTES
        ),
    )(mixed, d_mixed, w_out, p_out, curvature)


def local(tokens, norm_gain, curvature, weight_slots, probe_slots, block_counts):
    n_columns = lax.axis_size("seq")
    n_owners = lax.axis_size("fsdp")
    q_heads = HQ // n_columns
    kv_heads = HK // n_columns
    row_blocks = D // BLK
    qkv_cols = (q_heads + 2 * kv_heads) * HD // BLK
    out_rows = q_heads * HD // BLK
    grid_qkv, grid_out = (row_blocks, qkv_cols), (out_rows, row_blocks)
    total_blocks = row_blocks * qkv_cols + out_rows * row_blocks
    slots = weight_slots.shape[1]
    length = tokens.shape[1]
    counts = block_counts[0]
    range_ends = jnp.cumsum(counts)
    starts = range_ends - counts
    owner_ids = jnp.arange(n_owners, dtype=jnp.int32)
    block_ids = jnp.arange(total_blocks, dtype=jnp.int32)
    owners = jnp.sum((range_ends[None, :] <= block_ids[:, None]).astype(jnp.int32), axis=1)
    first_block = jnp.sum(
        jnp.where(owners[:, None] == owner_ids[None, :], starts[None, :], 0), axis=1
    )
    slot_of = (owners * slots + block_ids - first_block).astype(jnp.int32)
    projected, d_projected, w_out, p_out, normed_t = gather_weights(
        slot_of,
        weight_slots[0],
        probe_slots[0],
        tokens[0],
        norm_gain[None, :],
        n_owners,
        grid_qkv,
        grid_out,
    )
    cosine, sine = rotary(length, HD)

    def inner(projected):
        return attention(projected, cosine, sine, q_heads, kv_heads)

    mixed, d_mixed = jax.jvp(inner, (projected,), (d_projected,))
    weighted, back_mixed = exchange(mixed, d_mixed, w_out, p_out, curvature[0])
    mixed_again, pullback = jax.vjp(inner, projected)
    (back_projected,) = pullback(back_mixed)
    slot_index = jnp.arange(n_owners * slots, dtype=jnp.int32)
    place = slot_index % slots
    owner_hot = (slot_index // slots)[:, None] == owner_ids[None, :]
    owner_first = jnp.sum(jnp.where(owner_hot, starts[None, :], 0), axis=1)
    own_count = jnp.sum(jnp.where(owner_hot, counts[None, :], 0), axis=1)
    picked = jnp.where(place < own_count, owner_first + place, total_blocks).astype(jnp.int32)
    scaled = reduce_slots(
        picked,
        normed_t,
        back_projected.astype(jnp.bfloat16),
        mixed_again.T,
        weighted,
        n_owners,
        (length * n_owners) ** -0.5,
        grid_qkv,
        grid_out,
    )
    return scaled.reshape(1, slots, BLK, BLK)


def spot():
    f = lax.axis_index("fsdp")
    s = lax.axis_index("seq")
    return lax.div(f, 2), lax.rem(f, 2), lax.div(s, 2), lax.rem(s, 2)


def device(z, y, x, c):
    return {"fsdp": 2 * z + y, "seq": 2 * x + c}


def mirrored(z, c, planes):
    return z + c * (planes - 1 - 2 * z)


def greet(peers):
    barrier = pltpu.get_barrier_semaphore()
    for peer in peers:
        pl.semaphore_signal(barrier, inc=1, device_id=peer, device_id_type=pl.DeviceIdType.MESH)
    pl.semaphore_wait(barrier, len(peers))


def shard_columns(x, j, width):
    return x * (width // 4) + j * (width // 8), width // 2 + j * (width // 4) + x * (width // 8)


def cut_count(slots):
    return 5 if slots % 5 == 0 else 1


def gather_grid_kernel(n, slots, grid_qkv, grid_out, slot_ref, w_ref, p_ref, tokens_ref, gain_ref,
                       curv_ref, proj_ref, d_proj_ref, wo_ref, po_ref, normed_t_ref, curv_out_ref,
                       held_w, held_p, matrix, normed, curv_part, send_y, send_core, send_z, recv, tok_send,
                       tok_recv, relay_send, relay_recv, curv_send, curv_recv):
    planes = n // 2
    z, y, x, c = spot()
    zeta = mirrored(z, c, planes)
    hub = lax.rem(zeta, 2) == 0
    spoke = lax.rem(zeta, 2) == 1
    mate = z + 1 - 2 * lax.rem(z, 2)
    y_peer = device(z, 1 - y, x, c)
    x_peer = device(z, y, 1 - x, c)
    core_peer = device(z, y, x, 1 - c)
    z_peer = device(mate, y, x, c)
    row = [device(lax.rem(z + i, planes), y, x, c) for i in range(1, planes)]
    greet(row + [core_peer, y_peer, x_peer])
    cuts = cut_count(slots)
    size = slots // cuts
    own = (w_ref, p_ref)
    held = (held_w, held_p)
    me = 2 * z + y
    tok_cuts = tok_send.shape[0]
    half = normed.shape[0] // 2
    tok_rows = half // tok_cuts
    width = normed.shape[1]
    part = width // 8

    def at(zeta_at):
        return mirrored(zeta_at, c, planes)

    def spread(which, d, j):
        return held[which].at[pl.ds(d * slots + j * size, size)]

    def move(src, which, d, j, peer, sem):
        return pltpu.make_async_remote_copy(
            src_ref=src,
            dst_ref=spread(which, d, j),
            send_sem=sem,
            recv_sem=recv.at[d, which * cuts + j],
            device_id=peer,
            device_id_type=pl.DeviceIdType.MESH,
        )

    def own_chunk(which, j):
        return own[which].at[pl.ds(j * size, size)]

    def arrive(which, d, j):
        move(spread(which, d, j), which, d, j, core_peer, send_y.at[0, 0]).wait_recv()

    other_hub = device(at(2 - zeta), y, x, c)
    near_hub = device(at(2), y, x, c)
    end_hub = device(at(0), y, x, c)

    def token_copy(i, rows_half, peer, s_sem, r_sem, src):
        rows = pl.ds(rows_half * half + i * tok_rows, tok_rows)
        return pltpu.make_async_remote_copy(
            src_ref=src.at[rows],
            dst_ref=normed.at[rows],
            send_sem=s_sem.at[i],
            recv_sem=r_sem.at[i],
            device_id=peer,
            device_id_type=pl.DeviceIdType.MESH,
        )

    def curv_copy(i):
        first = shard_columns(x, lax.rem(mate, 2), width)[i]
        return pltpu.make_async_remote_copy(
            src_ref=curv_ref.at[:, pl.ds(pl.multiple_of(first, part), part)],
            dst_ref=curv_part.at[i],
            send_sem=curv_send.at[i],
            recv_sem=curv_recv.at[i],
            device_id=z_peer,
            device_id_type=pl.DeviceIdType.MESH,
        )

    def curv_local(i):
        first = shard_columns(x, lax.rem(z, 2), width)[i]
        return pltpu.make_async_copy(
            curv_ref.at[:, pl.ds(pl.multiple_of(first, part), part)],
            curv_part.at[i],
            curv_recv.at[i],
        )

    def to_z(which, j):
        k = which * cuts + j
        return move(own_chunk(which, j), which, me, j, other_hub, send_z.at[0, k])

    def to_y(which, j):
        k = which * cuts + j
        return move(own_chunk(which, j), which, me, j, y_peer, send_y.at[0, k])

    def to_core(which, j):
        k = which * cuts + j
        return move(own_chunk(which, j), which, me, j, core_peer, send_core.at[0, k])

    def spoke_own(which, j):
        src = own_chunk(which, j)
        k = which * cuts + j
        return (
            move(src, which, me, j, near_hub, send_z.at[0, k]),
            move(src, which, me, j, end_hub, send_z.at[1, k]),
        )

    lead = min(2, 2 * cuts)
    every = [(which, j) for which in range(2) for j in range(cuts)]

    @pl.when(hub)
    def _():
        for k in range(lead):
            to_y(*every[k]).start()
        for k, one in enumerate(every):
            to_z(*one).start()
            if k < tok_cuts:
                token_copy(k, x, z_peer, tok_send, tok_recv, tokens_ref).start()
            to_core(*one).start()
        for k in range(len(every), tok_cuts):
            token_copy(k, x, z_peer, tok_send, tok_recv, tokens_ref).start()
        for i in range(2):
            curv_copy(i).start()
            curv_local(i).start()

    @pl.when(spoke)
    def _():
        for one in every:
            for copy in spoke_own(*one):
                copy.start()

    def pass_row(k):
        which, j = every[k]
        for r in range(1, planes):
            d = 2 * at(lax.rem(zeta + r, planes)) + y
            arrive(which, d, j)
            src = spread(which, d, j)
            move(src, which, d, j, y_peer, send_y.at[r, k]).start()
            move(src, which, d, j, core_peer, send_core.at[r, k]).start()
            if r == 1 and k + lead < len(every):
                to_y(*every[k + lead]).start()

    def pass_across(k):
        which, j = every[k]
        for r in range(planes):
            d = 2 * at(lax.rem(zeta + r, planes)) + 1 - y
            arrive(which, d, j)
            move(spread(which, d, j), which, d, j, core_peer, send_core.at[planes + r, k]).start()

    def forward(which, j):
        k = which * cuts + j
        pass_row(k)
        if k not in (0, cuts):
            pass_across(k - 1)
        if k in (cuts - 1, 2 * cuts - 1):
            pass_across(k)

    def step(which, j):
        @pl.when(hub)
        def _():
            forward(which, j)

        @pl.when(spoke)
        def _():
            for d in range(n):
                arrive(which, d, j)

    def normalize(source):
        rows = 32

        def some(i, carry):
            here = pl.ds(pl.multiple_of(i * rows, rows), rows)
            values = source[here, :].astype(jnp.float32)
            factor = lax.rsqrt(jnp.mean(values * values, axis=-1, keepdims=True) + EPS)
            normed[here, :] = (values * factor * gain_ref[...]).astype(jnp.bfloat16)
            return carry

        lax.fori_loop(0, normed.shape[0] // rows, some, 0)

    def transpose():
        edge = held_w.shape[-1]

        def some(i, carry):
            here = pl.ds(pl.multiple_of(i * edge, edge), edge)
            normed_t_ref[here, :] = normed[:, here].T
            return carry

        lax.fori_loop(0, normed.shape[1] // edge, some, 0)

    def project(result_ref):
        rows = 256

        def some(i, carry):
            here = pl.ds(pl.multiple_of(i * rows, rows), rows)
            result_ref[here, :] = jnp.dot(
                normed[here, :], matrix[...], preferred_element_type=jnp.float32
            )
            return carry

        lax.fori_loop(0, normed.shape[0] // rows, some, 0)

    def unpack_qkv(which):
        rows, cols = grid_qkv
        edge = held_w.shape[-1]

        def qkv_row(i, carry):
            for col in range(cols):
                matrix[pl.ds(pl.multiple_of(i * edge, edge), edge), col * edge:(col + 1) * edge] = (
                    held[which][slot_ref[i * cols + col]]
                )
            return carry

        lax.fori_loop(0, rows, qkv_row, 0)

    def unpack_out(which, out_ref):
        rows, cols = grid_qkv
        out_rows, out_cols = grid_out
        edge = held_w.shape[-1]

        def out_col(i, carry):
            for r in range(out_rows):
                out_ref[r * edge:(r + 1) * edge, pl.ds(pl.multiple_of(i * edge, edge), edge)] = (
                    held[which][slot_ref[rows * cols + r * out_cols + i]]
                )
            return carry

        lax.fori_loop(0, out_cols, out_col, 0)

    def keep_own(which):
        @pl.when(hub)
        def _():
            held[which][pl.ds(me * slots, slots)] = own[which][...]

    @pl.when(hub)
    def _():
        normalize(tokens_ref)

    @pl.when(spoke)
    def _():
        for i in range(tok_cuts):
            token_copy(i, x, z_peer, tok_send, tok_recv, normed).wait_recv()
            token_copy(i, x, x_peer, relay_send, relay_recv, normed).start()
        for i in range(tok_cuts):
            token_copy(i, 1 - x, x_peer, relay_send, relay_recv, normed).wait_recv()
        for i in range(tok_cuts):
            token_copy(i, x, x_peer, relay_send, relay_recv, normed).wait_send()
        normalize(normed)

    for j in range(cuts):
        step(0, j)
        if j == 0:
            transpose()
    keep_own(0)
    todo = [
        lambda: unpack_qkv(0),
        lambda: project(proj_ref),
        lambda: unpack_out(0, wo_ref),
    ]
    for j in range(cuts):
        step(1, j)
        if j < cuts - 1 and todo:
            todo.pop(0)()
    while todo:
        todo.pop(0)()
    keep_own(1)
    unpack_qkv(1)
    project(d_proj_ref)
    unpack_out(1, po_ref)

    @pl.when(hub)
    def _():
        for i in range(2):
            curv_local(i).wait()

    @pl.when(spoke)
    def _():
        for i in range(2):
            curv_copy(i).wait_recv()

    curv_out_ref[...] = curv_part[...]

    @pl.when(hub)
    def _():
        for i in range(tok_cuts):
            token_copy(i, x, z_peer, tok_send, tok_recv, tokens_ref).wait_send()
        for i in range(2):
            curv_copy(i).wait_send()
        for k, (which, j) in enumerate(every):
            to_z(which, j).wait_send()
            to_y(which, j).wait_send()
            to_core(which, j).wait_send()
            src = spread(which, me, j)
            for r in range(1, planes):
                move(src, which, me, j, y_peer, send_y.at[r, k]).wait_send()
            for r in range(1, n):
                move(src, which, me, j, core_peer, send_core.at[r, k]).wait_send()

    @pl.when(spoke)
    def _():
        for one in every:
            for copy in spoke_own(*one):
                copy.wait_send()


def gather_grid(slot_of, weights, probes, tokens, gain, curvature, n, grid_qkv, grid_out):
    slots, edge, _ = weights.shape
    cuts = cut_count(slots)
    length, width = tokens.shape
    proj = jax.ShapeDtypeStruct((length, grid_qkv[1] * edge), jnp.float32)
    turned = jax.ShapeDtypeStruct((width, length), jnp.bfloat16)
    out = jax.ShapeDtypeStruct((grid_out[0] * edge, grid_out[1] * edge), jnp.bfloat16)
    shard = (2, length, width // 8)
    vmem = pl.BlockSpec(memory_space=pltpu.VMEM)
    dma = pltpu.SemaphoreType.DMA
    return pl.pallas_call(
        functools.partial(gather_grid_kernel, n, slots, grid_qkv, grid_out),
        out_shape=(proj, proj, out, out, turned, jax.ShapeDtypeStruct(shard, jnp.bfloat16)),
        in_specs=[pl.BlockSpec(memory_space=pltpu.SMEM)] + [vmem] * 4
        + [pl.BlockSpec(memory_space=pl.ANY)],
        out_specs=(vmem,) * 6,
        scratch_shapes=[
            pltpu.VMEM((n * slots, edge, edge), jnp.bfloat16),
            pltpu.VMEM((n * slots, edge, edge), jnp.bfloat16),
            pltpu.VMEM((grid_qkv[0] * edge, grid_qkv[1] * edge), jnp.bfloat16),
            pltpu.VMEM((length, width), jnp.bfloat16),
            pltpu.VMEM(shard, jnp.bfloat16),
            dma((n // 2, 2 * cuts)),
            dma((n, 2 * cuts)),
            dma((2, 2 * cuts)),
            dma((n, 2 * cuts)),
            dma((4,)),
            dma((4,)),
            dma((4,)),
            dma((4,)),
            dma((2,)),
            dma((2,)),
        ],
        compiler_params=pltpu.CompilerParams(
            collective_id=3, has_side_effects=True, vmem_limit_bytes=GRID_VMEM_BYTES
        ),
    )(slot_of, weights, probes, tokens, gain, curvature)


def square_kernel(mixed_ref, d_mixed_ref, w_ref, p_ref, curv_ref, weighted_ref, back_ref, terms,
                  near_x, near_z, pair_a, pair_b, far_z, far_x, full, send_sem, recv_sem):
    z, y, x, c = spot()
    side = lax.rem(z, 2)
    x_peer = device(z, y, 1 - x, c)
    z_peer = device(z + 1 - 2 * side, y, x, c)
    greet([x_peer, z_peer])
    length, width = terms.shape
    quarter, part = width // 4, width // 8
    chunks = recv_sem.shape[1]
    rows = length // chunks

    def block(i):
        return pl.ds(i * rows, rows)

    def cols(first, count):
        return pl.ds(pl.multiple_of(first, count), count)

    keep_a, give_a = cols(x * quarter, quarter), cols((1 - x) * quarter, quarter)
    keep_b = cols(width // 2 + side * quarter, quarter)
    give_b = cols(width // 2 + (1 - side) * quarter, quarter)
    first_a, first_b = shard_columns(x, side, width)
    own_a, own_b = cols(first_a, part), cols(first_b, part)

    def copy(kind, i, here, there, target):
        return pltpu.make_async_remote_copy(
            src_ref=here,
            dst_ref=there,
            send_sem=send_sem.at[kind, i],
            recv_sem=recv_sem.at[kind, i],
            device_id=target,
            device_id_type=pl.DeviceIdType.MESH,
        )

    def stage(i):
        b = block(i)
        return (
            copy(0, i, terms.at[b, give_a], near_x.at[b], x_peer),
            copy(1, i, terms.at[b, give_b], near_z.at[b], z_peer),
            copy(2, i, pair_a.at[b, cols((1 - side) * part, part)], far_z.at[b], z_peer),
            copy(3, i, pair_b.at[b, cols((1 - x) * part, part)], far_x.at[b], x_peer),
            copy(4, i, full.at[b, own_a], full.at[b, own_a], z_peer),
            copy(5, i, full.at[b, own_b], full.at[b, own_b], x_peer),
            copy(6, i, full.at[b, keep_a], full.at[b, keep_a], x_peer),
            copy(7, i, full.at[b, keep_b], full.at[b, keep_b], z_peer),
        )

    def incoming(kind, i, there):
        copy(kind, i, there, there, x_peer).wait_recv()

    def terms_of(i):
        tile = width // 4

        def columns(j, carry):
            here = pl.ds(pl.multiple_of(j * tile, tile), tile)
            terms[block(i), here] = (
                jnp.dot(d_mixed_ref[block(i), :], w_ref[:, here], preferred_element_type=jnp.float32)
                + jnp.dot(mixed_ref[block(i), :], p_ref[:, here], preferred_element_type=jnp.float32)
            ).astype(jnp.bfloat16)
            return carry

        lax.fori_loop(0, 4, columns, 0)

    plans = [stage(i) for i in range(chunks)]

    def pair_up(i):
        b = block(i)
        for kind, pair, keep, near in ((0, pair_a, keep_a, near_x), (1, pair_b, keep_b, near_z)):
            incoming(kind, i, near.at[b])
            pair[b] = (
                terms[b, keep].astype(jnp.float32) + near[b].astype(jnp.float32)
            ).astype(jnp.bfloat16)
            plans[i][2 + kind].start()

    def weigh(i):
        b = block(i)
        for kind, pair, mine, far, own_cols in (
            (0, pair_a, side, far_z, own_a), (1, pair_b, x, far_x, own_b)
        ):
            incoming(2 + kind, i, far.at[b])
            total = pair[b, cols(mine * part, part)].astype(jnp.float32) + far[b].astype(jnp.float32)
            full[b, own_cols] = (curv_ref[kind, b].astype(jnp.float32) * total).astype(jnp.bfloat16)
            plans[i][4 + kind].start()

    def widen(i):
        b = block(i)
        other_a, other_b = shard_columns(x, 1 - side, width)[0], shard_columns(1 - x, side, width)[1]
        incoming(4, i, full.at[b, cols(other_a, part)])
        plans[i][6].start()
        incoming(5, i, full.at[b, cols(other_b, part)])
        plans[i][7].start()

    def finish(i):
        b = block(i)
        incoming(6, i, full.at[b, give_a])
        incoming(7, i, full.at[b, give_b])
        weighted_ref[b, :] = full[b, :]
        back_ref[b, :] = lax.dot_general(
            full[b, :], w_ref[...], (((1,), (1,)), ((), ())), preferred_element_type=jnp.float32
        ).astype(jnp.bfloat16)

    for i in range(chunks + 3):
        if i < chunks:
            terms_of(i)
            plans[i][0].start()
            plans[i][1].start()
        if 0 <= i - 1 < chunks:
            pair_up(i - 1)
        if 0 <= i - 2 < chunks:
            weigh(i - 2)
        if 0 <= i - 3 < chunks:
            widen(i - 3)
    for i in range(chunks):
        finish(i)
    for plan in plans:
        for one in plan:
            one.wait_send()


def square_exchange(mixed, d_mixed, w_out, p_out, curvature):
    length, inner = mixed.shape
    width = w_out.shape[1]
    chunks = 4
    vmem = pl.BlockSpec(memory_space=pltpu.VMEM)
    quarter = pltpu.VMEM((length, width // 4), jnp.bfloat16)
    part = pltpu.VMEM((length, width // 8), jnp.bfloat16)
    whole = pltpu.VMEM((length, width), jnp.bfloat16)
    return pl.pallas_call(
        square_kernel,
        out_shape=(
            jax.ShapeDtypeStruct((length, width), jnp.bfloat16),
            jax.ShapeDtypeStruct(mixed.shape, jnp.bfloat16),
        ),
        in_specs=[vmem] * 5,
        out_specs=(vmem, vmem),
        scratch_shapes=[
            whole, quarter, quarter, quarter, quarter, part, part, whole,
            pltpu.SemaphoreType.DMA((8, chunks)),
            pltpu.SemaphoreType.DMA((8, chunks)),
        ],
        compiler_params=pltpu.CompilerParams(
            collective_id=4, has_side_effects=True, vmem_limit_bytes=GRID_VMEM_BYTES
        ),
    )(mixed, d_mixed, w_out, p_out, curvature)


def reduce_grid_kernel(n, slots, scale, grid_qkv, grid_out, pick_ref, normed_t_ref, d_proj_ref,
                       mixed_t_ref, weighted_ref, out_ref, grads, peer, begin, across, onward,
                       landed, core_send, core_recv, y_send, y_recv, z_send, z_recv):
    planes = n // 2
    z, y, x, c = spot()
    zeta = mirrored(z, c, planes)
    hub = lax.rem(zeta, 2) == 0
    spoke = lax.rem(zeta, 2) == 1
    late = lax.div(zeta, 2)
    y_peer = device(z, 1 - y, x, c)
    core_peer = device(z, y, x, 1 - c)
    row = [device(lax.rem(z + i, planes), y, x, c) for i in range(1, planes)]
    greet(row + [core_peer, y_peer])
    cuts = cut_count(slots)
    size = slots // cuts
    rows, cols = grid_qkv
    out_rows, out_cols = grid_out
    total = rows * cols + out_rows * out_cols
    edge = out_ref.shape[-1]
    legs = core_send.shape[0] - 1
    leg_rows = rows // legs
    group = 2

    def core_copy(i):
        if i == legs:
            here = pl.ds(rows * cols, out_rows * out_cols)
        else:
            here = pl.ds(i * leg_rows * cols, leg_rows * cols)
        return pltpu.make_async_remote_copy(
            src_ref=grads.at[here],
            dst_ref=peer.at[here],
            send_sem=core_send.at[i],
            recv_sem=core_recv.at[i],
            device_id=core_peer,
            device_id_type=pl.DeviceIdType.MESH,
        )

    def out_columns(i, carry):
        width = group * edge
        right = weighted_ref[:, pl.ds(pl.multiple_of(i * width, width), width)]
        block = jnp.dot(
            mixed_t_ref[...], right, preferred_element_type=jnp.float32
        ).astype(jnp.bfloat16)
        for r in range(out_rows):
            for k in range(group):
                grads[rows * cols + r * out_cols + i * group + k] = block[
                    r * edge:(r + 1) * edge, k * edge:(k + 1) * edge
                ]
        return carry

    def qkv_rows(i, carry):
        width = group * edge
        left = normed_t_ref[pl.ds(pl.multiple_of(i * width, width), width), :]
        block = jnp.dot(
            left, d_proj_ref[...], preferred_element_type=jnp.float32
        ).astype(jnp.bfloat16)
        for r in range(group):
            for k in range(cols):
                grads[(i * group + r) * cols + k] = block[
                    r * edge:(r + 1) * edge, k * edge:(k + 1) * edge
                ]
        return carry

    def hand_over(i):
        @pl.when(spoke)
        def _():
            core_copy(i).start()

    grads[total] = jnp.zeros((edge, edge), grads.dtype)
    peer[total] = jnp.zeros((edge, edge), peer.dtype)
    lax.fori_loop(0, out_cols // group, out_columns, 0)
    hand_over(legs)
    for i in range(legs):
        steps = leg_rows // group
        lax.fori_loop(i * steps, (i + 1) * steps, qkv_rows, 0)
        hand_over(i)

    def owner(i, at_y):
        first = (3, 2, 1, 0)[i]
        second = (0, 1, 3, 2)[i]
        o = (1 - late) * first + late * second
        return 2 * mirrored(o, c, planes) + at_y

    def both(index):
        return grads[index].astype(jnp.float32) + peer[index].astype(jnp.float32)

    def y_copy(i, j):
        here = pl.ds(i * slots + j * size, size)
        return pltpu.make_async_remote_copy(
            src_ref=begin.at[here],
            dst_ref=across.at[here],
            send_sem=y_send.at[i, j],
            recv_sem=y_recv.at[i, j],
            device_id=y_peer,
            device_id_type=pl.DeviceIdType.MESH,
        )

    def z_copy(i, j):
        goal = (1 - late) * (2, 2, 1)[i] + late * (0, 1, 3)[i]
        buffer = (0, 1, 0)[i]
        return pltpu.make_async_remote_copy(
            src_ref=onward.at[i, pl.ds(j * size, size)],
            dst_ref=landed.at[buffer, pl.ds(j * size, size)],
            send_sem=z_send.at[i, j],
            recv_sem=z_recv.at[buffer, j],
            device_id=device(mirrored(goal, c, planes), y, x, c),
            device_id_type=pl.DeviceIdType.MESH,
        )

    def z_wait(buffer, j):
        here = landed.at[buffer, pl.ds(j * size, size)]
        pltpu.make_async_remote_copy(
            src_ref=here,
            dst_ref=here,
            send_sem=z_send.at[0, j],
            recv_sem=z_recv.at[buffer, j],
            device_id=core_peer,
            device_id_type=pl.DeviceIdType.MESH,
        ).wait_recv()

    def each(j, body):
        def some(t, carry):
            body(j * size + t)
            return carry

        lax.fori_loop(0, size, some, 0)

    @pl.when(hub)
    def _():
        for i in (legs,) + tuple(range(legs)):
            core_copy(i).wait_recv()
        for i in range(planes):
            base = owner(i, 1 - y) * slots

            def start(j, carry, i=i, base=base):
                def fill(t):
                    begin[i * slots + t] = both(pick_ref[base + t]).astype(jnp.bfloat16)

                each(j, fill)
                y_copy(i, j).start()
                return carry

            lax.fori_loop(0, cuts, start, 0)
        for i in range(planes):
            base = owner(i, y) * slots

            def value(t, i=i, base=base):
                return both(pick_ref[base + t]) + across[i * slots + t].astype(jnp.float32)

            def go(j, carry, i=i, value=value):
                y_copy(i, j).wait_recv()
                if i < 2:

                    def pass_on(t):
                        onward[i, t] = value(t).astype(jnp.bfloat16)

                    each(j, pass_on)
                    z_copy(i, j).start()
                elif i == 2:

                    @pl.when(late == 0)
                    def _():
                        def pass_on(t):
                            onward[i, t] = value(t).astype(jnp.bfloat16)

                        each(j, pass_on)

                    @pl.when(late == 1)
                    def _():
                        z_wait(0, j)

                        def pass_on(t):
                            onward[i, t] = (
                                value(t) + landed[0, t].astype(jnp.float32)
                            ).astype(jnp.bfloat16)

                        each(j, pass_on)

                    z_copy(i, j).start()
                else:
                    z_wait(late, j)

                    def last(t):
                        out_ref[t] = (value(t) + landed[late, t].astype(jnp.float32)) * scale

                    each(j, last)
                return carry

            lax.fori_loop(0, cuts, go, 0)

        def close(j, carry):
            for i in range(planes):
                y_copy(i, j).wait_send()
            for i in range(3):
                z_copy(i, j).wait_send()
            return carry

        lax.fori_loop(0, cuts, close, 0)

    @pl.when(spoke)
    def _():
        @pl.when(zeta == 1)
        def _():
            def go(j, carry):
                z_wait(0, j)
                z_wait(1, j)

                def last(t):
                    out_ref[t] = (
                        landed[0, t].astype(jnp.float32) + landed[1, t].astype(jnp.float32)
                    ) * scale

                each(j, last)
                return carry

            lax.fori_loop(0, cuts, go, 0)

        @pl.when(zeta == 3)
        def _():
            def go(j, carry):
                z_wait(0, j)

                def last(t):
                    out_ref[t] = landed[0, t].astype(jnp.float32) * scale

                each(j, last)
                return carry

            lax.fori_loop(0, cuts, go, 0)

        for i in range(legs + 1):
            core_copy(i).wait_send()


def reduce_grid(picked, normed_t, d_proj, mixed_t, weighted, n, scale, grid_qkv, grid_out):
    slots = picked.shape[0] // n
    edge = BLK
    total_blocks = grid_qkv[0] * grid_qkv[1] + grid_out[0] * grid_out[1]
    cuts = cut_count(slots)
    legs = 4
    vmem = pl.BlockSpec(memory_space=pltpu.VMEM)
    dma = pltpu.SemaphoreType.DMA
    return pl.pallas_call(
        functools.partial(reduce_grid_kernel, n, slots, scale, grid_qkv, grid_out),
        out_shape=jax.ShapeDtypeStruct((slots, edge, edge), jnp.float32),
        in_specs=[pl.BlockSpec(memory_space=pltpu.SMEM)] + [vmem] * 4,
        out_specs=vmem,
        scratch_shapes=[
            pltpu.VMEM((total_blocks + 1, edge, edge), jnp.bfloat16),
            pltpu.VMEM((total_blocks + 1, edge, edge), jnp.bfloat16),
            pltpu.VMEM((n // 2 * slots, edge, edge), jnp.bfloat16),
            pltpu.VMEM((n // 2 * slots, edge, edge), jnp.bfloat16),
            pltpu.VMEM((3, slots, edge, edge), jnp.bfloat16),
            pltpu.VMEM((2, slots, edge, edge), jnp.bfloat16),
            dma((legs + 1,)),
            dma((legs + 1,)),
            dma((n // 2, cuts)),
            dma((n // 2, cuts)),
            dma((3, cuts)),
            dma((2, cuts)),
        ],
        compiler_params=pltpu.CompilerParams(
            collective_id=5, has_side_effects=True, vmem_limit_bytes=GRID_VMEM_BYTES
        ),
    )(picked, normed_t, d_proj, mixed_t, weighted)


def local_grid(tokens, norm_gain, curvature, weight_slots, probe_slots, block_counts):
    n_columns = lax.axis_size("seq")
    n_owners = lax.axis_size("fsdp")
    q_heads = HQ // n_columns
    kv_heads = HK // n_columns
    row_blocks = D // BLK
    qkv_cols = (q_heads + 2 * kv_heads) * HD // BLK
    out_rows = q_heads * HD // BLK
    grid_qkv, grid_out = (row_blocks, qkv_cols), (out_rows, row_blocks)
    total_blocks = row_blocks * qkv_cols + out_rows * row_blocks
    slots = weight_slots.shape[1]
    length = tokens.shape[1]
    z, _, _, c = spot()
    theirs = lax.ppermute(block_counts, "seq", [(i, i ^ 1) for i in range(n_columns)])
    counts = jnp.where(lax.rem(z, 2) == c, block_counts, theirs)[0]
    range_ends = jnp.cumsum(counts)
    starts = range_ends - counts
    owner_ids = jnp.arange(n_owners, dtype=jnp.int32)
    block_ids = jnp.arange(total_blocks, dtype=jnp.int32)
    owners = jnp.sum((range_ends[None, :] <= block_ids[:, None]).astype(jnp.int32), axis=1)
    first_block = jnp.sum(
        jnp.where(owners[:, None] == owner_ids[None, :], starts[None, :], 0), axis=1
    )
    slot_of = (owners * slots + block_ids - first_block).astype(jnp.int32)
    projected, d_projected, w_out, p_out, normed_t, curv_part = gather_grid(
        slot_of,
        weight_slots[0],
        probe_slots[0],
        tokens[0],
        norm_gain[None, :],
        curvature[0],
        n_owners,
        grid_qkv,
        grid_out,
    )
    cosine, sine = rotary(length, HD)

    def inner(projected):
        return attention(projected, cosine, sine, q_heads, kv_heads)

    mixed, d_mixed = jax.jvp(inner, (projected,), (d_projected,))
    weighted, back_mixed = square_exchange(mixed, d_mixed, w_out, p_out, curv_part)
    mixed_again, pullback = jax.vjp(inner, projected)
    (back_projected,) = pullback(back_mixed)
    slot_index = jnp.arange(n_owners * slots, dtype=jnp.int32)
    place = slot_index % slots
    owner_hot = (slot_index // slots)[:, None] == owner_ids[None, :]
    owner_first = jnp.sum(jnp.where(owner_hot, starts[None, :], 0), axis=1)
    own_count = jnp.sum(jnp.where(owner_hot, counts[None, :], 0), axis=1)
    picked = jnp.where(place < own_count, owner_first + place, total_blocks).astype(jnp.int32)
    scaled = reduce_grid(
        picked,
        normed_t,
        back_projected.astype(jnp.bfloat16),
        mixed_again.T,
        weighted,
        n_owners,
        (length * n_owners) ** -0.5,
        grid_qkv,
        grid_out,
    )
    return scaled.reshape(1, slots, BLK, BLK)


def solution(mesh):
    in_specs = (
        P("fsdp", None, None),
        P(),
        P("fsdp", None, None),
        P("seq", "fsdp", None, None),
        P("seq", "fsdp", None, None),
        P("seq", None),
    )
    out_specs = P("seq", "fsdp", None, None)
    body = local_grid if mesh.shape["fsdp"] == 8 and mesh.shape["seq"] == 4 else local
    return jax.shard_map(body, mesh=mesh, in_specs=in_specs, out_specs=out_specs, check_vma=False)
```

```python
import functools

import jax
import jax.numpy as jnp
from jax import lax
from jax.experimental import pallas as pl
from jax.experimental.pallas import tpu as pltpu
from jax.sharding import PartitionSpec as P

D = 4096
HQ = 16
HK = 4
HD = 128
BLK = 128


THETA = 500000.0
EPS = 1e-05
NEGATIVE = -1e30


def rotary(length, head_dim):
    half_dim = head_dim // 2
    frequency = jnp.exp(-jnp.log(THETA) * 2.0 * jnp.arange(half_dim, dtype=jnp.float32) / head_dim)
    angles = jnp.arange(length, dtype=jnp.float32)[:, None] * frequency[None, :]
    return (jnp.cos(angles)[:, None, :], jnp.sin(angles)[:, None, :])


def rotate(field_in, cosine, sine):
    half_dim = field_in.shape[-1] // 2
    first_half = field_in[..., :half_dim]
    second = field_in[..., half_dim:]
    return jnp.concatenate(
        [first_half * cosine - second * sine, second * cosine + first_half * sine], axis=-1
    )


VMEM_BYTES = 62 * 1024 * 1024
GRID_VMEM_BYTES = 67043328


def attention(projected, cosine, sine, q_heads, kv_heads):
    length = projected.shape[0]
    head_dim = projected.shape[1] // (q_heads + 2 * kv_heads)
    q_end = q_heads * head_dim
    k_end = q_end + kv_heads * head_dim
    queries = rotate(projected[:, :q_end].reshape(length, q_heads, head_dim), cosine, sine).astype(
        jnp.bfloat16
    )
    key_rows = rotate(
        projected[:, q_end:k_end].reshape(length, kv_heads, head_dim), cosine, sine
    ).astype(jnp.bfloat16)
    values = projected[:, k_end:].reshape(length, kv_heads, head_dim).astype(jnp.bfloat16)
    queries = queries.reshape(length, kv_heads, q_heads // kv_heads, head_dim)
    scores = jnp.einsum(
        "qkgd,skd->kgqs", queries, key_rows, preferred_element_type=jnp.float32
    ) * head_dim ** (-0.5)
    causal = jnp.arange(length)[:, None] >= jnp.arange(length)[None, :]
    scores = jnp.where(causal, scores, NEGATIVE)
    attn_probs = jax.nn.softmax(scores, axis=-1).astype(jnp.bfloat16)
    mixed_heads = jnp.einsum(
        "kgqs,skd->qkgd", attn_probs, values, preferred_element_type=jnp.float32
    )
    return mixed_heads.reshape(length, q_heads * head_dim).astype(jnp.bfloat16)


def ring_position(index, n):
    odd = lax.rem(index, 2)
    half = lax.div(index, 2)
    return (1 - odd) * half + odd * (n - 1 - half)


def ring_index(position, n):
    back = lax.div(position, n // 2)
    return (1 - back) * 2 * position + back * (2 * (n - 1 - position) + 1)


def pieces(slots):
    half = slots // 2
    out = []
    for direction, first, count in ((0, 0, half), (1, half, slots - half)):
        cuts = 5 if count % 5 == 0 else 1
        size = count // cuts
        out.append([(first + i * size, size) for i in range(cuts)])
    return out


def enter(neighbours, axis="fsdp"):
    barrier = pltpu.get_barrier_semaphore()
    for neighbour in neighbours:
        pl.semaphore_signal(
            barrier, inc=1, device_id={axis: neighbour}, device_id_type=pl.DeviceIdType.MESH
        )
    pl.semaphore_wait(barrier, len(neighbours))


def gather_kernel(n, slots, grid_qkv, grid_out, slot_ref, w_ref, p_ref, tokens_ref, gain_ref,
                  proj_ref, d_proj_ref, wo_ref, po_ref, normed_t_ref, held_w, held_p, matrix,
                  normed, send_sem, recv_sem):
    me = lax.axis_index("fsdp")
    pos = ring_position(me, n)
    right = ring_index(lax.rem(pos + 1, n), n)
    left = ring_index(lax.rem(pos + n - 1, n), n)
    towards = (right, left)
    enter((left, right))
    parts = pieces(slots)
    arrays = ((w_ref, held_w), (p_ref, held_p))

    def copy(which, step, direction, j):
        own, held = arrays[which]
        first, size = parts[direction][j]
        shift = n - step if direction == 0 else step
        origin = ring_index(lax.rem(pos + shift, n), n)
        there = held.at[pl.ds(origin * slots + first, size)]
        here = own.at[pl.ds(first, size)] if step == 0 else there
        return pltpu.make_async_remote_copy(
            src_ref=here,
            dst_ref=there,
            send_sem=send_sem.at[which, step, direction, j],
            recv_sem=recv_sem.at[which, step, direction, j],
            device_id={"fsdp": towards[direction]},
            device_id_type=pl.DeviceIdType.MESH,
        )

    def arrival(which, step, direction, j):
        first, size = parts[direction][j]
        own, held = arrays[which]
        shift = n - step - 1 if direction == 0 else step + 1
        origin = ring_index(lax.rem(pos + shift, n), n)
        there = held.at[pl.ds(origin * slots + first, size)]
        pltpu.make_async_remote_copy(
            src_ref=there,
            dst_ref=there,
            send_sem=send_sem.at[which, step, direction, j],
            recv_sem=recv_sem.at[which, step, direction, j],
            device_id={"fsdp": towards[direction]},
            device_id_type=pl.DeviceIdType.MESH,
        ).wait_recv()

    def each():
        for j in range(max(len(parts[0]), len(parts[1]))):
            for direction in range(2):
                if j < len(parts[direction]):
                    yield direction, j

    def normalize():
        rows = 32

        def some(i, carry):
            here = pl.ds(pl.multiple_of(i * rows, rows), rows)
            values = tokens_ref[here, :].astype(jnp.float32)
            factor = lax.rsqrt(jnp.mean(values * values, axis=-1, keepdims=True) + EPS)
            normed[here, :] = (values * factor * gain_ref[...]).astype(jnp.bfloat16)
            return carry

        lax.fori_loop(0, normed.shape[0] // rows, some, 0)

    def transpose():
        edge = held_w.shape[-1]

        def some(i, carry):
            here = pl.ds(pl.multiple_of(i * edge, edge), edge)
            normed_t_ref[here, :] = normed[:, here].T
            return carry

        lax.fori_loop(0, normed.shape[1] // edge, some, 0)

    def project(result_ref):
        rows = 256

        def some(i, carry):
            here = pl.ds(pl.multiple_of(i * rows, rows), rows)
            result_ref[here, :] = jnp.dot(
                normed[here, :], matrix[...], preferred_element_type=jnp.float32
            )
            return carry

        lax.fori_loop(0, normed.shape[0] // rows, some, 0)

    def unpack(which, qkv_ref, out_ref):
        own, held = arrays[which]
        rows, cols = grid_qkv
        edge = held.shape[-1]

        def qkv_row(i, carry):
            for c in range(cols):
                qkv_ref[pl.ds(pl.multiple_of(i * edge, edge), edge), c * edge:(c + 1) * edge] = (
                    held[slot_ref[i * cols + c]]
                )
            return carry

        lax.fori_loop(0, rows, qkv_row, 0)
        out_rows, out_cols = grid_out

        def out_col(i, carry):
            for r in range(out_rows):
                out_ref[r * edge:(r + 1) * edge, pl.ds(pl.multiple_of(i * edge, edge), edge)] = (
                    held[slot_ref[rows * cols + r * out_cols + i]]
                )
            return carry

        lax.fori_loop(0, out_cols, out_col, 0)

    def finish(which, qkv_ref, out_ref):
        own, held = arrays[which]
        for direction, j in each():
            arrival(which, n - 2, direction, j)
        held[pl.ds(me * slots, slots)] = own[...]
        unpack(which, qkv_ref, out_ref)

    sent = []
    for which in range(2):
        for step in range(n - 1):
            for direction, j in each():
                if step > 0:
                    arrival(which, step - 1, direction, j)
                one = copy(which, step, direction, j)
                one.start()
                sent.append(one)
            if which == 0 and step == 0:
                normalize()
            if which == 0 and step == 1:
                transpose()
            if which == 1 and step == 0:
                finish(0, matrix, wo_ref)
            if which == 1 and step == 1:
                project(proj_ref)
    finish(1, matrix, po_ref)
    project(d_proj_ref)
    for one in sent:
        one.wait_send()


def gather_weights(slot_of, weights, probes, tokens, gain, n, grid_qkv, grid_out):
    slots, edge, _ = weights.shape
    cuts = max(len(part) for part in pieces(slots))
    length, width = tokens.shape
    proj = jax.ShapeDtypeStruct((length, grid_qkv[1] * edge), jnp.float32)
    turned = jax.ShapeDtypeStruct((width, length), jnp.bfloat16)
    out = jax.ShapeDtypeStruct((grid_out[0] * edge, grid_out[1] * edge), jnp.bfloat16)
    vmem = pl.BlockSpec(memory_space=pltpu.VMEM)
    return pl.pallas_call(
        functools.partial(gather_kernel, n, slots, grid_qkv, grid_out),
        out_shape=(proj, proj, out, out, turned),
        in_specs=[pl.BlockSpec(memory_space=pltpu.SMEM)] + [vmem] * 4,
        out_specs=(vmem,) * 5,
        scratch_shapes=[
            pltpu.VMEM((n * slots, edge, edge), jnp.bfloat16),
            pltpu.VMEM((n * slots, edge, edge), jnp.bfloat16),
            pltpu.VMEM((grid_qkv[0] * edge, grid_qkv[1] * edge), jnp.bfloat16),
            pltpu.VMEM((length, width), jnp.bfloat16),
            pltpu.SemaphoreType.DMA((2, n - 1, 2, cuts)),
            pltpu.SemaphoreType.DMA((2, n - 1, 2, cuts)),
        ],
        compiler_params=pltpu.CompilerParams(
            collective_id=0, has_side_effects=True, vmem_limit_bytes=VMEM_BYTES
        ),
    )(slot_of, weights, probes, tokens, gain)


def gradient_blocks(grid_qkv, grid_out, normed_t_ref, d_proj_ref, mixed_t_ref, weighted_ref,
                    out_ref):
    edge = out_ref.shape[-1]
    rows, cols = grid_qkv
    out_rows, out_cols = grid_out
    group = 2

    out_ref[rows * cols + out_rows * out_cols] = jnp.zeros((edge, edge), out_ref.dtype)

    def qkv_rows(i, carry):
        width = group * edge
        left = normed_t_ref[pl.ds(pl.multiple_of(i * width, width), width), :]
        block = jnp.dot(
            left, d_proj_ref[...], preferred_element_type=jnp.float32
        ).astype(jnp.bfloat16)
        for r in range(group):
            for c in range(cols):
                out_ref[(i * group + r) * cols + c] = block[
                    r * edge:(r + 1) * edge, c * edge:(c + 1) * edge
                ]
        return carry

    lax.fori_loop(0, rows // group, qkv_rows, 0)

    def out_columns(i, carry):
        width = group * edge
        right = weighted_ref[:, pl.ds(pl.multiple_of(i * width, width), width)]
        block = jnp.dot(
            mixed_t_ref[...], right, preferred_element_type=jnp.float32
        ).astype(jnp.bfloat16)
        for r in range(out_rows):
            for c in range(group):
                out_ref[rows * cols + r * out_cols + i * group + c] = block[
                    r * edge:(r + 1) * edge, c * edge:(c + 1) * edge
                ]
        return carry

    lax.fori_loop(0, out_cols // group, out_columns, 0)


def reduce_kernel(n, slots, scale, grid_qkv, grid_out, pick_ref, normed_t_ref, d_proj_ref,
                  mixed_t_ref, weighted_ref, out_ref, grads, begin, held, send_sem, recv_sem):
    me = lax.axis_index("fsdp")
    pos = ring_position(me, n)
    right = ring_index(lax.rem(pos + 1, n), n)
    left = ring_index(lax.rem(pos + n - 1, n), n)
    towards = (right, left)
    enter((left, right))
    parts = pieces(slots)
    gradient_blocks(
        grid_qkv, grid_out, normed_t_ref, d_proj_ref, mixed_t_ref, weighted_ref, grads
    )

    def own(step, direction, j):
        shift = n - 1 - step if direction == 0 else 1 + step
        target = ring_index(lax.rem(pos + shift, n), n)
        return target * slots

    def each_block(direction, j, body):
        first, size = parts[direction][j]

        def some(i, carry):
            body(first + i)
            return carry

        lax.fori_loop(0, size, some, 0)

    def copy(step, direction, j):
        first, size = parts[direction][j]
        here = begin.at[pl.ds(first, size)] if step == 0 else held.at[step - 1, pl.ds(first, size)]
        return pltpu.make_async_remote_copy(
            src_ref=here,
            dst_ref=held.at[step, pl.ds(first, size)],
            send_sem=send_sem.at[step, direction, j],
            recv_sem=recv_sem.at[step, direction, j],
            device_id={"fsdp": towards[direction]},
            device_id_type=pl.DeviceIdType.MESH,
        )

    def each():
        for j in range(max(len(parts[0]), len(parts[1]))):
            for direction in range(2):
                if j < len(parts[direction]):
                    yield direction, j

    sent = {}
    for step in range(n - 1):
        for direction, j in each():
            first, size = parts[direction][j]
            base = own(step, direction, j)
            if step > 0:
                sent[step - 1, direction, j].wait_recv()

                def add(t, step=step, base=base):
                    held[step - 1, t] = (
                        held[step - 1, t].astype(jnp.float32)
                        + grads[pick_ref[base + t]].astype(jnp.float32)
                    ).astype(jnp.bfloat16)

                each_block(direction, j, add)
            else:

                def fill(t, base=base):
                    begin[t] = grads[pick_ref[base + t]]

                each_block(direction, j, fill)
            one = copy(step, direction, j)
            one.start()
            sent[step, direction, j] = one
    for direction, j in each():
        first, size = parts[direction][j]
        sent[n - 2, direction, j].wait_recv()
        base = own(n - 1, direction, j)

        def last(t, base=base):
            out_ref[t] = (
                held[n - 2, t].astype(jnp.float32) + grads[pick_ref[base + t]].astype(jnp.float32)
            ) * scale

        each_block(direction, j, last)
    for one in sent.values():
        one.wait_send()


def reduce_slots(picked, normed_t, d_proj, mixed_t, weighted, n, scale, grid_qkv, grid_out):
    slots = picked.shape[0] // n
    edge = BLK
    total_blocks = grid_qkv[0] * grid_qkv[1] + grid_out[0] * grid_out[1]
    cuts = max(len(part) for part in pieces(slots))
    vmem = pl.BlockSpec(memory_space=pltpu.VMEM)
    return pl.pallas_call(
        functools.partial(reduce_kernel, n, slots, scale, grid_qkv, grid_out),
        out_shape=jax.ShapeDtypeStruct((slots, edge, edge), jnp.float32),
        in_specs=[pl.BlockSpec(memory_space=pltpu.SMEM)] + [vmem] * 4,
        out_specs=vmem,
        scratch_shapes=[
            pltpu.VMEM((total_blocks + 1, edge, edge), jnp.bfloat16),
            pltpu.VMEM((slots, edge, edge), jnp.bfloat16),
            pltpu.VMEM((n - 1, slots, edge, edge), jnp.bfloat16),
            pltpu.SemaphoreType.DMA((n - 1, 2, cuts)),
            pltpu.SemaphoreType.DMA((n - 1, 2, cuts)),
        ],
        compiler_params=pltpu.CompilerParams(
            collective_id=1, has_side_effects=True, vmem_limit_bytes=VMEM_BYTES
        ),
    )(picked, normed_t, d_proj, mixed_t, weighted)


def exchange_kernel(mixed_ref, d_mixed_ref, w_ref, p_ref, curv_ref, weighted_ref, back_ref,
                    terms, near, pair, far, share, rest, send_sem, recv_sem):
    me = lax.axis_index("seq")
    side = lax.rem(me, 2)
    core = me + 1 - 2 * side
    across = me + 2 - 4 * lax.rem(lax.div(me, 2), 2)
    enter((core, across), "seq")
    length, width = terms.shape
    half = width // 2
    chunks = recv_sem.shape[1]
    rows = length // chunks
    mine = pl.ds(pl.multiple_of(side * half, half), half)
    other = pl.ds(pl.multiple_of((1 - side) * half, half), half)

    def block(i):
        return pl.ds(i * rows, rows)

    def copy(stage, i, here, there, target):
        return pltpu.make_async_remote_copy(
            src_ref=here,
            dst_ref=there,
            send_sem=send_sem.at[stage, i],
            recv_sem=recv_sem.at[stage, i],
            device_id={"seq": target},
            device_id_type=pl.DeviceIdType.MESH,
        )

    def terms_of(i):
        tile = width // 4

        def columns(j, carry):
            cols = pl.ds(pl.multiple_of(j * tile, tile), tile)
            terms[block(i), cols] = (
                jnp.dot(d_mixed_ref[block(i), :], w_ref[:, cols], preferred_element_type=jnp.float32)
                + jnp.dot(mixed_ref[block(i), :], p_ref[:, cols], preferred_element_type=jnp.float32)
            ).astype(jnp.bfloat16)
            return carry

        lax.fori_loop(0, 4, columns, 0)

    first = [copy(0, i, terms.at[block(i), other], near.at[block(i)], core) for i in range(chunks)]
    second = [copy(1, i, pair.at[block(i)], far.at[block(i)], across) for i in range(chunks)]
    third = [copy(2, i, share.at[block(i)], rest.at[block(i)], core) for i in range(chunks)]

    def send_pair(i):
        first[i].wait_recv()
        pair[block(i)] = (
            terms[block(i), mine].astype(jnp.float32) + near[block(i)].astype(jnp.float32)
        ).astype(jnp.bfloat16)
        second[i].start()

    def send_share(i):
        second[i].wait_recv()
        total = pair[block(i)].astype(jnp.float32) + far[block(i)].astype(jnp.float32)
        share[block(i)] = (curv_ref[block(i), mine].astype(jnp.float32) * total).astype(
            jnp.bfloat16
        )
        third[i].start()

    def finish(i):
        weighted_ref[block(i), mine] = share[block(i)]
        third[i].wait_recv()
        weighted_ref[block(i), other] = rest[block(i)]
        back_ref[block(i), :] = lax.dot_general(
            weighted_ref[block(i), :],
            w_ref[...],
            (((1,), (1,)), ((), ())),
            preferred_element_type=jnp.float32,
        ).astype(jnp.bfloat16)

    for i in range(chunks):
        terms_of(i)
        first[i].start()
        if i > 0:
            send_pair(i - 1)
    send_pair(chunks - 1)
    for i in range(chunks):
        send_share(i)
        if i > 0:
            finish(i - 1)
    finish(chunks - 1)
    for one in first + second + third:
        one.wait_send()


def exchange(mixed, d_mixed, w_out, p_out, curvature):
    length, width = curvature.shape
    chunks = 4
    vmem = pl.BlockSpec(memory_space=pltpu.VMEM)
    half = pltpu.VMEM((length, width // 2), jnp.bfloat16)
    return pl.pallas_call(
        exchange_kernel,
        out_shape=(
            jax.ShapeDtypeStruct((length, width), jnp.bfloat16),
            jax.ShapeDtypeStruct(mixed.shape, jnp.bfloat16),
        ),
        in_specs=[vmem] * 5,
        out_specs=(vmem, vmem),
        scratch_shapes=[
            pltpu.VMEM((length, width), jnp.bfloat16),
            half,
            half,
            half,
            half,
            half,
            pltpu.SemaphoreType.DMA((3, chunks)),
            pltpu.SemaphoreType.DMA((3, chunks)),
        ],
        compiler_params=pltpu.CompilerParams(
            collective_id=2, has_side_effects=True, vmem_limit_bytes=VMEM_BYTES
        ),
    )(mixed, d_mixed, w_out, p_out, curvature)


def local(tokens, norm_gain, curvature, weight_slots, probe_slots, block_counts):
    n_columns = lax.axis_size("seq")
    n_owners = lax.axis_size("fsdp")
    q_heads = HQ // n_columns
    kv_heads = HK // n_columns
    row_blocks = D // BLK
    qkv_cols = (q_heads + 2 * kv_heads) * HD // BLK
    out_rows = q_heads * HD // BLK
    grid_qkv, grid_out = (row_blocks, qkv_cols), (out_rows, row_blocks)
    total_blocks = row_blocks * qkv_cols + out_rows * row_blocks
    slots = weight_slots.shape[1]
    length = tokens.shape[1]
    counts = block_counts[0]
    range_ends = jnp.cumsum(counts)
    starts = range_ends - counts
    owner_ids = jnp.arange(n_owners, dtype=jnp.int32)
    block_ids = jnp.arange(total_blocks, dtype=jnp.int32)
    owners = jnp.sum((range_ends[None, :] <= block_ids[:, None]).astype(jnp.int32), axis=1)
    first_block = jnp.sum(
        jnp.where(owners[:, None] == owner_ids[None, :], starts[None, :], 0), axis=1
    )
    slot_of = (owners * slots + block_ids - first_block).astype(jnp.int32)
    projected, d_projected, w_out, p_out, normed_t = gather_weights(
        slot_of,
        weight_slots[0],
        probe_slots[0],
        tokens[0],
        norm_gain[None, :],
        n_owners,
        grid_qkv,
        grid_out,
    )
    cosine, sine = rotary(length, HD)

    def inner(projected):
        return attention(projected, cosine, sine, q_heads, kv_heads)

    mixed, d_mixed = jax.jvp(inner, (projected,), (d_projected,))
    weighted, back_mixed = exchange(mixed, d_mixed, w_out, p_out, curvature[0])
    mixed_again, pullback = jax.vjp(inner, projected)
    (back_projected,) = pullback(back_mixed)
    slot_index = jnp.arange(n_owners * slots, dtype=jnp.int32)
    place = slot_index % slots
    owner_hot = (slot_index // slots)[:, None] == owner_ids[None, :]
    owner_first = jnp.sum(jnp.where(owner_hot, starts[None, :], 0), axis=1)
    own_count = jnp.sum(jnp.where(owner_hot, counts[None, :], 0), axis=1)
    picked = jnp.where(place < own_count, owner_first + place, total_blocks).astype(jnp.int32)
    scaled = reduce_slots(
        picked,
        normed_t,
        back_projected.astype(jnp.bfloat16),
        mixed_again.T,
        weighted,
        n_owners,
        (length * n_owners) ** -0.5,
        grid_qkv,
        grid_out,
    )
    return scaled.reshape(1, slots, BLK, BLK)


def spot():
    f = lax.axis_index("fsdp")
    s = lax.axis_index("seq")
    return lax.div(f, 2), lax.rem(f, 2), lax.div(s, 2), lax.rem(s, 2)


def device(z, y, x, c):
    return {"fsdp": 2 * z + y, "seq": 2 * x + c}


def mirrored(z, c, planes):
    return z + c * (planes - 1 - 2 * z)


def greet(peers):
    barrier = pltpu.get_barrier_semaphore()
    for peer in peers:
        pl.semaphore_signal(barrier, inc=1, device_id=peer, device_id_type=pl.DeviceIdType.MESH)
    pl.semaphore_wait(barrier, len(peers))


def shard_columns(x, j, width):
    return x * (width // 4) + j * (width // 8), width // 2 + j * (width // 4) + x * (width // 8)


def cut_count(slots):
    return 5 if slots % 5 == 0 else 1


def gather_grid_kernel(n, slots, grid_qkv, grid_out, slot_ref, w_ref, p_ref, tokens_ref, gain_ref,
                       curv_ref, proj_ref, d_proj_ref, wo_ref, po_ref, normed_t_ref, curv_out_ref,
                       held_w, held_p, matrix, normed, curv_part, send_y, send_core, send_z, recv, tok_send,
                       tok_recv, relay_send, relay_recv, curv_send, curv_recv):
    planes = n // 2
    z, y, x, c = spot()
    zeta = mirrored(z, c, planes)
    hub = lax.rem(zeta, 2) == 0
    spoke = lax.rem(zeta, 2) == 1
    mate = z + 1 - 2 * lax.rem(z, 2)
    y_peer = device(z, 1 - y, x, c)
    x_peer = device(z, y, 1 - x, c)
    core_peer = device(z, y, x, 1 - c)
    z_peer = device(mate, y, x, c)
    row = [device(lax.rem(z + i, planes), y, x, c) for i in range(1, planes)]
    greet(row + [core_peer, y_peer, x_peer])
    cuts = cut_count(slots)
    size = slots // cuts
    own = (w_ref, p_ref)
    held = (held_w, held_p)
    me = 2 * z + y
    tok_cuts = tok_send.shape[0]
    half = normed.shape[0] // 2
    tok_rows = half // tok_cuts
    width = normed.shape[1]
    part = width // 8

    def at(zeta_at):
        return mirrored(zeta_at, c, planes)

    def spread(which, d, j):
        return held[which].at[pl.ds(d * slots + j * size, size)]

    def move(src, which, d, j, peer, sem):
        return pltpu.make_async_remote_copy(
            src_ref=src,
            dst_ref=spread(which, d, j),
            send_sem=sem,
            recv_sem=recv.at[d, which * cuts + j],
            device_id=peer,
            device_id_type=pl.DeviceIdType.MESH,
        )

    def own_chunk(which, j):
        return own[which].at[pl.ds(j * size, size)]

    def arrive(which, d, j):
        move(spread(which, d, j), which, d, j, core_peer, send_y.at[0, 0]).wait_recv()

    other_hub = device(at(2 - zeta), y, x, c)
    near_hub = device(at(2), y, x, c)
    end_hub = device(at(0), y, x, c)

    def token_copy(i, rows_half, peer, s_sem, r_sem, src):
        rows = pl.ds(rows_half * half + i * tok_rows, tok_rows)
        return pltpu.make_async_remote_copy(
            src_ref=src.at[rows],
            dst_ref=normed.at[rows],
            send_sem=s_sem.at[i],
            recv_sem=r_sem.at[i],
            device_id=peer,
            device_id_type=pl.DeviceIdType.MESH,
        )

    def curv_copy(i):
        first = shard_columns(x, lax.rem(mate, 2), width)[i]
        return pltpu.make_async_remote_copy(
            src_ref=curv_ref.at[:, pl.ds(pl.multiple_of(first, part), part)],
            dst_ref=curv_part.at[i],
            send_sem=curv_send.at[i],
            recv_sem=curv_recv.at[i],
            device_id=z_peer,
            device_id_type=pl.DeviceIdType.MESH,
        )

    def curv_local(i):
        first = shard_columns(x, lax.rem(z, 2), width)[i]
        return pltpu.make_async_copy(
            curv_ref.at[:, pl.ds(pl.multiple_of(first, part), part)],
            curv_part.at[i],
            curv_recv.at[i],
        )

    def to_z(which, j):
        k = which * cuts + j
        return move(own_chunk(which, j), which, me, j, other_hub, send_z.at[0, k])

    def to_y(which, j):
        k = which * cuts + j
        return move(own_chunk(which, j), which, me, j, y_peer, send_y.at[0, k])

    def to_core(which, j):
        k = which * cuts + j
        return move(own_chunk(which, j), which, me, j, core_peer, send_core.at[0, k])

    def spoke_own(which, j):
        src = own_chunk(which, j)
        k = which * cuts + j
        return (
            move(src, which, me, j, near_hub, send_z.at[0, k]),
            move(src, which, me, j, end_hub, send_z.at[1, k]),
        )

    lead = min(2, 2 * cuts)
    every = [(which, j) for which in range(2) for j in range(cuts)]

    @pl.when(hub)
    def _():
        for k in range(lead):
            to_y(*every[k]).start()
        for k, one in enumerate(every):
            to_z(*one).start()
            if k < tok_cuts:
                token_copy(k, x, z_peer, tok_send, tok_recv, tokens_ref).start()
            to_core(*one).start()
        for k in range(len(every), tok_cuts):
            token_copy(k, x, z_peer, tok_send, tok_recv, tokens_ref).start()
        for i in range(2):
            curv_copy(i).start()
            curv_local(i).start()

    @pl.when(spoke)
    def _():
        for one in every:
            for copy in spoke_own(*one):
                copy.start()

    def pass_row(k):
        which, j = every[k]
        for r in range(1, planes):
            d = 2 * at(lax.rem(zeta + r, planes)) + y
            arrive(which, d, j)
            src = spread(which, d, j)
            move(src, which, d, j, y_peer, send_y.at[r, k]).start()
            move(src, which, d, j, core_peer, send_core.at[r, k]).start()
            if r == 1 and k + lead < len(every):
                to_y(*every[k + lead]).start()

    def pass_across(k):
        which, j = every[k]
        for r in range(planes):
            d = 2 * at(lax.rem(zeta + r, planes)) + 1 - y
            arrive(which, d, j)
            move(spread(which, d, j), which, d, j, core_peer, send_core.at[planes + r, k]).start()

    def forward(which, j):
        k = which * cuts + j
        pass_row(k)
        if k not in (0, cuts):
            pass_across(k - 1)
        if k in (cuts - 1, 2 * cuts - 1):
            pass_across(k)

    def step(which, j):
        @pl.when(hub)
        def _():
            forward(which, j)

        @pl.when(spoke)
        def _():
            for d in range(n):
                arrive(which, d, j)

    def normalize(source):
        rows = 32

        def some(i, carry):
            here = pl.ds(pl.multiple_of(i * rows, rows), rows)
            values = source[here, :].astype(jnp.float32)
            factor = lax.rsqrt(jnp.mean(values * values, axis=-1, keepdims=True) + EPS)
            normed[here, :] = (values * factor * gain_ref[...]).astype(jnp.bfloat16)
            return carry

        lax.fori_loop(0, normed.shape[0] // rows, some, 0)

    def transpose():
        edge = held_w.shape[-1]

        def some(i, carry):
            here = pl.ds(pl.multiple_of(i * edge, edge), edge)
            normed_t_ref[here, :] = normed[:, here].T
            return carry

        lax.fori_loop(0, normed.shape[1] // edge, some, 0)

    def project(result_ref):
        rows = 256

        def some(i, carry):
            here = pl.ds(pl.multiple_of(i * rows, rows), rows)
            result_ref[here, :] = jnp.dot(
                normed[here, :], matrix[...], preferred_element_type=jnp.float32
            )
            return carry

        lax.fori_loop(0, normed.shape[0] // rows, some, 0)

    def unpack_qkv(which):
        rows, cols = grid_qkv
        edge = held_w.shape[-1]

        def qkv_row(i, carry):
            for col in range(cols):
                matrix[pl.ds(pl.multiple_of(i * edge, edge), edge), col * edge:(col + 1) * edge] = (
                    held[which][slot_ref[i * cols + col]]
                )
            return carry

        lax.fori_loop(0, rows, qkv_row, 0)

    def unpack_out(which, out_ref):
        rows, cols = grid_qkv
        out_rows, out_cols = grid_out
        edge = held_w.shape[-1]

        def out_col(i, carry):
            for r in range(out_rows):
                out_ref[r * edge:(r + 1) * edge, pl.ds(pl.multiple_of(i * edge, edge), edge)] = (
                    held[which][slot_ref[rows * cols + r * out_cols + i]]
                )
            return carry

        lax.fori_loop(0, out_cols, out_col, 0)

    def keep_own(which):
        @pl.when(hub)
        def _():
            held[which][pl.ds(me * slots, slots)] = own[which][...]

    @pl.when(hub)
    def _():
        normalize(tokens_ref)

    @pl.when(spoke)
    def _():
        for i in range(tok_cuts):
            token_copy(i, x, z_peer, tok_send, tok_recv, normed).wait_recv()
            token_copy(i, x, x_peer, relay_send, relay_recv, normed).start()
        for i in range(tok_cuts):
            token_copy(i, 1 - x, x_peer, relay_send, relay_recv, normed).wait_recv()
        for i in range(tok_cuts):
            token_copy(i, x, x_peer, relay_send, relay_recv, normed).wait_send()
        normalize(normed)

    for j in range(cuts):
        step(0, j)
        if j == 0:
            transpose()
    keep_own(0)
    todo = [
        lambda: unpack_qkv(0),
        lambda: project(proj_ref),
        lambda: unpack_out(0, wo_ref),
    ]
    for j in range(cuts):
        step(1, j)
        if j < cuts - 1 and todo:
            todo.pop(0)()
    while todo:
        todo.pop(0)()
    keep_own(1)
    unpack_qkv(1)
    project(d_proj_ref)
    unpack_out(1, po_ref)

    @pl.when(hub)
    def _():
        for i in range(2):
            curv_local(i).wait()

    @pl.when(spoke)
    def _():
        for i in range(2):
            curv_copy(i).wait_recv()

    curv_out_ref[...] = curv_part[...]

    @pl.when(hub)
    def _():
        for i in range(tok_cuts):
            token_copy(i, x, z_peer, tok_send, tok_recv, tokens_ref).wait_send()
        for i in range(2):
            curv_copy(i).wait_send()
        for k, (which, j) in enumerate(every):
            to_z(which, j).wait_send()
            to_y(which, j).wait_send()
            to_core(which, j).wait_send()
            src = spread(which, me, j)
            for r in range(1, planes):
                move(src, which, me, j, y_peer, send_y.at[r, k]).wait_send()
            for r in range(1, n):
                move(src, which, me, j, core_peer, send_core.at[r, k]).wait_send()

    @pl.when(spoke)
    def _():
        for one in every:
            for copy in spoke_own(*one):
                copy.wait_send()


def gather_grid(slot_of, weights, probes, tokens, gain, curvature, n, grid_qkv, grid_out):
    slots, edge, _ = weights.shape
    cuts = cut_count(slots)
    length, width = tokens.shape
    proj = jax.ShapeDtypeStruct((length, grid_qkv[1] * edge), jnp.float32)
    turned = jax.ShapeDtypeStruct((width, length), jnp.bfloat16)
    out = jax.ShapeDtypeStruct((grid_out[0] * edge, grid_out[1] * edge), jnp.bfloat16)
    shard = (2, length, width // 8)
    vmem = pl.BlockSpec(memory_space=pltpu.VMEM)
    dma = pltpu.SemaphoreType.DMA
    return pl.pallas_call(
        functools.partial(gather_grid_kernel, n, slots, grid_qkv, grid_out),
        out_shape=(proj, proj, out, out, turned, jax.ShapeDtypeStruct(shard, jnp.bfloat16)),
        in_specs=[pl.BlockSpec(memory_space=pltpu.SMEM)] + [vmem] * 4
        + [pl.BlockSpec(memory_space=pl.ANY)],
        out_specs=(vmem,) * 6,
        scratch_shapes=[
            pltpu.VMEM((n * slots, edge, edge), jnp.bfloat16),
            pltpu.VMEM((n * slots, edge, edge), jnp.bfloat16),
            pltpu.VMEM((grid_qkv[0] * edge, grid_qkv[1] * edge), jnp.bfloat16),
            pltpu.VMEM((length, width), jnp.bfloat16),
            pltpu.VMEM(shard, jnp.bfloat16),
            dma((n // 2, 2 * cuts)),
            dma((n, 2 * cuts)),
            dma((2, 2 * cuts)),
            dma((n, 2 * cuts)),
            dma((4,)),
            dma((4,)),
            dma((4,)),
            dma((4,)),
            dma((2,)),
            dma((2,)),
        ],
        compiler_params=pltpu.CompilerParams(
            collective_id=3, has_side_effects=True, vmem_limit_bytes=GRID_VMEM_BYTES
        ),
    )(slot_of, weights, probes, tokens, gain, curvature)


def turn_tables(length, head_dim):
    cosine, sine = rotary(length, head_dim)
    cosine, sine = cosine[:, 0, :], sine[:, 0, :]
    return jnp.concatenate([cosine, cosine], axis=1), jnp.concatenate([-sine, sine], axis=1)


def turn(values, cosine, sine):
    return values * cosine + pltpu.roll(values, values.shape[1] // 2, 1) * sine


def attend(heads, proj_ref, d_proj_ref, cos_ref, sin_ref, mixed_ref, d_mixed_ref, mixed_t_ref,
           probs_ref, rot_ref, d_rot):
    length = proj_ref.shape[0]
    hd = cos_ref.shape[1]
    key_at = heads * hd
    val_at = key_at + hd
    scale = hd ** -0.5

    def spin(source, target):
        def some(h, carry):
            here = pl.ds(pl.multiple_of(h * hd, hd), hd)
            target[:, here] = turn(source[:, here], cos_ref[...], sin_ref[...]).astype(jnp.bfloat16)
            return carry

        lax.fori_loop(0, heads + 1, some, 0)
        target[:, val_at:] = source[:, val_at:].astype(jnp.bfloat16)

    spin(proj_ref, rot_ref)
    spin(d_proj_ref, d_rot)
    tile = hd

    def head(h, carry):
        here = pl.ds(pl.multiple_of(h * hd, hd), hd)
        for i in range(length // tile):
            rows = slice(i * tile, (i + 1) * tile)
            span = (i + 1) * tile
            q, dq = rot_ref[rows, here], d_rot[rows, here]
            k, dk = rot_ref[:span, key_at:val_at], d_rot[:span, key_at:val_at]
            v, dv = rot_ref[:span, val_at:], d_rot[:span, val_at:]
            contract = (((1,), (1,)), ((), ()))
            scores = lax.dot_general(q, k, contract, preferred_element_type=jnp.float32) * scale
            slopes = lax.dot_general(
                jnp.concatenate([dq, q], axis=1),
                jnp.concatenate([k, dk], axis=1),
                contract,
                preferred_element_type=jnp.float32,
            ) * scale
            at_row = i * tile + lax.broadcasted_iota(jnp.int32, (tile, span), 0)
            at_col = lax.broadcasted_iota(jnp.int32, (tile, span), 1)
            seen = at_row >= at_col
            scores = jnp.where(seen, scores, NEGATIVE)
            slopes = jnp.where(seen, slopes, 0.0)
            raised = jnp.exp(scores - jnp.max(scores, axis=1, keepdims=True))
            probs = raised / jnp.sum(raised, axis=1, keepdims=True)
            d_probs = probs * (slopes - jnp.sum(probs * slopes, axis=1, keepdims=True))
            probs = probs.astype(jnp.bfloat16)
            d_probs = d_probs.astype(jnp.bfloat16)
            probs_ref[h, rows, :span] = probs
            if span < length:
                probs_ref[h, rows, span:] = jnp.zeros((tile, length - span), jnp.bfloat16)
            mixed = jnp.dot(probs, v, preferred_element_type=jnp.float32).astype(jnp.bfloat16)
            mixed_ref[rows, here] = mixed
            mixed_t_ref[here, rows] = mixed.T
            d_mixed_ref[rows, here] = (
                jnp.dot(d_probs, v, preferred_element_type=jnp.float32)
                + jnp.dot(probs, dv, preferred_element_type=jnp.float32)
            ).astype(jnp.bfloat16)
        return carry

    lax.fori_loop(0, heads, head, 0)


def attend_back(heads, back_ref, probs_ref, rot_ref, cos_ref, sin_ref, out_ref, slope_ref):
    length = back_ref.shape[0]
    hd = cos_ref.shape[1]
    key_at = heads * hd
    val_at = key_at + hd
    scale = hd ** -0.5
    tile = hd

    def unturn(values):
        rounded = values.astype(jnp.bfloat16).astype(jnp.float32)
        return turn(rounded, cos_ref[...], -sin_ref[...]).astype(jnp.bfloat16)

    def head(h, totals):
        here = pl.ds(pl.multiple_of(h * hd, hd), hd)
        key_total, val_total = totals
        for i in range(length // tile):
            rows = slice(i * tile, (i + 1) * tile)
            span = (i + 1) * tile
            back = back_ref[rows, here]
            d_probs = lax.dot_general(
                back, rot_ref[:span, val_at:], (((1,), (1,)), ((), ())),
                preferred_element_type=jnp.float32,
            ).astype(jnp.bfloat16).astype(jnp.float32)
            probs = probs_ref[h, rows, :span].astype(jnp.float32)
            slopes = probs * (d_probs - jnp.sum(probs * d_probs, axis=1, keepdims=True)) * scale
            slope_ref[rows, :span] = slopes.astype(jnp.bfloat16)
            if span < length:
                slope_ref[rows, span:] = jnp.zeros((tile, length - span), jnp.bfloat16)
        slopes = slope_ref[...]
        d_query = jnp.dot(slopes, rot_ref[:, key_at:val_at], preferred_element_type=jnp.float32)
        out_ref[:, here] = unturn(d_query)
        first = (((0,), (0,)), ((), ()))
        key_total = key_total + lax.dot_general(
            rot_ref[:, here], slopes, first, preferred_element_type=jnp.float32
        )
        val_total = val_total + lax.dot_general(
            back_ref[:, here], probs_ref[h], first, preferred_element_type=jnp.float32
        )
        return key_total, val_total

    zero = jnp.zeros((hd, length), jnp.float32)
    key_total, val_total = lax.fori_loop(0, heads, head, (zero, zero))
    out_ref[:, key_at:val_at] = unturn(key_total.T)
    out_ref[:, val_at:] = val_total.T.astype(jnp.bfloat16)


def square_kernel(heads, proj_ref, d_proj_ref, w_out, p_out, curv_ref, cos_ref, sin_ref,
                  weighted_ref, back_proj_ref, mixed_t_ref, w_ref, p_ref, mixed_ref, d_mixed_ref,
                  probs, rot, d_rot, slope, back_ref, terms, near_x, near_z, pair_a, pair_b, far_z,
                  far_x, full, load_sem, send_sem, recv_sem):
    z, y, x, c = spot()
    side = lax.rem(z, 2)
    x_peer = device(z, y, 1 - x, c)
    z_peer = device(z + 1 - 2 * side, y, x, c)
    loads = [
        pltpu.make_async_copy(w_out, w_ref, load_sem.at[0]),
        pltpu.make_async_copy(p_out, p_ref, load_sem.at[1]),
    ]
    for load in loads:
        load.start()
    greet([x_peer, z_peer])
    attend(
        heads, proj_ref, d_proj_ref, cos_ref, sin_ref, mixed_ref, d_mixed_ref, mixed_t_ref, probs,
        rot, d_rot,
    )
    for load in loads:
        load.wait()
    length, width = terms.shape
    quarter, part = width // 4, width // 8
    chunks = recv_sem.shape[1]
    rows = length // chunks

    def block(i):
        return pl.ds(i * rows, rows)

    def cols(first, count):
        return pl.ds(pl.multiple_of(first, count), count)

    keep_a, give_a = cols(x * quarter, quarter), cols((1 - x) * quarter, quarter)
    keep_b = cols(width // 2 + side * quarter, quarter)
    give_b = cols(width // 2 + (1 - side) * quarter, quarter)
    first_a, first_b = shard_columns(x, side, width)
    own_a, own_b = cols(first_a, part), cols(first_b, part)

    def copy(kind, i, here, there, target):
        return pltpu.make_async_remote_copy(
            src_ref=here,
            dst_ref=there,
            send_sem=send_sem.at[kind, i],
            recv_sem=recv_sem.at[kind, i],
            device_id=target,
            device_id_type=pl.DeviceIdType.MESH,
        )

    def stage(i):
        b = block(i)
        return (
            copy(0, i, terms.at[b, give_a], near_x.at[b], x_peer),
            copy(1, i, terms.at[b, give_b], near_z.at[b], z_peer),
            copy(2, i, pair_a.at[b, cols((1 - side) * part, part)], far_z.at[b], z_peer),
            copy(3, i, pair_b.at[b, cols((1 - x) * part, part)], far_x.at[b], x_peer),
            copy(4, i, full.at[b, own_a], full.at[b, own_a], z_peer),
            copy(5, i, full.at[b, own_b], full.at[b, own_b], x_peer),
            copy(6, i, full.at[b, keep_a], full.at[b, keep_a], x_peer),
            copy(7, i, full.at[b, keep_b], full.at[b, keep_b], z_peer),
        )

    def incoming(kind, i, there):
        copy(kind, i, there, there, x_peer).wait_recv()

    def terms_of(i):
        tile = width // 4

        def columns(j, carry):
            here = pl.ds(pl.multiple_of(j * tile, tile), tile)
            terms[block(i), here] = (
                jnp.dot(d_mixed_ref[block(i), :], w_ref[:, here], preferred_element_type=jnp.float32)
                + jnp.dot(mixed_ref[block(i), :], p_ref[:, here], preferred_element_type=jnp.float32)
            ).astype(jnp.bfloat16)
            return carry

        lax.fori_loop(0, 4, columns, 0)

    plans = [stage(i) for i in range(chunks)]

    def pair_up(i):
        b = block(i)
        for kind, pair, keep, near in ((0, pair_a, keep_a, near_x), (1, pair_b, keep_b, near_z)):
            incoming(kind, i, near.at[b])
            pair[b] = (
                terms[b, keep].astype(jnp.float32) + near[b].astype(jnp.float32)
            ).astype(jnp.bfloat16)
            plans[i][2 + kind].start()

    def weigh(i):
        b = block(i)
        for kind, pair, mine, far, own_cols in (
            (0, pair_a, side, far_z, own_a), (1, pair_b, x, far_x, own_b)
        ):
            incoming(2 + kind, i, far.at[b])
            total = pair[b, cols(mine * part, part)].astype(jnp.float32) + far[b].astype(jnp.float32)
            full[b, own_cols] = (curv_ref[kind, b].astype(jnp.float32) * total).astype(jnp.bfloat16)
            plans[i][4 + kind].start()

    def widen(i):
        b = block(i)
        other_a, other_b = shard_columns(x, 1 - side, width)[0], shard_columns(1 - x, side, width)[1]
        incoming(4, i, full.at[b, cols(other_a, part)])
        plans[i][6].start()
        incoming(5, i, full.at[b, cols(other_b, part)])
        plans[i][7].start()

    def finish(i):
        b = block(i)
        incoming(6, i, full.at[b, give_a])
        incoming(7, i, full.at[b, give_b])
        weighted_ref[b, :] = full[b, :]
        back_ref[b, :] = lax.dot_general(
            full[b, :], w_ref[...], (((1,), (1,)), ((), ())), preferred_element_type=jnp.float32
        ).astype(jnp.bfloat16)

    for i in range(chunks + 3):
        if i < chunks:
            terms_of(i)
            plans[i][0].start()
            plans[i][1].start()
        if 0 <= i - 1 < chunks:
            pair_up(i - 1)
        if 0 <= i - 2 < chunks:
            weigh(i - 2)
        if 0 <= i - 3 < chunks:
            widen(i - 3)
    for i in range(chunks):
        finish(i)
    attend_back(heads, back_ref, probs, rot, cos_ref, sin_ref, back_proj_ref, slope)
    for plan in plans:
        for one in plan:
            one.wait_send()


def square_exchange(projected, d_projected, w_out, p_out, curvature, cosine, sine, heads):
    length, inputs = projected.shape
    inner, width = w_out.shape
    chunks = 4
    half = jnp.bfloat16
    vmem = pl.BlockSpec(memory_space=pltpu.VMEM)
    anywhere = pl.BlockSpec(memory_space=pl.ANY)
    quarter = pltpu.VMEM((length, width // 4), half)
    part = pltpu.VMEM((length, width // 8), half)
    whole = pltpu.VMEM((length, width), half)
    narrow = pltpu.VMEM((length, inner), half)
    return pl.pallas_call(
        functools.partial(square_kernel, heads),
        out_shape=(
            jax.ShapeDtypeStruct((length, width), half),
            jax.ShapeDtypeStruct((length, inputs), half),
            jax.ShapeDtypeStruct((inner, length), half),
        ),
        in_specs=[vmem] * 2 + [anywhere] * 2 + [vmem] * 3,
        out_specs=(vmem,) * 3,
        scratch_shapes=[
            pltpu.VMEM((inner, width), half),
            pltpu.VMEM((inner, width), half),
            narrow,
            narrow,
            pltpu.VMEM((heads, length, length), half),
            pltpu.VMEM((length, inputs), half),
            pltpu.VMEM((length, inputs), half),
            pltpu.VMEM((length, length), half),
            narrow,
            whole, quarter, quarter, quarter, quarter, part, part, whole,
            pltpu.SemaphoreType.DMA((2,)),
            pltpu.SemaphoreType.DMA((8, chunks)),
            pltpu.SemaphoreType.DMA((8, chunks)),
        ],
        compiler_params=pltpu.CompilerParams(
            collective_id=4, has_side_effects=True, vmem_limit_bytes=GRID_VMEM_BYTES
        ),
    )(projected, d_projected, w_out, p_out, curvature, cosine, sine)


def reduce_grid_kernel(n, slots, scale, grid_qkv, grid_out, pick_ref, normed_t_ref, d_proj_ref,
                       mixed_t_ref, weighted_ref, out_ref, grads, peer, begin, across, onward,
                       landed, core_send, core_recv, y_send, y_recv, z_send, z_recv):
    planes = n // 2
    z, y, x, c = spot()
    zeta = mirrored(z, c, planes)
    hub = lax.rem(zeta, 2) == 0
    spoke = lax.rem(zeta, 2) == 1
    late = lax.div(zeta, 2)
    y_peer = device(z, 1 - y, x, c)
    core_peer = device(z, y, x, 1 - c)
    row = [device(lax.rem(z + i, planes), y, x, c) for i in range(1, planes)]
    greet(row + [core_peer, y_peer])
    cuts = cut_count(slots)
    size = slots // cuts
    rows, cols = grid_qkv
    out_rows, out_cols = grid_out
    total = rows * cols + out_rows * out_cols
    edge = out_ref.shape[-1]
    legs = core_send.shape[0] - 1
    leg_rows = rows // legs
    group = 2

    def core_copy(i):
        if i == legs:
            here = pl.ds(rows * cols, out_rows * out_cols)
        else:
            here = pl.ds(i * leg_rows * cols, leg_rows * cols)
        return pltpu.make_async_remote_copy(
            src_ref=grads.at[here],
            dst_ref=peer.at[here],
            send_sem=core_send.at[i],
            recv_sem=core_recv.at[i],
            device_id=core_peer,
            device_id_type=pl.DeviceIdType.MESH,
        )

    def out_columns(i, carry):
        width = group * edge
        right = weighted_ref[:, pl.ds(pl.multiple_of(i * width, width), width)]
        block = jnp.dot(
            mixed_t_ref[...], right, preferred_element_type=jnp.float32
        ).astype(jnp.bfloat16)
        for r in range(out_rows):
            for k in range(group):
                grads[rows * cols + r * out_cols + i * group + k] = block[
                    r * edge:(r + 1) * edge, k * edge:(k + 1) * edge
                ]
        return carry

    def qkv_rows(i, carry):
        width = group * edge
        left = normed_t_ref[pl.ds(pl.multiple_of(i * width, width), width), :]
        block = jnp.dot(
            left, d_proj_ref[...], preferred_element_type=jnp.float32
        ).astype(jnp.bfloat16)
        for r in range(group):
            for k in range(cols):
                grads[(i * group + r) * cols + k] = block[
                    r * edge:(r + 1) * edge, k * edge:(k + 1) * edge
                ]
        return carry

    def hand_over(i):
        @pl.when(spoke)
        def _():
            core_copy(i).start()

    grads[total] = jnp.zeros((edge, edge), grads.dtype)
    peer[total] = jnp.zeros((edge, edge), peer.dtype)
    lax.fori_loop(0, out_cols // group, out_columns, 0)
    hand_over(legs)
    for i in range(legs):
        steps = leg_rows // group
        lax.fori_loop(i * steps, (i + 1) * steps, qkv_rows, 0)
        hand_over(i)

    def owner(i, at_y):
        first = (3, 2, 1, 0)[i]
        second = (0, 1, 3, 2)[i]
        o = (1 - late) * first + late * second
        return 2 * mirrored(o, c, planes) + at_y

    def both(index):
        return grads[index].astype(jnp.float32) + peer[index].astype(jnp.float32)

    def y_copy(i, j):
        here = pl.ds(i * slots + j * size, size)
        return pltpu.make_async_remote_copy(
            src_ref=begin.at[here],
            dst_ref=across.at[here],
            send_sem=y_send.at[i, j],
            recv_sem=y_recv.at[i, j],
            device_id=y_peer,
            device_id_type=pl.DeviceIdType.MESH,
        )

    def z_copy(i, j):
        goal = (1 - late) * (2, 2, 1)[i] + late * (0, 1, 3)[i]
        buffer = (0, 1, 0)[i]
        return pltpu.make_async_remote_copy(
            src_ref=onward.at[i, pl.ds(j * size, size)],
            dst_ref=landed.at[buffer, pl.ds(j * size, size)],
            send_sem=z_send.at[i, j],
            recv_sem=z_recv.at[buffer, j],
            device_id=device(mirrored(goal, c, planes), y, x, c),
            device_id_type=pl.DeviceIdType.MESH,
        )

    def z_wait(buffer, j):
        here = landed.at[buffer, pl.ds(j * size, size)]
        pltpu.make_async_remote_copy(
            src_ref=here,
            dst_ref=here,
            send_sem=z_send.at[0, j],
            recv_sem=z_recv.at[buffer, j],
            device_id=core_peer,
            device_id_type=pl.DeviceIdType.MESH,
        ).wait_recv()

    def each(j, body):
        def some(t, carry):
            body(j * size + t)
            return carry

        lax.fori_loop(0, size, some, 0)

    @pl.when(hub)
    def _():
        for i in (legs,) + tuple(range(legs)):
            core_copy(i).wait_recv()
        for i in range(planes):
            base = owner(i, 1 - y) * slots

            def start(j, carry, i=i, base=base):
                def fill(t):
                    begin[i * slots + t] = both(pick_ref[base + t]).astype(jnp.bfloat16)

                each(j, fill)
                y_copy(i, j).start()
                return carry

            lax.fori_loop(0, cuts, start, 0)
        for i in range(planes):
            base = owner(i, y) * slots

            def value(t, i=i, base=base):
                return both(pick_ref[base + t]) + across[i * slots + t].astype(jnp.float32)

            def go(j, carry, i=i, value=value):
                y_copy(i, j).wait_recv()
                if i < 2:

                    def pass_on(t):
                        onward[i, t] = value(t).astype(jnp.bfloat16)

                    each(j, pass_on)
                    z_copy(i, j).start()
                elif i == 2:

                    @pl.when(late == 0)
                    def _():
                        def pass_on(t):
                            onward[i, t] = value(t).astype(jnp.bfloat16)

                        each(j, pass_on)

                    @pl.when(late == 1)
                    def _():
                        z_wait(0, j)

                        def pass_on(t):
                            onward[i, t] = (
                                value(t) + landed[0, t].astype(jnp.float32)
                            ).astype(jnp.bfloat16)

                        each(j, pass_on)

                    z_copy(i, j).start()
                else:
                    z_wait(late, j)

                    def last(t):
                        out_ref[t] = (value(t) + landed[late, t].astype(jnp.float32)) * scale

                    each(j, last)
                return carry

            lax.fori_loop(0, cuts, go, 0)

        def close(j, carry):
            for i in range(planes):
                y_copy(i, j).wait_send()
            for i in range(3):
                z_copy(i, j).wait_send()
            return carry

        lax.fori_loop(0, cuts, close, 0)

    @pl.when(spoke)
    def _():
        @pl.when(zeta == 1)
        def _():
            def go(j, carry):
                z_wait(0, j)
                z_wait(1, j)

                def last(t):
                    out_ref[t] = (
                        landed[0, t].astype(jnp.float32) + landed[1, t].astype(jnp.float32)
                    ) * scale

                each(j, last)
                return carry

            lax.fori_loop(0, cuts, go, 0)

        @pl.when(zeta == 3)
        def _():
            def go(j, carry):
                z_wait(0, j)

                def last(t):
                    out_ref[t] = landed[0, t].astype(jnp.float32) * scale

                each(j, last)
                return carry

            lax.fori_loop(0, cuts, go, 0)

        for i in range(legs + 1):
            core_copy(i).wait_send()


def reduce_grid(picked, normed_t, d_proj, mixed_t, weighted, n, scale, grid_qkv, grid_out):
    slots = picked.shape[0] // n
    edge = BLK
    total_blocks = grid_qkv[0] * grid_qkv[1] + grid_out[0] * grid_out[1]
    cuts = cut_count(slots)
    legs = 4
    vmem = pl.BlockSpec(memory_space=pltpu.VMEM)
    dma = pltpu.SemaphoreType.DMA
    return pl.pallas_call(
        functools.partial(reduce_grid_kernel, n, slots, scale, grid_qkv, grid_out),
        out_shape=jax.ShapeDtypeStruct((slots, edge, edge), jnp.float32),
        in_specs=[pl.BlockSpec(memory_space=pltpu.SMEM)] + [vmem] * 4,
        out_specs=vmem,
        scratch_shapes=[
            pltpu.VMEM((total_blocks + 1, edge, edge), jnp.bfloat16),
            pltpu.VMEM((total_blocks + 1, edge, edge), jnp.bfloat16),
            pltpu.VMEM((n // 2 * slots, edge, edge), jnp.bfloat16),
            pltpu.VMEM((n // 2 * slots, edge, edge), jnp.bfloat16),
            pltpu.VMEM((3, slots, edge, edge), jnp.bfloat16),
            pltpu.VMEM((2, slots, edge, edge), jnp.bfloat16),
            dma((legs + 1,)),
            dma((legs + 1,)),
            dma((n // 2, cuts)),
            dma((n // 2, cuts)),
            dma((3, cuts)),
            dma((2, cuts)),
        ],
        compiler_params=pltpu.CompilerParams(
            collective_id=5, has_side_effects=True, vmem_limit_bytes=GRID_VMEM_BYTES
        ),
    )(picked, normed_t, d_proj, mixed_t, weighted)


def local_grid(tokens, norm_gain, curvature, weight_slots, probe_slots, block_counts):
    n_columns = lax.axis_size("seq")
    n_owners = lax.axis_size("fsdp")
    q_heads = HQ // n_columns
    kv_heads = HK // n_columns
    row_blocks = D // BLK
    qkv_cols = (q_heads + 2 * kv_heads) * HD // BLK
    out_rows = q_heads * HD // BLK
    grid_qkv, grid_out = (row_blocks, qkv_cols), (out_rows, row_blocks)
    total_blocks = row_blocks * qkv_cols + out_rows * row_blocks
    slots = weight_slots.shape[1]
    length = tokens.shape[1]
    z, _, _, c = spot()
    theirs = lax.ppermute(block_counts, "seq", [(i, i ^ 1) for i in range(n_columns)])
    counts = jnp.where(lax.rem(z, 2) == c, block_counts, theirs)[0]
    range_ends = jnp.cumsum(counts)
    starts = range_ends - counts
    owner_ids = jnp.arange(n_owners, dtype=jnp.int32)
    block_ids = jnp.arange(total_blocks, dtype=jnp.int32)
    owners = jnp.sum((range_ends[None, :] <= block_ids[:, None]).astype(jnp.int32), axis=1)
    first_block = jnp.sum(
        jnp.where(owners[:, None] == owner_ids[None, :], starts[None, :], 0), axis=1
    )
    slot_of = (owners * slots + block_ids - first_block).astype(jnp.int32)
    projected, d_projected, w_out, p_out, normed_t, curv_part = gather_grid(
        slot_of,
        weight_slots[0],
        probe_slots[0],
        tokens[0],
        norm_gain[None, :],
        curvature[0],
        n_owners,
        grid_qkv,
        grid_out,
    )
    cosine, sine = turn_tables(length, HD)
    weighted, back_projected, mixed_t = square_exchange(
        projected, d_projected, w_out, p_out, curv_part, cosine, sine, q_heads
    )
    slot_index = jnp.arange(n_owners * slots, dtype=jnp.int32)
    place = slot_index % slots
    owner_hot = (slot_index // slots)[:, None] == owner_ids[None, :]
    owner_first = jnp.sum(jnp.where(owner_hot, starts[None, :], 0), axis=1)
    own_count = jnp.sum(jnp.where(owner_hot, counts[None, :], 0), axis=1)
    picked = jnp.where(place < own_count, owner_first + place, total_blocks).astype(jnp.int32)
    scaled = reduce_grid(
        picked,
        normed_t,
        back_projected,
        mixed_t,
        weighted,
        n_owners,
        (length * n_owners) ** -0.5,
        grid_qkv,
        grid_out,
    )
    return scaled.reshape(1, slots, BLK, BLK)


def solution(mesh):
    in_specs = (
        P("fsdp", None, None),
        P(),
        P("fsdp", None, None),
        P("seq", "fsdp", None, None),
        P("seq", "fsdp", None, None),
        P("seq", None),
    )
    out_specs = P("seq", "fsdp", None, None)
    body = local_grid if mesh.shape["fsdp"] == 8 and mesh.shape["seq"] == 4 else local
    return jax.shard_map(body, mesh=mesh, in_specs=in_specs, out_specs=out_specs, check_vma=False)
```

```python
import functools

import jax
import jax.numpy as jnp
from jax import lax
from jax.experimental import pallas as pl
from jax.experimental.pallas import tpu as pltpu
from jax.sharding import PartitionSpec as P

D = 4096
HQ = 16
HK = 4
HD = 128
BLK = 128


THETA = 500000.0
EPS = 1e-05
NEGATIVE = -1e30


def rotary(length, head_dim):
    half_dim = head_dim // 2
    frequency = jnp.exp(-jnp.log(THETA) * 2.0 * jnp.arange(half_dim, dtype=jnp.float32) / head_dim)
    angles = jnp.arange(length, dtype=jnp.float32)[:, None] * frequency[None, :]
    return (jnp.cos(angles)[:, None, :], jnp.sin(angles)[:, None, :])


def rotate(field_in, cosine, sine):
    half_dim = field_in.shape[-1] // 2
    first_half = field_in[..., :half_dim]
    second = field_in[..., half_dim:]
    return jnp.concatenate(
        [first_half * cosine - second * sine, second * cosine + first_half * sine], axis=-1
    )


VMEM_BYTES = 62 * 1024 * 1024
GRID_VMEM_BYTES = 67043328


def attention(projected, cosine, sine, q_heads, kv_heads):
    length = projected.shape[0]
    head_dim = projected.shape[1] // (q_heads + 2 * kv_heads)
    q_end = q_heads * head_dim
    k_end = q_end + kv_heads * head_dim
    queries = rotate(projected[:, :q_end].reshape(length, q_heads, head_dim), cosine, sine).astype(
        jnp.bfloat16
    )
    key_rows = rotate(
        projected[:, q_end:k_end].reshape(length, kv_heads, head_dim), cosine, sine
    ).astype(jnp.bfloat16)
    values = projected[:, k_end:].reshape(length, kv_heads, head_dim).astype(jnp.bfloat16)
    queries = queries.reshape(length, kv_heads, q_heads // kv_heads, head_dim)
    scores = jnp.einsum(
        "qkgd,skd->kgqs", queries, key_rows, preferred_element_type=jnp.float32
    ) * head_dim ** (-0.5)
    causal = jnp.arange(length)[:, None] >= jnp.arange(length)[None, :]
    scores = jnp.where(causal, scores, NEGATIVE)
    attn_probs = jax.nn.softmax(scores, axis=-1).astype(jnp.bfloat16)
    mixed_heads = jnp.einsum(
        "kgqs,skd->qkgd", attn_probs, values, preferred_element_type=jnp.float32
    )
    return mixed_heads.reshape(length, q_heads * head_dim).astype(jnp.bfloat16)


def ring_position(index, n):
    odd = lax.rem(index, 2)
    half = lax.div(index, 2)
    return (1 - odd) * half + odd * (n - 1 - half)


def ring_index(position, n):
    back = lax.div(position, n // 2)
    return (1 - back) * 2 * position + back * (2 * (n - 1 - position) + 1)


def pieces(slots):
    half = slots // 2
    out = []
    for direction, first, count in ((0, 0, half), (1, half, slots - half)):
        cuts = 5 if count % 5 == 0 else 1
        size = count // cuts
        out.append([(first + i * size, size) for i in range(cuts)])
    return out


def enter(neighbours, axis="fsdp"):
    barrier = pltpu.get_barrier_semaphore()
    for neighbour in neighbours:
        pl.semaphore_signal(
            barrier, inc=1, device_id={axis: neighbour}, device_id_type=pl.DeviceIdType.MESH
        )
    pl.semaphore_wait(barrier, len(neighbours))


def gather_kernel(n, slots, grid_qkv, grid_out, slot_ref, w_ref, p_ref, tokens_ref, gain_ref,
                  proj_ref, d_proj_ref, wo_ref, po_ref, normed_t_ref, held_w, held_p, matrix,
                  normed, send_sem, recv_sem):
    me = lax.axis_index("fsdp")
    pos = ring_position(me, n)
    right = ring_index(lax.rem(pos + 1, n), n)
    left = ring_index(lax.rem(pos + n - 1, n), n)
    towards = (right, left)
    enter((left, right))
    parts = pieces(slots)
    arrays = ((w_ref, held_w), (p_ref, held_p))

    def copy(which, step, direction, j):
        own, held = arrays[which]
        first, size = parts[direction][j]
        shift = n - step if direction == 0 else step
        origin = ring_index(lax.rem(pos + shift, n), n)
        there = held.at[pl.ds(origin * slots + first, size)]
        here = own.at[pl.ds(first, size)] if step == 0 else there
        return pltpu.make_async_remote_copy(
            src_ref=here,
            dst_ref=there,
            send_sem=send_sem.at[which, step, direction, j],
            recv_sem=recv_sem.at[which, step, direction, j],
            device_id={"fsdp": towards[direction]},
            device_id_type=pl.DeviceIdType.MESH,
        )

    def arrival(which, step, direction, j):
        first, size = parts[direction][j]
        own, held = arrays[which]
        shift = n - step - 1 if direction == 0 else step + 1
        origin = ring_index(lax.rem(pos + shift, n), n)
        there = held.at[pl.ds(origin * slots + first, size)]
        pltpu.make_async_remote_copy(
            src_ref=there,
            dst_ref=there,
            send_sem=send_sem.at[which, step, direction, j],
            recv_sem=recv_sem.at[which, step, direction, j],
            device_id={"fsdp": towards[direction]},
            device_id_type=pl.DeviceIdType.MESH,
        ).wait_recv()

    def each():
        for j in range(max(len(parts[0]), len(parts[1]))):
            for direction in range(2):
                if j < len(parts[direction]):
                    yield direction, j

    def normalize():
        rows = 32

        def some(i, carry):
            here = pl.ds(pl.multiple_of(i * rows, rows), rows)
            values = tokens_ref[here, :].astype(jnp.float32)
            factor = lax.rsqrt(jnp.mean(values * values, axis=-1, keepdims=True) + EPS)
            normed[here, :] = (values * factor * gain_ref[...]).astype(jnp.bfloat16)
            return carry

        lax.fori_loop(0, normed.shape[0] // rows, some, 0)

    def transpose():
        edge = held_w.shape[-1]

        def some(i, carry):
            here = pl.ds(pl.multiple_of(i * edge, edge), edge)
            normed_t_ref[here, :] = normed[:, here].T
            return carry

        lax.fori_loop(0, normed.shape[1] // edge, some, 0)

    def project(result_ref):
        rows = 256

        def some(i, carry):
            here = pl.ds(pl.multiple_of(i * rows, rows), rows)
            result_ref[here, :] = jnp.dot(
                normed[here, :], matrix[...], preferred_element_type=jnp.float32
            )
            return carry

        lax.fori_loop(0, normed.shape[0] // rows, some, 0)

    def unpack(which, qkv_ref, out_ref):
        own, held = arrays[which]
        rows, cols = grid_qkv
        edge = held.shape[-1]

        def qkv_row(i, carry):
            for c in range(cols):
                qkv_ref[pl.ds(pl.multiple_of(i * edge, edge), edge), c * edge:(c + 1) * edge] = (
                    held[slot_ref[i * cols + c]]
                )
            return carry

        lax.fori_loop(0, rows, qkv_row, 0)
        out_rows, out_cols = grid_out

        def out_col(i, carry):
            for r in range(out_rows):
                out_ref[r * edge:(r + 1) * edge, pl.ds(pl.multiple_of(i * edge, edge), edge)] = (
                    held[slot_ref[rows * cols + r * out_cols + i]]
                )
            return carry

        lax.fori_loop(0, out_cols, out_col, 0)

    def finish(which, qkv_ref, out_ref):
        own, held = arrays[which]
        for direction, j in each():
            arrival(which, n - 2, direction, j)
        held[pl.ds(me * slots, slots)] = own[...]
        unpack(which, qkv_ref, out_ref)

    sent = []
    for which in range(2):
        for step in range(n - 1):
            for direction, j in each():
                if step > 0:
                    arrival(which, step - 1, direction, j)
                one = copy(which, step, direction, j)
                one.start()
                sent.append(one)
            if which == 0 and step == 0:
                normalize()
            if which == 0 and step == 1:
                transpose()
            if which == 1 and step == 0:
                finish(0, matrix, wo_ref)
            if which == 1 and step == 1:
                project(proj_ref)
    finish(1, matrix, po_ref)
    project(d_proj_ref)
    for one in sent:
        one.wait_send()


def gather_weights(slot_of, weights, probes, tokens, gain, n, grid_qkv, grid_out):
    slots, edge, _ = weights.shape
    cuts = max(len(part) for part in pieces(slots))
    length, width = tokens.shape
    proj = jax.ShapeDtypeStruct((length, grid_qkv[1] * edge), jnp.float32)
    turned = jax.ShapeDtypeStruct((width, length), jnp.bfloat16)
    out = jax.ShapeDtypeStruct((grid_out[0] * edge, grid_out[1] * edge), jnp.bfloat16)
    vmem = pl.BlockSpec(memory_space=pltpu.VMEM)
    return pl.pallas_call(
        functools.partial(gather_kernel, n, slots, grid_qkv, grid_out),
        out_shape=(proj, proj, out, out, turned),
        in_specs=[pl.BlockSpec(memory_space=pltpu.SMEM)] + [vmem] * 4,
        out_specs=(vmem,) * 5,
        scratch_shapes=[
            pltpu.VMEM((n * slots, edge, edge), jnp.bfloat16),
            pltpu.VMEM((n * slots, edge, edge), jnp.bfloat16),
            pltpu.VMEM((grid_qkv[0] * edge, grid_qkv[1] * edge), jnp.bfloat16),
            pltpu.VMEM((length, width), jnp.bfloat16),
            pltpu.SemaphoreType.DMA((2, n - 1, 2, cuts)),
            pltpu.SemaphoreType.DMA((2, n - 1, 2, cuts)),
        ],
        compiler_params=pltpu.CompilerParams(
            collective_id=0, has_side_effects=True, vmem_limit_bytes=VMEM_BYTES
        ),
    )(slot_of, weights, probes, tokens, gain)


def gradient_blocks(grid_qkv, grid_out, normed_t_ref, d_proj_ref, mixed_t_ref, weighted_ref,
                    out_ref):
    edge = out_ref.shape[-1]
    rows, cols = grid_qkv
    out_rows, out_cols = grid_out
    group = 2

    out_ref[rows * cols + out_rows * out_cols] = jnp.zeros((edge, edge), out_ref.dtype)

    def qkv_rows(i, carry):
        width = group * edge
        left = normed_t_ref[pl.ds(pl.multiple_of(i * width, width), width), :]
        block = jnp.dot(
            left, d_proj_ref[...], preferred_element_type=jnp.float32
        ).astype(jnp.bfloat16)
        for r in range(group):
            for c in range(cols):
                out_ref[(i * group + r) * cols + c] = block[
                    r * edge:(r + 1) * edge, c * edge:(c + 1) * edge
                ]
        return carry

    lax.fori_loop(0, rows // group, qkv_rows, 0)

    def out_columns(i, carry):
        width = group * edge
        right = weighted_ref[:, pl.ds(pl.multiple_of(i * width, width), width)]
        block = jnp.dot(
            mixed_t_ref[...], right, preferred_element_type=jnp.float32
        ).astype(jnp.bfloat16)
        for r in range(out_rows):
            for c in range(group):
                out_ref[rows * cols + r * out_cols + i * group + c] = block[
                    r * edge:(r + 1) * edge, c * edge:(c + 1) * edge
                ]
        return carry

    lax.fori_loop(0, out_cols // group, out_columns, 0)


def reduce_kernel(n, slots, scale, grid_qkv, grid_out, pick_ref, normed_t_ref, d_proj_ref,
                  mixed_t_ref, weighted_ref, out_ref, grads, begin, held, send_sem, recv_sem):
    me = lax.axis_index("fsdp")
    pos = ring_position(me, n)
    right = ring_index(lax.rem(pos + 1, n), n)
    left = ring_index(lax.rem(pos + n - 1, n), n)
    towards = (right, left)
    enter((left, right))
    parts = pieces(slots)
    gradient_blocks(
        grid_qkv, grid_out, normed_t_ref, d_proj_ref, mixed_t_ref, weighted_ref, grads
    )

    def own(step, direction, j):
        shift = n - 1 - step if direction == 0 else 1 + step
        target = ring_index(lax.rem(pos + shift, n), n)
        return target * slots

    def each_block(direction, j, body):
        first, size = parts[direction][j]

        def some(i, carry):
            body(first + i)
            return carry

        lax.fori_loop(0, size, some, 0)

    def copy(step, direction, j):
        first, size = parts[direction][j]
        here = begin.at[pl.ds(first, size)] if step == 0 else held.at[step - 1, pl.ds(first, size)]
        return pltpu.make_async_remote_copy(
            src_ref=here,
            dst_ref=held.at[step, pl.ds(first, size)],
            send_sem=send_sem.at[step, direction, j],
            recv_sem=recv_sem.at[step, direction, j],
            device_id={"fsdp": towards[direction]},
            device_id_type=pl.DeviceIdType.MESH,
        )

    def each():
        for j in range(max(len(parts[0]), len(parts[1]))):
            for direction in range(2):
                if j < len(parts[direction]):
                    yield direction, j

    sent = {}
    for step in range(n - 1):
        for direction, j in each():
            first, size = parts[direction][j]
            base = own(step, direction, j)
            if step > 0:
                sent[step - 1, direction, j].wait_recv()

                def add(t, step=step, base=base):
                    held[step - 1, t] = (
                        held[step - 1, t].astype(jnp.float32)
                        + grads[pick_ref[base + t]].astype(jnp.float32)
                    ).astype(jnp.bfloat16)

                each_block(direction, j, add)
            else:

                def fill(t, base=base):
                    begin[t] = grads[pick_ref[base + t]]

                each_block(direction, j, fill)
            one = copy(step, direction, j)
            one.start()
            sent[step, direction, j] = one
    for direction, j in each():
        first, size = parts[direction][j]
        sent[n - 2, direction, j].wait_recv()
        base = own(n - 1, direction, j)

        def last(t, base=base):
            out_ref[t] = (
                held[n - 2, t].astype(jnp.float32) + grads[pick_ref[base + t]].astype(jnp.float32)
            ) * scale

        each_block(direction, j, last)
    for one in sent.values():
        one.wait_send()


def reduce_slots(picked, normed_t, d_proj, mixed_t, weighted, n, scale, grid_qkv, grid_out):
    slots = picked.shape[0] // n
    edge = BLK
    total_blocks = grid_qkv[0] * grid_qkv[1] + grid_out[0] * grid_out[1]
    cuts = max(len(part) for part in pieces(slots))
    vmem = pl.BlockSpec(memory_space=pltpu.VMEM)
    return pl.pallas_call(
        functools.partial(reduce_kernel, n, slots, scale, grid_qkv, grid_out),
        out_shape=jax.ShapeDtypeStruct((slots, edge, edge), jnp.float32),
        in_specs=[pl.BlockSpec(memory_space=pltpu.SMEM)] + [vmem] * 4,
        out_specs=vmem,
        scratch_shapes=[
            pltpu.VMEM((total_blocks + 1, edge, edge), jnp.bfloat16),
            pltpu.VMEM((slots, edge, edge), jnp.bfloat16),
            pltpu.VMEM((n - 1, slots, edge, edge), jnp.bfloat16),
            pltpu.SemaphoreType.DMA((n - 1, 2, cuts)),
            pltpu.SemaphoreType.DMA((n - 1, 2, cuts)),
        ],
        compiler_params=pltpu.CompilerParams(
            collective_id=1, has_side_effects=True, vmem_limit_bytes=VMEM_BYTES
        ),
    )(picked, normed_t, d_proj, mixed_t, weighted)


def exchange_kernel(mixed_ref, d_mixed_ref, w_ref, p_ref, curv_ref, weighted_ref, back_ref,
                    terms, near, pair, far, share, rest, send_sem, recv_sem):
    me = lax.axis_index("seq")
    side = lax.rem(me, 2)
    core = me + 1 - 2 * side
    across = me + 2 - 4 * lax.rem(lax.div(me, 2), 2)
    enter((core, across), "seq")
    length, width = terms.shape
    half = width // 2
    chunks = recv_sem.shape[1]
    rows = length // chunks
    mine = pl.ds(pl.multiple_of(side * half, half), half)
    other = pl.ds(pl.multiple_of((1 - side) * half, half), half)

    def block(i):
        return pl.ds(i * rows, rows)

    def copy(stage, i, here, there, target):
        return pltpu.make_async_remote_copy(
            src_ref=here,
            dst_ref=there,
            send_sem=send_sem.at[stage, i],
            recv_sem=recv_sem.at[stage, i],
            device_id={"seq": target},
            device_id_type=pl.DeviceIdType.MESH,
        )

    def terms_of(i):
        tile = width // 4

        def columns(j, carry):
            cols = pl.ds(pl.multiple_of(j * tile, tile), tile)
            terms[block(i), cols] = (
                jnp.dot(d_mixed_ref[block(i), :], w_ref[:, cols], preferred_element_type=jnp.float32)
                + jnp.dot(mixed_ref[block(i), :], p_ref[:, cols], preferred_element_type=jnp.float32)
            ).astype(jnp.bfloat16)
            return carry

        lax.fori_loop(0, 4, columns, 0)

    first = [copy(0, i, terms.at[block(i), other], near.at[block(i)], core) for i in range(chunks)]
    second = [copy(1, i, pair.at[block(i)], far.at[block(i)], across) for i in range(chunks)]
    third = [copy(2, i, share.at[block(i)], rest.at[block(i)], core) for i in range(chunks)]

    def send_pair(i):
        first[i].wait_recv()
        pair[block(i)] = (
            terms[block(i), mine].astype(jnp.float32) + near[block(i)].astype(jnp.float32)
        ).astype(jnp.bfloat16)
        second[i].start()

    def send_share(i):
        second[i].wait_recv()
        total = pair[block(i)].astype(jnp.float32) + far[block(i)].astype(jnp.float32)
        share[block(i)] = (curv_ref[block(i), mine].astype(jnp.float32) * total).astype(
            jnp.bfloat16
        )
        third[i].start()

    def finish(i):
        weighted_ref[block(i), mine] = share[block(i)]
        third[i].wait_recv()
        weighted_ref[block(i), other] = rest[block(i)]
        back_ref[block(i), :] = lax.dot_general(
            weighted_ref[block(i), :],
            w_ref[...],
            (((1,), (1,)), ((), ())),
            preferred_element_type=jnp.float32,
        ).astype(jnp.bfloat16)

    for i in range(chunks):
        terms_of(i)
        first[i].start()
        if i > 0:
            send_pair(i - 1)
    send_pair(chunks - 1)
    for i in range(chunks):
        send_share(i)
        if i > 0:
            finish(i - 1)
    finish(chunks - 1)
    for one in first + second + third:
        one.wait_send()


def exchange(mixed, d_mixed, w_out, p_out, curvature):
    length, width = curvature.shape
    chunks = 4
    vmem = pl.BlockSpec(memory_space=pltpu.VMEM)
    half = pltpu.VMEM((length, width // 2), jnp.bfloat16)
    return pl.pallas_call(
        exchange_kernel,
        out_shape=(
            jax.ShapeDtypeStruct((length, width), jnp.bfloat16),
            jax.ShapeDtypeStruct(mixed.shape, jnp.bfloat16),
        ),
        in_specs=[vmem] * 5,
        out_specs=(vmem, vmem),
        scratch_shapes=[
            pltpu.VMEM((length, width), jnp.bfloat16),
            half,
            half,
            half,
            half,
            half,
            pltpu.SemaphoreType.DMA((3, chunks)),
            pltpu.SemaphoreType.DMA((3, chunks)),
        ],
        compiler_params=pltpu.CompilerParams(
            collective_id=2, has_side_effects=True, vmem_limit_bytes=VMEM_BYTES
        ),
    )(mixed, d_mixed, w_out, p_out, curvature)


def local(tokens, norm_gain, curvature, weight_slots, probe_slots, block_counts):
    n_columns = lax.axis_size("seq")
    n_owners = lax.axis_size("fsdp")
    q_heads = HQ // n_columns
    kv_heads = HK // n_columns
    row_blocks = D // BLK
    qkv_cols = (q_heads + 2 * kv_heads) * HD // BLK
    out_rows = q_heads * HD // BLK
    grid_qkv, grid_out = (row_blocks, qkv_cols), (out_rows, row_blocks)
    total_blocks = row_blocks * qkv_cols + out_rows * row_blocks
    slots = weight_slots.shape[1]
    length = tokens.shape[1]
    counts = block_counts[0]
    range_ends = jnp.cumsum(counts)
    starts = range_ends - counts
    owner_ids = jnp.arange(n_owners, dtype=jnp.int32)
    block_ids = jnp.arange(total_blocks, dtype=jnp.int32)
    owners = jnp.sum((range_ends[None, :] <= block_ids[:, None]).astype(jnp.int32), axis=1)
    first_block = jnp.sum(
        jnp.where(owners[:, None] == owner_ids[None, :], starts[None, :], 0), axis=1
    )
    slot_of = (owners * slots + block_ids - first_block).astype(jnp.int32)
    projected, d_projected, w_out, p_out, normed_t = gather_weights(
        slot_of,
        weight_slots[0],
        probe_slots[0],
        tokens[0],
        norm_gain[None, :],
        n_owners,
        grid_qkv,
        grid_out,
    )
    cosine, sine = rotary(length, HD)

    def inner(projected):
        return attention(projected, cosine, sine, q_heads, kv_heads)

    mixed, d_mixed = jax.jvp(inner, (projected,), (d_projected,))
    weighted, back_mixed = exchange(mixed, d_mixed, w_out, p_out, curvature[0])
    mixed_again, pullback = jax.vjp(inner, projected)
    (back_projected,) = pullback(back_mixed)
    slot_index = jnp.arange(n_owners * slots, dtype=jnp.int32)
    place = slot_index % slots
    owner_hot = (slot_index // slots)[:, None] == owner_ids[None, :]
    owner_first = jnp.sum(jnp.where(owner_hot, starts[None, :], 0), axis=1)
    own_count = jnp.sum(jnp.where(owner_hot, counts[None, :], 0), axis=1)
    picked = jnp.where(place < own_count, owner_first + place, total_blocks).astype(jnp.int32)
    scaled = reduce_slots(
        picked,
        normed_t,
        back_projected.astype(jnp.bfloat16),
        mixed_again.T,
        weighted,
        n_owners,
        (length * n_owners) ** -0.5,
        grid_qkv,
        grid_out,
    )
    return scaled.reshape(1, slots, BLK, BLK)


def spot():
    f = lax.axis_index("fsdp")
    s = lax.axis_index("seq")
    return lax.div(f, 2), lax.rem(f, 2), lax.div(s, 2), lax.rem(s, 2)


def device(z, y, x, c):
    return {"fsdp": 2 * z + y, "seq": 2 * x + c}


def mirrored(z, c, planes):
    return z + c * (planes - 1 - 2 * z)


def greet(peers):
    barrier = pltpu.get_barrier_semaphore()
    for peer in peers:
        pl.semaphore_signal(barrier, inc=1, device_id=peer, device_id_type=pl.DeviceIdType.MESH)
    pl.semaphore_wait(barrier, len(peers))


def shard_columns(x, j, width):
    return x * (width // 4) + j * (width // 8), width // 2 + j * (width // 4) + x * (width // 8)


def cut_count(slots):
    return 5 if slots % 5 == 0 else 1


def gather_grid_kernel(n, slots, grid_qkv, grid_out, slot_ref, w_ref, p_ref, tokens_ref, gain_ref,
                       curv_ref, proj_out, d_proj_ref, wo_out, po_out, normed_t_out, curv_out,
                       held_w, held_p, matrix, normed, wo_ref, po_ref, normed_t_ref, proj_ref,
                       curv_part, in_sem, out_sem, send_y, send_core, send_z, recv, tok_send,
                       tok_recv, relay_send, relay_recv, curv_send, curv_recv):
    planes = n // 2
    z, y, x, c = spot()
    zeta = mirrored(z, c, planes)
    hub = lax.rem(zeta, 2) == 0
    spoke = lax.rem(zeta, 2) == 1
    mate = z + 1 - 2 * lax.rem(z, 2)
    y_peer = device(z, 1 - y, x, c)
    x_peer = device(z, y, 1 - x, c)
    core_peer = device(z, y, x, 1 - c)
    z_peer = device(mate, y, x, c)
    row = [device(lax.rem(z + i, planes), y, x, c) for i in range(1, planes)]
    cuts = cut_count(slots)
    size = slots // cuts
    own = (w_ref, p_ref)
    held = (held_w, held_p)
    me = 2 * z + y

    def own_load(which):
        here = held[which].at[pl.ds(me * slots, slots)]
        return pltpu.make_async_copy(own[which], here, in_sem.at[which])

    def token_load():
        return pltpu.make_async_copy(tokens_ref, normed, in_sem.at[2])

    stores = [
        pltpu.make_async_copy(here, there, out_sem.at[i])
        for i, (here, there) in enumerate((
            (normed_t_ref, normed_t_out), (proj_ref, proj_out), (wo_ref, wo_out),
            (po_ref, po_out), (curv_part, curv_out),
        ))
    ]

    @pl.when(hub)
    def _():
        token_load().start()
        for which in range(2):
            own_load(which).start()

    greet(row + [core_peer, y_peer, x_peer])
    tok_cuts = tok_send.shape[0]
    half = normed.shape[0] // 2
    tok_rows = half // tok_cuts
    width = normed.shape[1]
    part = width // 8

    def at(zeta_at):
        return mirrored(zeta_at, c, planes)

    def spread(which, d, j):
        return held[which].at[pl.ds(d * slots + j * size, size)]

    def move(src, which, d, j, peer, sem):
        return pltpu.make_async_remote_copy(
            src_ref=src,
            dst_ref=spread(which, d, j),
            send_sem=sem,
            recv_sem=recv.at[d, which * cuts + j],
            device_id=peer,
            device_id_type=pl.DeviceIdType.MESH,
        )

    def own_chunk(which, j):
        return own[which].at[pl.ds(j * size, size)]

    def arrive(which, d, j):
        move(spread(which, d, j), which, d, j, core_peer, send_y.at[0, 0]).wait_recv()

    other_hub = device(at(2 - zeta), y, x, c)
    near_hub = device(at(2), y, x, c)
    end_hub = device(at(0), y, x, c)

    def token_copy(i, rows_half, peer, s_sem, r_sem, src):
        rows = pl.ds(rows_half * half + i * tok_rows, tok_rows)
        return pltpu.make_async_remote_copy(
            src_ref=src.at[rows],
            dst_ref=normed.at[rows],
            send_sem=s_sem.at[i],
            recv_sem=r_sem.at[i],
            device_id=peer,
            device_id_type=pl.DeviceIdType.MESH,
        )

    def curv_copy(i):
        first = shard_columns(x, lax.rem(mate, 2), width)[i]
        return pltpu.make_async_remote_copy(
            src_ref=curv_ref.at[:, pl.ds(pl.multiple_of(first, part), part)],
            dst_ref=curv_part.at[i],
            send_sem=curv_send.at[i],
            recv_sem=curv_recv.at[i],
            device_id=z_peer,
            device_id_type=pl.DeviceIdType.MESH,
        )

    def curv_local(i):
        first = shard_columns(x, lax.rem(z, 2), width)[i]
        return pltpu.make_async_copy(
            curv_ref.at[:, pl.ds(pl.multiple_of(first, part), part)],
            curv_part.at[i],
            curv_recv.at[i],
        )

    def to_z(which, j):
        k = which * cuts + j
        return move(own_chunk(which, j), which, me, j, other_hub, send_z.at[0, k])

    def to_y(which, j):
        k = which * cuts + j
        return move(own_chunk(which, j), which, me, j, y_peer, send_y.at[0, k])

    def to_core(which, j):
        k = which * cuts + j
        return move(own_chunk(which, j), which, me, j, core_peer, send_core.at[0, k])

    def spoke_own(which, j):
        src = own_chunk(which, j)
        k = which * cuts + j
        return (
            move(src, which, me, j, near_hub, send_z.at[0, k]),
            move(src, which, me, j, end_hub, send_z.at[1, k]),
        )

    lead = min(6, 2 * cuts)
    every = [(which, j) for which in range(2) for j in range(cuts)]

    @pl.when(hub)
    def _():
        for k in range(lead):
            to_y(*every[k]).start()
        for k in range(max(len(every), tok_cuts)):
            if k < len(every):
                to_z(*every[k]).start()
            if k < tok_cuts:
                token_copy(k, x, z_peer, tok_send, tok_recv, tokens_ref).start()
        for i in range(2):
            curv_copy(i).start()
            curv_local(i).start()

    @pl.when(spoke)
    def _():
        for one in every:
            for copy in spoke_own(*one):
                copy.start()

    def pass_row(k):
        which, j = every[k]
        to_core(which, j).start()
        for r in range(1, planes):
            d = 2 * at(lax.rem(zeta + r, planes)) + y
            arrive(which, d, j)
            src = spread(which, d, j)
            move(src, which, d, j, y_peer, send_y.at[r, k]).start()
            move(src, which, d, j, core_peer, send_core.at[r, k]).start()
            if r == 1 and k + lead < len(every):
                to_y(*every[k + lead]).start()

    def pass_across(k):
        which, j = every[k]
        for r in range(planes):
            d = 2 * at(lax.rem(zeta + r, planes)) + 1 - y
            arrive(which, d, j)
            move(spread(which, d, j), which, d, j, core_peer, send_core.at[planes + r, k]).start()

    def forward(which, j):
        k = which * cuts + j
        pass_row(k)
        if k not in (0, cuts):
            pass_across(k - 1)
        if k in (cuts - 1, 2 * cuts - 1):
            pass_across(k)

    def step(which, j):
        @pl.when(hub)
        def _():
            forward(which, j)

        @pl.when(spoke)
        def _():
            for d in range(n):
                arrive(which, d, j)

    def normalize():
        rows = 32

        def some(i, carry):
            here = pl.ds(pl.multiple_of(i * rows, rows), rows)
            values = normed[here, :].astype(jnp.float32)
            factor = lax.rsqrt(jnp.mean(values * values, axis=-1, keepdims=True) + EPS)
            normed[here, :] = (values * factor * gain_ref[...]).astype(jnp.bfloat16)
            return carry

        lax.fori_loop(0, normed.shape[0] // rows, some, 0)

    def transpose():
        edge = held_w.shape[-1]

        def some(i, carry):
            here = pl.ds(pl.multiple_of(i * edge, edge), edge)
            normed_t_ref[here, :] = normed[:, here].T
            return carry

        lax.fori_loop(0, normed.shape[1] // edge, some, 0)

    def project(result_ref):
        rows = 256

        def some(i, carry):
            here = pl.ds(pl.multiple_of(i * rows, rows), rows)
            result_ref[here, :] = jnp.dot(
                normed[here, :], matrix[...], preferred_element_type=jnp.float32
            )
            return carry

        lax.fori_loop(0, normed.shape[0] // rows, some, 0)

    def unpack_qkv(which):
        rows, cols = grid_qkv
        edge = held_w.shape[-1]

        def qkv_row(i, carry):
            for col in range(cols):
                matrix[pl.ds(pl.multiple_of(i * edge, edge), edge), col * edge:(col + 1) * edge] = (
                    held[which][slot_ref[i * cols + col]]
                )
            return carry

        lax.fori_loop(0, rows, qkv_row, 0)

    def unpack_out(which, out_ref):
        rows, cols = grid_qkv
        out_rows, out_cols = grid_out
        edge = held_w.shape[-1]

        def out_col(i, carry):
            for r in range(out_rows):
                out_ref[r * edge:(r + 1) * edge, pl.ds(pl.multiple_of(i * edge, edge), edge)] = (
                    held[which][slot_ref[rows * cols + r * out_cols + i]]
                )
            return carry

        lax.fori_loop(0, out_cols, out_col, 0)

    def keep_own(which):
        @pl.when(hub)
        def _():
            own_load(which).wait()

    @pl.when(hub)
    def _():
        token_load().wait()

    @pl.when(spoke)
    def _():
        for i in range(tok_cuts):
            token_copy(i, x, z_peer, tok_send, tok_recv, normed).wait_recv()
            token_copy(i, x, x_peer, relay_send, relay_recv, normed).start()
        for i in range(tok_cuts):
            token_copy(i, 1 - x, x_peer, relay_send, relay_recv, normed).wait_recv()
        for i in range(tok_cuts):
            token_copy(i, x, x_peer, relay_send, relay_recv, normed).wait_send()

    normalize()
    for j in range(cuts):
        step(0, j)
        if j == 0:
            transpose()
            stores[0].start()
    keep_own(0)
    def first_proj():
        project(proj_ref)
        stores[1].start()

    def first_out():
        unpack_out(0, wo_ref)
        stores[2].start()

    todo = [lambda: unpack_qkv(0), first_proj, first_out]
    for j in range(cuts):
        step(1, j)
        if j < cuts - 1 and todo:
            todo.pop(0)()
    while todo:
        todo.pop(0)()
    keep_own(1)
    unpack_out(1, po_ref)
    stores[3].start()

    @pl.when(hub)
    def _():
        for i in range(2):
            curv_local(i).wait()

    @pl.when(spoke)
    def _():
        for i in range(2):
            curv_copy(i).wait_recv()

    stores[4].start()
    unpack_qkv(1)
    project(d_proj_ref)

    @pl.when(hub)
    def _():
        for i in range(tok_cuts):
            token_copy(i, x, z_peer, tok_send, tok_recv, tokens_ref).wait_send()
        for i in range(2):
            curv_copy(i).wait_send()
        for k, (which, j) in enumerate(every):
            to_z(which, j).wait_send()
            to_y(which, j).wait_send()
            to_core(which, j).wait_send()
            src = spread(which, me, j)
            for r in range(1, planes):
                move(src, which, me, j, y_peer, send_y.at[r, k]).wait_send()
            for r in range(1, n):
                move(src, which, me, j, core_peer, send_core.at[r, k]).wait_send()

    @pl.when(spoke)
    def _():
        for one in every:
            for copy in spoke_own(*one):
                copy.wait_send()

    for store in stores:
        store.wait()


def gather_grid(slot_of, weights, probes, tokens, gain, curvature, n, grid_qkv, grid_out):
    slots, edge, _ = weights.shape
    cuts = cut_count(slots)
    length, width = tokens.shape
    proj = jax.ShapeDtypeStruct((length, grid_qkv[1] * edge), jnp.float32)
    turned = jax.ShapeDtypeStruct((width, length), jnp.bfloat16)
    out = jax.ShapeDtypeStruct((grid_out[0] * edge, grid_out[1] * edge), jnp.bfloat16)
    shard = (2, length, width // 8)
    vmem = pl.BlockSpec(memory_space=pltpu.VMEM)
    anywhere = pl.BlockSpec(memory_space=pl.ANY)
    dma = pltpu.SemaphoreType.DMA
    return pl.pallas_call(
        functools.partial(gather_grid_kernel, n, slots, grid_qkv, grid_out),
        out_shape=(proj, proj, out, out, turned, jax.ShapeDtypeStruct(shard, jnp.bfloat16)),
        in_specs=[pl.BlockSpec(memory_space=pltpu.SMEM)] + [anywhere] * 3 + [vmem, anywhere],
        out_specs=(anywhere, vmem) + (anywhere,) * 4,
        scratch_shapes=[
            pltpu.VMEM((n * slots, edge, edge), jnp.bfloat16),
            pltpu.VMEM((n * slots, edge, edge), jnp.bfloat16),
            pltpu.VMEM((grid_qkv[0] * edge, grid_qkv[1] * edge), jnp.bfloat16),
            pltpu.VMEM((length, width), jnp.bfloat16),
            pltpu.VMEM(out.shape, out.dtype),
            pltpu.VMEM(out.shape, out.dtype),
            pltpu.VMEM(turned.shape, turned.dtype),
            pltpu.VMEM(proj.shape, proj.dtype),
            pltpu.VMEM(shard, jnp.bfloat16),
            dma((3,)),
            dma((5,)),
            dma((n // 2, 2 * cuts)),
            dma((n, 2 * cuts)),
            dma((2, 2 * cuts)),
            dma((n, 2 * cuts)),
            dma((4,)),
            dma((4,)),
            dma((4,)),
            dma((4,)),
            dma((2,)),
            dma((2,)),
        ],
        compiler_params=pltpu.CompilerParams(
            collective_id=3, has_side_effects=True, vmem_limit_bytes=GRID_VMEM_BYTES
        ),
    )(slot_of, weights, probes, tokens, gain, curvature)


def turn_tables(length, head_dim):
    cosine, sine = rotary(length, head_dim)
    cosine, sine = cosine[:, 0, :], sine[:, 0, :]
    return jnp.concatenate([cosine, cosine], axis=1), jnp.concatenate([-sine, sine], axis=1)


def turn(values, cosine, sine):
    return values * cosine + pltpu.roll(values, values.shape[1] // 2, 1) * sine


def attend(heads, proj_ref, d_proj_ref, cos_ref, sin_ref, mixed_ref, d_mixed_ref, mixed_t_ref,
           probs_ref, rot_ref, d_rot):
    length = proj_ref.shape[0]
    hd = cos_ref.shape[1]
    key_at = heads * hd
    val_at = key_at + hd
    scale = hd ** -0.5

    def spin(source, target):
        def some(h, carry):
            here = pl.ds(pl.multiple_of(h * hd, hd), hd)
            target[:, here] = turn(source[:, here], cos_ref[...], sin_ref[...]).astype(jnp.bfloat16)
            return carry

        lax.fori_loop(0, heads + 1, some, 0)
        target[:, val_at:] = source[:, val_at:].astype(jnp.bfloat16)

    spin(proj_ref, rot_ref)
    spin(d_proj_ref, d_rot)
    tile = hd

    def head(h, carry):
        here = pl.ds(pl.multiple_of(h * hd, hd), hd)
        for i in range(length // tile):
            rows = slice(i * tile, (i + 1) * tile)
            span = (i + 1) * tile
            q, dq = rot_ref[rows, here], d_rot[rows, here]
            k, dk = rot_ref[:span, key_at:val_at], d_rot[:span, key_at:val_at]
            v, dv = rot_ref[:span, val_at:], d_rot[:span, val_at:]
            contract = (((1,), (1,)), ((), ()))
            scores = lax.dot_general(q, k, contract, preferred_element_type=jnp.float32) * scale
            slopes = lax.dot_general(
                jnp.concatenate([dq, q], axis=1),
                jnp.concatenate([k, dk], axis=1),
                contract,
                preferred_element_type=jnp.float32,
            ) * scale
            at_row = i * tile + lax.broadcasted_iota(jnp.int32, (tile, span), 0)
            at_col = lax.broadcasted_iota(jnp.int32, (tile, span), 1)
            seen = at_row >= at_col
            scores = jnp.where(seen, scores, NEGATIVE)
            slopes = jnp.where(seen, slopes, 0.0)
            raised = jnp.exp(scores - jnp.max(scores, axis=1, keepdims=True))
            probs = raised / jnp.sum(raised, axis=1, keepdims=True)
            d_probs = probs * (slopes - jnp.sum(probs * slopes, axis=1, keepdims=True))
            probs = probs.astype(jnp.bfloat16)
            d_probs = d_probs.astype(jnp.bfloat16)
            probs_ref[h, rows, :span] = probs
            if span < length:
                probs_ref[h, rows, span:] = jnp.zeros((tile, length - span), jnp.bfloat16)
            mixed = jnp.dot(probs, v, preferred_element_type=jnp.float32).astype(jnp.bfloat16)
            mixed_ref[rows, here] = mixed
            mixed_t_ref[here, rows] = mixed.T
            d_mixed_ref[rows, here] = (
                jnp.dot(d_probs, v, preferred_element_type=jnp.float32)
                + jnp.dot(probs, dv, preferred_element_type=jnp.float32)
            ).astype(jnp.bfloat16)
        return carry

    lax.fori_loop(0, heads, head, 0)


def attend_back(heads, back_ref, probs_ref, rot_ref, cos_ref, sin_ref, out_ref, slope_ref):
    length = back_ref.shape[0]
    hd = cos_ref.shape[1]
    key_at = heads * hd
    val_at = key_at + hd
    scale = hd ** -0.5
    tile = hd

    def unturn(values):
        rounded = values.astype(jnp.bfloat16).astype(jnp.float32)
        return turn(rounded, cos_ref[...], -sin_ref[...]).astype(jnp.bfloat16)

    def head(h, totals):
        here = pl.ds(pl.multiple_of(h * hd, hd), hd)
        key_total, val_total = totals
        for i in range(length // tile):
            rows = slice(i * tile, (i + 1) * tile)
            span = (i + 1) * tile
            back = back_ref[rows, here]
            d_probs = lax.dot_general(
                back, rot_ref[:span, val_at:], (((1,), (1,)), ((), ())),
                preferred_element_type=jnp.float32,
            ).astype(jnp.bfloat16).astype(jnp.float32)
            probs = probs_ref[h, rows, :span].astype(jnp.float32)
            slopes = probs * (d_probs - jnp.sum(probs * d_probs, axis=1, keepdims=True)) * scale
            slope_ref[rows, :span] = slopes.astype(jnp.bfloat16)
            if span < length:
                slope_ref[rows, span:] = jnp.zeros((tile, length - span), jnp.bfloat16)
        slopes = slope_ref[...]
        d_query = jnp.dot(slopes, rot_ref[:, key_at:val_at], preferred_element_type=jnp.float32)
        out_ref[:, here] = unturn(d_query)
        first = (((0,), (0,)), ((), ()))
        key_total = key_total + lax.dot_general(
            rot_ref[:, here], slopes, first, preferred_element_type=jnp.float32
        )
        val_total = val_total + lax.dot_general(
            back_ref[:, here], probs_ref[h], first, preferred_element_type=jnp.float32
        )
        return key_total, val_total

    zero = jnp.zeros((hd, length), jnp.float32)
    key_total, val_total = lax.fori_loop(0, heads, head, (zero, zero))
    out_ref[:, key_at:val_at] = unturn(key_total.T)
    out_ref[:, val_at:] = val_total.T.astype(jnp.bfloat16)


def square_kernel(heads, proj_ref, d_proj_ref, w_out, p_out, curv_ref, cos_ref, sin_ref,
                  weighted_out, back_proj_ref, mixed_t_ref, w_ref, p_ref, mixed_ref, d_mixed_ref,
                  probs, rot, d_rot, slope, back_ref, terms, near_x, near_z, pair_a, pair_b, far_z,
                  far_x, full, load_sem, store_sem, send_sem, recv_sem):
    z, y, x, c = spot()
    side = lax.rem(z, 2)
    x_peer = device(z, y, 1 - x, c)
    z_peer = device(z + 1 - 2 * side, y, x, c)
    loads = [
        pltpu.make_async_copy(w_out, w_ref, load_sem.at[0]),
        pltpu.make_async_copy(p_out, p_ref, load_sem.at[1]),
    ]
    for load in loads:
        load.start()
    greet([x_peer, z_peer])
    attend(
        heads, proj_ref, d_proj_ref, cos_ref, sin_ref, mixed_ref, d_mixed_ref, mixed_t_ref, probs,
        rot, d_rot,
    )
    for load in loads:
        load.wait()
    length, width = terms.shape
    quarter, part = width // 4, width // 8
    chunks = recv_sem.shape[1]
    rows = length // chunks

    def block(i):
        return pl.ds(i * rows, rows)

    def cols(first, count):
        return pl.ds(pl.multiple_of(first, count), count)

    keep_a, give_a = cols(x * quarter, quarter), cols((1 - x) * quarter, quarter)
    keep_b = cols(width // 2 + side * quarter, quarter)
    give_b = cols(width // 2 + (1 - side) * quarter, quarter)
    first_a, first_b = shard_columns(x, side, width)
    own_a, own_b = cols(first_a, part), cols(first_b, part)

    def copy(kind, i, here, there, target):
        return pltpu.make_async_remote_copy(
            src_ref=here,
            dst_ref=there,
            send_sem=send_sem.at[kind, i],
            recv_sem=recv_sem.at[kind, i],
            device_id=target,
            device_id_type=pl.DeviceIdType.MESH,
        )

    def stage(i):
        b = block(i)
        return (
            copy(0, i, terms.at[b, give_a], near_x.at[b], x_peer),
            copy(1, i, terms.at[b, give_b], near_z.at[b], z_peer),
            copy(2, i, pair_a.at[b, cols((1 - side) * part, part)], far_z.at[b], z_peer),
            copy(3, i, pair_b.at[b, cols((1 - x) * part, part)], far_x.at[b], x_peer),
            copy(4, i, full.at[b, own_a], full.at[b, own_a], z_peer),
            copy(5, i, full.at[b, own_b], full.at[b, own_b], x_peer),
            copy(6, i, full.at[b, keep_a], full.at[b, keep_a], x_peer),
            copy(7, i, full.at[b, keep_b], full.at[b, keep_b], z_peer),
        )

    def incoming(kind, i, there):
        copy(kind, i, there, there, x_peer).wait_recv()

    def terms_of(i):
        tile = width // 4

        def columns(j, carry):
            here = pl.ds(pl.multiple_of(j * tile, tile), tile)
            terms[block(i), here] = (
                jnp.dot(d_mixed_ref[block(i), :], w_ref[:, here], preferred_element_type=jnp.float32)
                + jnp.dot(mixed_ref[block(i), :], p_ref[:, here], preferred_element_type=jnp.float32)
            ).astype(jnp.bfloat16)
            return carry

        lax.fori_loop(0, 4, columns, 0)

    plans = [stage(i) for i in range(chunks)]

    def pair_up(i):
        b = block(i)
        for kind, pair, keep, near in ((0, pair_a, keep_a, near_x), (1, pair_b, keep_b, near_z)):
            incoming(kind, i, near.at[b])
            pair[b] = (
                terms[b, keep].astype(jnp.float32) + near[b].astype(jnp.float32)
            ).astype(jnp.bfloat16)
            plans[i][2 + kind].start()

    def weigh(i):
        b = block(i)
        for kind, pair, mine, far, own_cols in (
            (0, pair_a, side, far_z, own_a), (1, pair_b, x, far_x, own_b)
        ):
            incoming(2 + kind, i, far.at[b])
            total = pair[b, cols(mine * part, part)].astype(jnp.float32) + far[b].astype(jnp.float32)
            full[b, own_cols] = (curv_ref[kind, b].astype(jnp.float32) * total).astype(jnp.bfloat16)
            plans[i][4 + kind].start()

    def widen(i):
        b = block(i)
        other_a, other_b = shard_columns(x, 1 - side, width)[0], shard_columns(1 - x, side, width)[1]
        incoming(4, i, full.at[b, cols(other_a, part)])
        plans[i][6].start()
        incoming(5, i, full.at[b, cols(other_b, part)])
        plans[i][7].start()

    def store(i):
        b = block(i)
        return pltpu.make_async_copy(full.at[b], weighted_out.at[b], store_sem.at[i])

    def finish(i):
        b = block(i)
        incoming(6, i, full.at[b, give_a])
        incoming(7, i, full.at[b, give_b])
        store(i).start()
        back_ref[b, :] = lax.dot_general(
            full[b, :], w_ref[...], (((1,), (1,)), ((), ())), preferred_element_type=jnp.float32
        ).astype(jnp.bfloat16)

    for i in range(chunks + 3):
        if i < chunks:
            terms_of(i)
            plans[i][0].start()
            plans[i][1].start()
        if 0 <= i - 1 < chunks:
            pair_up(i - 1)
        if 0 <= i - 2 < chunks:
            weigh(i - 2)
        if 0 <= i - 3 < chunks:
            widen(i - 3)
    for i in range(chunks):
        finish(i)
    attend_back(heads, back_ref, probs, rot, cos_ref, sin_ref, back_proj_ref, slope)
    for i in range(chunks):
        store(i).wait()
    for plan in plans:
        for one in plan:
            one.wait_send()


def square_exchange(projected, d_projected, w_out, p_out, curvature, cosine, sine, heads):
    length, inputs = projected.shape
    inner, width = w_out.shape
    chunks = 4
    half = jnp.bfloat16
    vmem = pl.BlockSpec(memory_space=pltpu.VMEM)
    anywhere = pl.BlockSpec(memory_space=pl.ANY)
    quarter = pltpu.VMEM((length, width // 4), half)
    part = pltpu.VMEM((length, width // 8), half)
    whole = pltpu.VMEM((length, width), half)
    narrow = pltpu.VMEM((length, inner), half)
    return pl.pallas_call(
        functools.partial(square_kernel, heads),
        out_shape=(
            jax.ShapeDtypeStruct((length, width), half),
            jax.ShapeDtypeStruct((length, inputs), half),
            jax.ShapeDtypeStruct((inner, length), half),
        ),
        in_specs=[vmem] * 2 + [anywhere] * 2 + [vmem] * 3,
        out_specs=(anywhere, vmem, vmem),
        scratch_shapes=[
            pltpu.VMEM((inner, width), half),
            pltpu.VMEM((inner, width), half),
            narrow,
            narrow,
            pltpu.VMEM((heads, length, length), half),
            pltpu.VMEM((length, inputs), half),
            pltpu.VMEM((length, inputs), half),
            pltpu.VMEM((length, length), half),
            narrow,
            whole, quarter, quarter, quarter, quarter, part, part, whole,
            pltpu.SemaphoreType.DMA((2,)),
            pltpu.SemaphoreType.DMA((chunks,)),
            pltpu.SemaphoreType.DMA((8, chunks)),
            pltpu.SemaphoreType.DMA((8, chunks)),
        ],
        compiler_params=pltpu.CompilerParams(
            collective_id=4, has_side_effects=True, vmem_limit_bytes=GRID_VMEM_BYTES
        ),
    )(projected, d_projected, w_out, p_out, curvature, cosine, sine)


def reduce_grid_kernel(n, slots, scale, grid_qkv, grid_out, pick_ref, normed_t_in, d_proj_ref,
                       mixed_t_ref, weighted_ref, out_ref, normed_t_ref, load_sem, grads, peer, begin, across, onward,
                       landed, core_send, core_recv, y_send, y_recv, z_send, z_recv):
    planes = n // 2
    z, y, x, c = spot()
    zeta = mirrored(z, c, planes)
    hub = lax.rem(zeta, 2) == 0
    spoke = lax.rem(zeta, 2) == 1
    late = lax.div(zeta, 2)
    y_peer = device(z, 1 - y, x, c)
    core_peer = device(z, y, x, 1 - c)
    row = [device(lax.rem(z + i, planes), y, x, c) for i in range(1, planes)]
    load = pltpu.make_async_copy(normed_t_in, normed_t_ref, load_sem.at[0])
    load.start()
    greet(row + [core_peer, y_peer])
    cuts = cut_count(slots)
    size = slots // cuts
    rows, cols = grid_qkv
    out_rows, out_cols = grid_out
    total = rows * cols + out_rows * out_cols
    edge = out_ref.shape[-1]
    legs = core_send.shape[0] - 1
    leg_rows = rows // legs
    group = 2

    def core_copy(i):
        if i == legs:
            here = pl.ds(rows * cols, out_rows * out_cols)
        else:
            here = pl.ds(i * leg_rows * cols, leg_rows * cols)
        return pltpu.make_async_remote_copy(
            src_ref=grads.at[here],
            dst_ref=peer.at[here],
            send_sem=core_send.at[i],
            recv_sem=core_recv.at[i],
            device_id=core_peer,
            device_id_type=pl.DeviceIdType.MESH,
        )

    def out_columns(i, carry):
        width = group * edge
        right = weighted_ref[:, pl.ds(pl.multiple_of(i * width, width), width)]
        block = jnp.dot(
            mixed_t_ref[...], right, preferred_element_type=jnp.float32
        ).astype(jnp.bfloat16)
        for r in range(out_rows):
            for k in range(group):
                grads[rows * cols + r * out_cols + i * group + k] = block[
                    r * edge:(r + 1) * edge, k * edge:(k + 1) * edge
                ]
        return carry

    def qkv_rows(i, carry):
        width = group * edge
        left = normed_t_ref[pl.ds(pl.multiple_of(i * width, width), width), :]
        block = jnp.dot(
            left, d_proj_ref[...], preferred_element_type=jnp.float32
        ).astype(jnp.bfloat16)
        for r in range(group):
            for k in range(cols):
                grads[(i * group + r) * cols + k] = block[
                    r * edge:(r + 1) * edge, k * edge:(k + 1) * edge
                ]
        return carry

    def hand_over(i):
        @pl.when(spoke)
        def _():
            core_copy(i).start()

    grads[total] = jnp.zeros((edge, edge), grads.dtype)
    peer[total] = jnp.zeros((edge, edge), peer.dtype)
    lax.fori_loop(0, out_cols // group, out_columns, 0)
    hand_over(legs)
    load.wait()
    for i in range(legs):
        steps = leg_rows // group
        lax.fori_loop(i * steps, (i + 1) * steps, qkv_rows, 0)
        hand_over(i)

    def owner(i, at_y):
        first = (3, 2, 1, 0)[i]
        second = (0, 1, 3, 2)[i]
        o = (1 - late) * first + late * second
        return 2 * mirrored(o, c, planes) + at_y

    def both(index):
        return grads[index].astype(jnp.float32) + peer[index].astype(jnp.float32)

    def y_copy(i, j):
        here = pl.ds(i * slots + j * size, size)
        return pltpu.make_async_remote_copy(
            src_ref=begin.at[here],
            dst_ref=across.at[here],
            send_sem=y_send.at[i, j],
            recv_sem=y_recv.at[i, j],
            device_id=y_peer,
            device_id_type=pl.DeviceIdType.MESH,
        )

    def z_copy(i, j):
        goal = (1 - late) * (2, 2, 1)[i] + late * (0, 1, 3)[i]
        buffer = (0, 1, 0)[i]
        return pltpu.make_async_remote_copy(
            src_ref=onward.at[i, pl.ds(j * size, size)],
            dst_ref=landed.at[buffer, pl.ds(j * size, size)],
            send_sem=z_send.at[i, j],
            recv_sem=z_recv.at[buffer, j],
            device_id=device(mirrored(goal, c, planes), y, x, c),
            device_id_type=pl.DeviceIdType.MESH,
        )

    def z_wait(buffer, j):
        here = landed.at[buffer, pl.ds(j * size, size)]
        pltpu.make_async_remote_copy(
            src_ref=here,
            dst_ref=here,
            send_sem=z_send.at[0, j],
            recv_sem=z_recv.at[buffer, j],
            device_id=core_peer,
            device_id_type=pl.DeviceIdType.MESH,
        ).wait_recv()

    def each(j, body):
        def some(t, carry):
            body(j * size + t)
            return carry

        lax.fori_loop(0, size, some, 0)

    @pl.when(hub)
    def _():
        for i in (legs,) + tuple(range(legs)):
            core_copy(i).wait_recv()
        def start(i, j):
            base = owner(i, 1 - y) * slots

            def fill(t):
                begin[i * slots + t] = both(pick_ref[base + t]).astype(jnp.bfloat16)

            each(j, fill)
            y_copy(i, j).start()

        def go(i, j):
            base = owner(i, y) * slots

            def value(t):
                return both(pick_ref[base + t]) + across[i * slots + t].astype(jnp.float32)

            def pass_on(t):
                onward[i, t] = value(t).astype(jnp.bfloat16)

            def join_on(t):
                onward[i, t] = (value(t) + landed[0, t].astype(jnp.float32)).astype(jnp.bfloat16)

            def last(t):
                out_ref[t] = (value(t) + landed[late, t].astype(jnp.float32)) * scale

            y_copy(i, j).wait_recv()
            if i < 2:
                each(j, pass_on)
                z_copy(i, j).start()
            elif i == 2:

                @pl.when(late == 0)
                def _():
                    each(j, pass_on)

                @pl.when(late == 1)
                def _():
                    z_wait(0, j)
                    each(j, join_on)

                z_copy(i, j).start()
            else:
                z_wait(late, j)
                each(j, last)

        for i in range(planes + 1):

            def turn_round(j, carry, i=i):
                if i < planes:
                    start(i, j)
                if i > 0:
                    go(i - 1, j)
                return carry

            lax.fori_loop(0, cuts, turn_round, 0)

        def close(j, carry):
            for i in range(planes):
                y_copy(i, j).wait_send()
            for i in range(3):
                z_copy(i, j).wait_send()
            return carry

        lax.fori_loop(0, cuts, close, 0)

    @pl.when(spoke)
    def _():
        @pl.when(zeta == 1)
        def _():
            def go(j, carry):
                z_wait(0, j)
                z_wait(1, j)

                def last(t):
                    out_ref[t] = (
                        landed[0, t].astype(jnp.float32) + landed[1, t].astype(jnp.float32)
                    ) * scale

                each(j, last)
                return carry

            lax.fori_loop(0, cuts, go, 0)

        @pl.when(zeta == 3)
        def _():
            def go(j, carry):
                z_wait(0, j)

                def last(t):
                    out_ref[t] = landed[0, t].astype(jnp.float32) * scale

                each(j, last)
                return carry

            lax.fori_loop(0, cuts, go, 0)

        for i in range(legs + 1):
            core_copy(i).wait_send()


def reduce_grid(picked, normed_t, d_proj, mixed_t, weighted, n, scale, grid_qkv, grid_out):
    slots = picked.shape[0] // n
    edge = BLK
    total_blocks = grid_qkv[0] * grid_qkv[1] + grid_out[0] * grid_out[1]
    cuts = cut_count(slots)
    legs = 4
    vmem = pl.BlockSpec(memory_space=pltpu.VMEM)
    dma = pltpu.SemaphoreType.DMA
    return pl.pallas_call(
        functools.partial(reduce_grid_kernel, n, slots, scale, grid_qkv, grid_out),
        out_shape=jax.ShapeDtypeStruct((slots, edge, edge), jnp.float32),
        in_specs=[pl.BlockSpec(memory_space=pltpu.SMEM), pl.BlockSpec(memory_space=pl.ANY)]
        + [vmem] * 3,
        out_specs=vmem,
        scratch_shapes=[
            pltpu.VMEM(normed_t.shape, normed_t.dtype),
            dma((1,)),
            pltpu.VMEM((total_blocks + 1, edge, edge), jnp.bfloat16),
            pltpu.VMEM((total_blocks + 1, edge, edge), jnp.bfloat16),
            pltpu.VMEM((n // 2 * slots, edge, edge), jnp.bfloat16),
            pltpu.VMEM((n // 2 * slots, edge, edge), jnp.bfloat16),
            pltpu.VMEM((3, slots, edge, edge), jnp.bfloat16),
            pltpu.VMEM((2, slots, edge, edge), jnp.bfloat16),
            dma((legs + 1,)),
            dma((legs + 1,)),
            dma((n // 2, cuts)),
            dma((n // 2, cuts)),
            dma((3, cuts)),
            dma((2, cuts)),
        ],
        compiler_params=pltpu.CompilerParams(
            collective_id=5, has_side_effects=True, vmem_limit_bytes=GRID_VMEM_BYTES
        ),
    )(picked, normed_t, d_proj, mixed_t, weighted)


def local_grid(tokens, norm_gain, curvature, weight_slots, probe_slots, block_counts):
    n_columns = lax.axis_size("seq")
    n_owners = lax.axis_size("fsdp")
    q_heads = HQ // n_columns
    kv_heads = HK // n_columns
    row_blocks = D // BLK
    qkv_cols = (q_heads + 2 * kv_heads) * HD // BLK
    out_rows = q_heads * HD // BLK
    grid_qkv, grid_out = (row_blocks, qkv_cols), (out_rows, row_blocks)
    total_blocks = row_blocks * qkv_cols + out_rows * row_blocks
    slots = weight_slots.shape[1]
    length = tokens.shape[1]
    z, _, _, c = spot()
    theirs = lax.ppermute(block_counts, "seq", [(i, i ^ 1) for i in range(n_columns)])
    counts = jnp.where(lax.rem(z, 2) == c, block_counts, theirs)[0]
    range_ends = jnp.cumsum(counts)
    starts = range_ends - counts
    owner_ids = jnp.arange(n_owners, dtype=jnp.int32)
    block_ids = jnp.arange(total_blocks, dtype=jnp.int32)
    owners = jnp.sum((range_ends[None, :] <= block_ids[:, None]).astype(jnp.int32), axis=1)
    first_block = jnp.sum(
        jnp.where(owners[:, None] == owner_ids[None, :], starts[None, :], 0), axis=1
    )
    slot_of = (owners * slots + block_ids - first_block).astype(jnp.int32)
    projected, d_projected, w_out, p_out, normed_t, curv_part = gather_grid(
        slot_of,
        weight_slots[0],
        probe_slots[0],
        tokens[0],
        norm_gain[None, :],
        curvature[0],
        n_owners,
        grid_qkv,
        grid_out,
    )
    cosine, sine = turn_tables(length, HD)
    weighted, back_projected, mixed_t = square_exchange(
        projected, d_projected, w_out, p_out, curv_part, cosine, sine, q_heads
    )
    slot_index = jnp.arange(n_owners * slots, dtype=jnp.int32)
    place = slot_index % slots
    owner_hot = (slot_index // slots)[:, None] == owner_ids[None, :]
    owner_first = jnp.sum(jnp.where(owner_hot, starts[None, :], 0), axis=1)
    own_count = jnp.sum(jnp.where(owner_hot, counts[None, :], 0), axis=1)
    picked = jnp.where(place < own_count, owner_first + place, total_blocks).astype(jnp.int32)
    scaled = reduce_grid(
        picked,
        normed_t,
        back_projected,
        mixed_t,
        weighted,
        n_owners,
        (length * n_owners) ** -0.5,
        grid_qkv,
        grid_out,
    )
    return scaled.reshape(1, slots, BLK, BLK)


def solution(mesh):
    in_specs = (
        P("fsdp", None, None),
        P(),
        P("fsdp", None, None),
        P("seq", "fsdp", None, None),
        P("seq", "fsdp", None, None),
        P("seq", None),
    )
    out_specs = P("seq", "fsdp", None, None)
    body = local_grid if mesh.shape["fsdp"] == 8 and mesh.shape["seq"] == 4 else local
    return jax.shard_map(body, mesh=mesh, in_specs=in_specs, out_specs=out_specs, check_vma=False)
```

```python
import functools

import jax
import jax.numpy as jnp
import numpy as np
from jax import lax
from jax.experimental import pallas as pl
from jax.experimental.pallas import tpu as pltpu
from jax.sharding import PartitionSpec as P

D = 4096
HQ = 16
HK = 4
HD = 128
BLK = 128


THETA = 500000.0
EPS = 1e-05
NEGATIVE = -1e30


def rotary(length, head_dim):
    half_dim = head_dim // 2
    frequency = jnp.exp(-jnp.log(THETA) * 2.0 * jnp.arange(half_dim, dtype=jnp.float32) / head_dim)
    angles = jnp.arange(length, dtype=jnp.float32)[:, None] * frequency[None, :]
    return (jnp.cos(angles)[:, None, :], jnp.sin(angles)[:, None, :])


def rotate(field_in, cosine, sine):
    half_dim = field_in.shape[-1] // 2
    first_half = field_in[..., :half_dim]
    second = field_in[..., half_dim:]
    return jnp.concatenate(
        [first_half * cosine - second * sine, second * cosine + first_half * sine], axis=-1
    )


VMEM_BYTES = 62 * 1024 * 1024
GRID_VMEM_BYTES = 67043328


def attention(projected, cosine, sine, q_heads, kv_heads):
    length = projected.shape[0]
    head_dim = projected.shape[1] // (q_heads + 2 * kv_heads)
    q_end = q_heads * head_dim
    k_end = q_end + kv_heads * head_dim
    queries = rotate(projected[:, :q_end].reshape(length, q_heads, head_dim), cosine, sine).astype(
        jnp.bfloat16
    )
    key_rows = rotate(
        projected[:, q_end:k_end].reshape(length, kv_heads, head_dim), cosine, sine
    ).astype(jnp.bfloat16)
    values = projected[:, k_end:].reshape(length, kv_heads, head_dim).astype(jnp.bfloat16)
    queries = queries.reshape(length, kv_heads, q_heads // kv_heads, head_dim)
    scores = jnp.einsum(
        "qkgd,skd->kgqs", queries, key_rows, preferred_element_type=jnp.float32
    ) * head_dim ** (-0.5)
    causal = jnp.arange(length)[:, None] >= jnp.arange(length)[None, :]
    scores = jnp.where(causal, scores, NEGATIVE)
    attn_probs = jax.nn.softmax(scores, axis=-1).astype(jnp.bfloat16)
    mixed_heads = jnp.einsum(
        "kgqs,skd->qkgd", attn_probs, values, preferred_element_type=jnp.float32
    )
    return mixed_heads.reshape(length, q_heads * head_dim).astype(jnp.bfloat16)


def ring_position(index, n):
    odd = lax.rem(index, 2)
    half = lax.div(index, 2)
    return (1 - odd) * half + odd * (n - 1 - half)


def ring_index(position, n):
    back = lax.div(position, n // 2)
    return (1 - back) * 2 * position + back * (2 * (n - 1 - position) + 1)


def pieces(slots):
    half = slots // 2
    out = []
    for direction, first, count in ((0, 0, half), (1, half, slots - half)):
        cuts = 5 if count % 5 == 0 else 1
        size = count // cuts
        out.append([(first + i * size, size) for i in range(cuts)])
    return out


def enter(neighbours, axis="fsdp"):
    barrier = pltpu.get_barrier_semaphore()
    for neighbour in neighbours:
        pl.semaphore_signal(
            barrier, inc=1, device_id={axis: neighbour}, device_id_type=pl.DeviceIdType.MESH
        )
    pl.semaphore_wait(barrier, len(neighbours))


def gather_kernel(n, slots, grid_qkv, grid_out, slot_ref, w_ref, p_ref, tokens_ref, gain_ref,
                  proj_ref, d_proj_ref, wo_ref, po_ref, normed_t_ref, held_w, held_p, matrix,
                  normed, send_sem, recv_sem):
    me = lax.axis_index("fsdp")
    pos = ring_position(me, n)
    right = ring_index(lax.rem(pos + 1, n), n)
    left = ring_index(lax.rem(pos + n - 1, n), n)
    towards = (right, left)
    enter((left, right))
    parts = pieces(slots)
    arrays = ((w_ref, held_w), (p_ref, held_p))

    def copy(which, step, direction, j):
        own, held = arrays[which]
        first, size = parts[direction][j]
        shift = n - step if direction == 0 else step
        origin = ring_index(lax.rem(pos + shift, n), n)
        there = held.at[pl.ds(origin * slots + first, size)]
        here = own.at[pl.ds(first, size)] if step == 0 else there
        return pltpu.make_async_remote_copy(
            src_ref=here,
            dst_ref=there,
            send_sem=send_sem.at[which, step, direction, j],
            recv_sem=recv_sem.at[which, step, direction, j],
            device_id={"fsdp": towards[direction]},
            device_id_type=pl.DeviceIdType.MESH,
        )

    def arrival(which, step, direction, j):
        first, size = parts[direction][j]
        own, held = arrays[which]
        shift = n - step - 1 if direction == 0 else step + 1
        origin = ring_index(lax.rem(pos + shift, n), n)
        there = held.at[pl.ds(origin * slots + first, size)]
        pltpu.make_async_remote_copy(
            src_ref=there,
            dst_ref=there,
            send_sem=send_sem.at[which, step, direction, j],
            recv_sem=recv_sem.at[which, step, direction, j],
            device_id={"fsdp": towards[direction]},
            device_id_type=pl.DeviceIdType.MESH,
        ).wait_recv()

    def each():
        for j in range(max(len(parts[0]), len(parts[1]))):
            for direction in range(2):
                if j < len(parts[direction]):
                    yield direction, j

    def normalize():
        rows = 32

        def some(i, carry):
            here = pl.ds(pl.multiple_of(i * rows, rows), rows)
            values = tokens_ref[here, :].astype(jnp.float32)
            factor = lax.rsqrt(jnp.mean(values * values, axis=-1, keepdims=True) + EPS)
            normed[here, :] = (values * factor * gain_ref[...]).astype(jnp.bfloat16)
            return carry

        lax.fori_loop(0, normed.shape[0] // rows, some, 0)

    def transpose():
        edge = held_w.shape[-1]

        def some(i, carry):
            here = pl.ds(pl.multiple_of(i * edge, edge), edge)
            normed_t_ref[here, :] = normed[:, here].T
            return carry

        lax.fori_loop(0, normed.shape[1] // edge, some, 0)

    def project(result_ref):
        rows = 256

        def some(i, carry):
            here = pl.ds(pl.multiple_of(i * rows, rows), rows)
            result_ref[here, :] = jnp.dot(
                normed[here, :], matrix[...], preferred_element_type=jnp.float32
            )
            return carry

        lax.fori_loop(0, normed.shape[0] // rows, some, 0)

    def unpack(which, qkv_ref, out_ref):
        own, held = arrays[which]
        rows, cols = grid_qkv
        edge = held.shape[-1]

        def qkv_row(i, carry):
            for c in range(cols):
                qkv_ref[pl.ds(pl.multiple_of(i * edge, edge), edge), c * edge:(c + 1) * edge] = (
                    held[slot_ref[i * cols + c]]
                )
            return carry

        lax.fori_loop(0, rows, qkv_row, 0)
        out_rows, out_cols = grid_out

        def out_col(i, carry):
            for r in range(out_rows):
                out_ref[r * edge:(r + 1) * edge, pl.ds(pl.multiple_of(i * edge, edge), edge)] = (
                    held[slot_ref[rows * cols + r * out_cols + i]]
                )
            return carry

        lax.fori_loop(0, out_cols, out_col, 0)

    def finish(which, qkv_ref, out_ref):
        own, held = arrays[which]
        for direction, j in each():
            arrival(which, n - 2, direction, j)
        held[pl.ds(me * slots, slots)] = own[...]
        unpack(which, qkv_ref, out_ref)

    sent = []
    for which in range(2):
        for step in range(n - 1):
            for direction, j in each():
                if step > 0:
                    arrival(which, step - 1, direction, j)
                one = copy(which, step, direction, j)
                one.start()
                sent.append(one)
            if which == 0 and step == 0:
                normalize()
            if which == 0 and step == 1:
                transpose()
            if which == 1 and step == 0:
                finish(0, matrix, wo_ref)
            if which == 1 and step == 1:
                project(proj_ref)
    finish(1, matrix, po_ref)
    project(d_proj_ref)
    for one in sent:
        one.wait_send()


def gather_weights(slot_of, weights, probes, tokens, gain, n, grid_qkv, grid_out):
    slots, edge, _ = weights.shape
    cuts = max(len(part) for part in pieces(slots))
    length, width = tokens.shape
    proj = jax.ShapeDtypeStruct((length, grid_qkv[1] * edge), jnp.float32)
    turned = jax.ShapeDtypeStruct((width, length), jnp.bfloat16)
    out = jax.ShapeDtypeStruct((grid_out[0] * edge, grid_out[1] * edge), jnp.bfloat16)
    vmem = pl.BlockSpec(memory_space=pltpu.VMEM)
    return pl.pallas_call(
        functools.partial(gather_kernel, n, slots, grid_qkv, grid_out),
        out_shape=(proj, proj, out, out, turned),
        in_specs=[pl.BlockSpec(memory_space=pltpu.SMEM)] + [vmem] * 4,
        out_specs=(vmem,) * 5,
        scratch_shapes=[
            pltpu.VMEM((n * slots, edge, edge), jnp.bfloat16),
            pltpu.VMEM((n * slots, edge, edge), jnp.bfloat16),
            pltpu.VMEM((grid_qkv[0] * edge, grid_qkv[1] * edge), jnp.bfloat16),
            pltpu.VMEM((length, width), jnp.bfloat16),
            pltpu.SemaphoreType.DMA((2, n - 1, 2, cuts)),
            pltpu.SemaphoreType.DMA((2, n - 1, 2, cuts)),
        ],
        compiler_params=pltpu.CompilerParams(
            collective_id=0, has_side_effects=True, vmem_limit_bytes=VMEM_BYTES
        ),
    )(slot_of, weights, probes, tokens, gain)


def gradient_blocks(grid_qkv, grid_out, normed_t_ref, d_proj_ref, mixed_t_ref, weighted_ref,
                    out_ref):
    edge = out_ref.shape[-1]
    rows, cols = grid_qkv
    out_rows, out_cols = grid_out
    group = 2

    out_ref[rows * cols + out_rows * out_cols] = jnp.zeros((edge, edge), out_ref.dtype)

    def qkv_rows(i, carry):
        width = group * edge
        left = normed_t_ref[pl.ds(pl.multiple_of(i * width, width), width), :]
        block = jnp.dot(
            left, d_proj_ref[...], preferred_element_type=jnp.float32
        ).astype(jnp.bfloat16)
        for r in range(group):
            for c in range(cols):
                out_ref[(i * group + r) * cols + c] = block[
                    r * edge:(r + 1) * edge, c * edge:(c + 1) * edge
                ]
        return carry

    lax.fori_loop(0, rows // group, qkv_rows, 0)

    def out_columns(i, carry):
        width = group * edge
        right = weighted_ref[:, pl.ds(pl.multiple_of(i * width, width), width)]
        block = jnp.dot(
            mixed_t_ref[...], right, preferred_element_type=jnp.float32
        ).astype(jnp.bfloat16)
        for r in range(out_rows):
            for c in range(group):
                out_ref[rows * cols + r * out_cols + i * group + c] = block[
                    r * edge:(r + 1) * edge, c * edge:(c + 1) * edge
                ]
        return carry

    lax.fori_loop(0, out_cols // group, out_columns, 0)


def reduce_kernel(n, slots, scale, grid_qkv, grid_out, pick_ref, normed_t_ref, d_proj_ref,
                  mixed_t_ref, weighted_ref, out_ref, grads, begin, held, send_sem, recv_sem):
    me = lax.axis_index("fsdp")
    pos = ring_position(me, n)
    right = ring_index(lax.rem(pos + 1, n), n)
    left = ring_index(lax.rem(pos + n - 1, n), n)
    towards = (right, left)
    enter((left, right))
    parts = pieces(slots)
    gradient_blocks(
        grid_qkv, grid_out, normed_t_ref, d_proj_ref, mixed_t_ref, weighted_ref, grads
    )

    def own(step, direction, j):
        shift = n - 1 - step if direction == 0 else 1 + step
        target = ring_index(lax.rem(pos + shift, n), n)
        return target * slots

    def each_block(direction, j, body):
        first, size = parts[direction][j]

        def some(i, carry):
            body(first + i)
            return carry

        lax.fori_loop(0, size, some, 0)

    def copy(step, direction, j):
        first, size = parts[direction][j]
        here = begin.at[pl.ds(first, size)] if step == 0 else held.at[step - 1, pl.ds(first, size)]
        return pltpu.make_async_remote_copy(
            src_ref=here,
            dst_ref=held.at[step, pl.ds(first, size)],
            send_sem=send_sem.at[step, direction, j],
            recv_sem=recv_sem.at[step, direction, j],
            device_id={"fsdp": towards[direction]},
            device_id_type=pl.DeviceIdType.MESH,
        )

    def each():
        for j in range(max(len(parts[0]), len(parts[1]))):
            for direction in range(2):
                if j < len(parts[direction]):
                    yield direction, j

    sent = {}
    for step in range(n - 1):
        for direction, j in each():
            first, size = parts[direction][j]
            base = own(step, direction, j)
            if step > 0:
                sent[step - 1, direction, j].wait_recv()

                def add(t, step=step, base=base):
                    held[step - 1, t] = (
                        held[step - 1, t].astype(jnp.float32)
                        + grads[pick_ref[base + t]].astype(jnp.float32)
                    ).astype(jnp.bfloat16)

                each_block(direction, j, add)
            else:

                def fill(t, base=base):
                    begin[t] = grads[pick_ref[base + t]]

                each_block(direction, j, fill)
            one = copy(step, direction, j)
            one.start()
            sent[step, direction, j] = one
    for direction, j in each():
        first, size = parts[direction][j]
        sent[n - 2, direction, j].wait_recv()
        base = own(n - 1, direction, j)

        def last(t, base=base):
            out_ref[t] = (
                held[n - 2, t].astype(jnp.float32) + grads[pick_ref[base + t]].astype(jnp.float32)
            ) * scale

        each_block(direction, j, last)
    for one in sent.values():
        one.wait_send()


def reduce_slots(picked, normed_t, d_proj, mixed_t, weighted, n, scale, grid_qkv, grid_out):
    slots = picked.shape[0] // n
    edge = BLK
    total_blocks = grid_qkv[0] * grid_qkv[1] + grid_out[0] * grid_out[1]
    cuts = max(len(part) for part in pieces(slots))
    vmem = pl.BlockSpec(memory_space=pltpu.VMEM)
    return pl.pallas_call(
        functools.partial(reduce_kernel, n, slots, scale, grid_qkv, grid_out),
        out_shape=jax.ShapeDtypeStruct((slots, edge, edge), jnp.float32),
        in_specs=[pl.BlockSpec(memory_space=pltpu.SMEM)] + [vmem] * 4,
        out_specs=vmem,
        scratch_shapes=[
            pltpu.VMEM((total_blocks + 1, edge, edge), jnp.bfloat16),
            pltpu.VMEM((slots, edge, edge), jnp.bfloat16),
            pltpu.VMEM((n - 1, slots, edge, edge), jnp.bfloat16),
            pltpu.SemaphoreType.DMA((n - 1, 2, cuts)),
            pltpu.SemaphoreType.DMA((n - 1, 2, cuts)),
        ],
        compiler_params=pltpu.CompilerParams(
            collective_id=1, has_side_effects=True, vmem_limit_bytes=VMEM_BYTES
        ),
    )(picked, normed_t, d_proj, mixed_t, weighted)


def exchange_kernel(mixed_ref, d_mixed_ref, w_ref, p_ref, curv_ref, weighted_ref, back_ref,
                    terms, near, pair, far, share, rest, send_sem, recv_sem):
    me = lax.axis_index("seq")
    side = lax.rem(me, 2)
    core = me + 1 - 2 * side
    across = me + 2 - 4 * lax.rem(lax.div(me, 2), 2)
    enter((core, across), "seq")
    length, width = terms.shape
    half = width // 2
    chunks = recv_sem.shape[1]
    rows = length // chunks
    mine = pl.ds(pl.multiple_of(side * half, half), half)
    other = pl.ds(pl.multiple_of((1 - side) * half, half), half)

    def block(i):
        return pl.ds(i * rows, rows)

    def copy(stage, i, here, there, target):
        return pltpu.make_async_remote_copy(
            src_ref=here,
            dst_ref=there,
            send_sem=send_sem.at[stage, i],
            recv_sem=recv_sem.at[stage, i],
            device_id={"seq": target},
            device_id_type=pl.DeviceIdType.MESH,
        )

    def terms_of(i):
        tile = width // 4

        def columns(j, carry):
            cols = pl.ds(pl.multiple_of(j * tile, tile), tile)
            terms[block(i), cols] = (
                jnp.dot(d_mixed_ref[block(i), :], w_ref[:, cols], preferred_element_type=jnp.float32)
                + jnp.dot(mixed_ref[block(i), :], p_ref[:, cols], preferred_element_type=jnp.float32)
            ).astype(jnp.bfloat16)
            return carry

        lax.fori_loop(0, 4, columns, 0)

    first = [copy(0, i, terms.at[block(i), other], near.at[block(i)], core) for i in range(chunks)]
    second = [copy(1, i, pair.at[block(i)], far.at[block(i)], across) for i in range(chunks)]
    third = [copy(2, i, share.at[block(i)], rest.at[block(i)], core) for i in range(chunks)]

    def send_pair(i):
        first[i].wait_recv()
        pair[block(i)] = (
            terms[block(i), mine].astype(jnp.float32) + near[block(i)].astype(jnp.float32)
        ).astype(jnp.bfloat16)
        second[i].start()

    def send_share(i):
        second[i].wait_recv()
        total = pair[block(i)].astype(jnp.float32) + far[block(i)].astype(jnp.float32)
        share[block(i)] = (curv_ref[block(i), mine].astype(jnp.float32) * total).astype(
            jnp.bfloat16
        )
        third[i].start()

    def finish(i):
        weighted_ref[block(i), mine] = share[block(i)]
        third[i].wait_recv()
        weighted_ref[block(i), other] = rest[block(i)]
        back_ref[block(i), :] = lax.dot_general(
            weighted_ref[block(i), :],
            w_ref[...],
            (((1,), (1,)), ((), ())),
            preferred_element_type=jnp.float32,
        ).astype(jnp.bfloat16)

    for i in range(chunks):
        terms_of(i)
        first[i].start()
        if i > 0:
            send_pair(i - 1)
    send_pair(chunks - 1)
    for i in range(chunks):
        send_share(i)
        if i > 0:
            finish(i - 1)
    finish(chunks - 1)
    for one in first + second + third:
        one.wait_send()


def exchange(mixed, d_mixed, w_out, p_out, curvature):
    length, width = curvature.shape
    chunks = 4
    vmem = pl.BlockSpec(memory_space=pltpu.VMEM)
    half = pltpu.VMEM((length, width // 2), jnp.bfloat16)
    return pl.pallas_call(
        exchange_kernel,
        out_shape=(
            jax.ShapeDtypeStruct((length, width), jnp.bfloat16),
            jax.ShapeDtypeStruct(mixed.shape, jnp.bfloat16),
        ),
        in_specs=[vmem] * 5,
        out_specs=(vmem, vmem),
        scratch_shapes=[
            pltpu.VMEM((length, width), jnp.bfloat16),
            half,
            half,
            half,
            half,
            half,
            pltpu.SemaphoreType.DMA((3, chunks)),
            pltpu.SemaphoreType.DMA((3, chunks)),
        ],
        compiler_params=pltpu.CompilerParams(
            collective_id=2, has_side_effects=True, vmem_limit_bytes=VMEM_BYTES
        ),
    )(mixed, d_mixed, w_out, p_out, curvature)


def local(tokens, norm_gain, curvature, weight_slots, probe_slots, block_counts):
    n_columns = lax.axis_size("seq")
    n_owners = lax.axis_size("fsdp")
    q_heads = HQ // n_columns
    kv_heads = HK // n_columns
    row_blocks = D // BLK
    qkv_cols = (q_heads + 2 * kv_heads) * HD // BLK
    out_rows = q_heads * HD // BLK
    grid_qkv, grid_out = (row_blocks, qkv_cols), (out_rows, row_blocks)
    total_blocks = row_blocks * qkv_cols + out_rows * row_blocks
    slots = weight_slots.shape[1]
    length = tokens.shape[1]
    counts = block_counts[0]
    range_ends = jnp.cumsum(counts)
    starts = range_ends - counts
    owner_ids = jnp.arange(n_owners, dtype=jnp.int32)
    block_ids = jnp.arange(total_blocks, dtype=jnp.int32)
    owners = jnp.sum((range_ends[None, :] <= block_ids[:, None]).astype(jnp.int32), axis=1)
    first_block = jnp.sum(
        jnp.where(owners[:, None] == owner_ids[None, :], starts[None, :], 0), axis=1
    )
    slot_of = (owners * slots + block_ids - first_block).astype(jnp.int32)
    projected, d_projected, w_out, p_out, normed_t = gather_weights(
        slot_of,
        weight_slots[0],
        probe_slots[0],
        tokens[0],
        norm_gain[None, :],
        n_owners,
        grid_qkv,
        grid_out,
    )
    cosine, sine = rotary(length, HD)

    def inner(projected):
        return attention(projected, cosine, sine, q_heads, kv_heads)

    mixed, d_mixed = jax.jvp(inner, (projected,), (d_projected,))
    weighted, back_mixed = exchange(mixed, d_mixed, w_out, p_out, curvature[0])
    mixed_again, pullback = jax.vjp(inner, projected)
    (back_projected,) = pullback(back_mixed)
    slot_index = jnp.arange(n_owners * slots, dtype=jnp.int32)
    place = slot_index % slots
    owner_hot = (slot_index // slots)[:, None] == owner_ids[None, :]
    owner_first = jnp.sum(jnp.where(owner_hot, starts[None, :], 0), axis=1)
    own_count = jnp.sum(jnp.where(owner_hot, counts[None, :], 0), axis=1)
    picked = jnp.where(place < own_count, owner_first + place, total_blocks).astype(jnp.int32)
    scaled = reduce_slots(
        picked,
        normed_t,
        back_projected.astype(jnp.bfloat16),
        mixed_again.T,
        weighted,
        n_owners,
        (length * n_owners) ** -0.5,
        grid_qkv,
        grid_out,
    )
    return scaled.reshape(1, slots, BLK, BLK)


def spot():
    f = lax.axis_index("fsdp")
    s = lax.axis_index("seq")
    return lax.div(f, 2), lax.rem(f, 2), lax.div(s, 2), lax.rem(s, 2)


def device(z, y, x, c):
    return {"fsdp": 2 * z + y, "seq": 2 * x + c}


def mirrored(z, c, planes):
    return z + c * (planes - 1 - 2 * z)


def greet(peers):
    barrier = pltpu.get_barrier_semaphore()
    for peer in peers:
        pl.semaphore_signal(barrier, inc=1, device_id=peer, device_id_type=pl.DeviceIdType.MESH)
    pl.semaphore_wait(barrier, len(peers))


def shard_columns(x, j, width):
    return x * (width // 4) + j * (width // 8), width // 2 + j * (width // 4) + x * (width // 8)


def cut_count(slots):
    return 5 if slots % 5 == 0 else 1


def gather_grid_kernel(n, slots, grid_qkv, grid_out, slot_ref, w_ref, p_ref, tokens_ref, gain_ref,
                       curv_ref, proj_out, d_proj_ref, wo_out, po_out, normed_t_out, curv_out,
                       held_w, held_p, matrix, normed, wo_ref, po_ref, normed_t_ref, proj_ref,
                       curv_part, turned, swap_send, swap_recv, in_sem, out_sem, send_y, send_core, send_z, recv, tok_send,
                       tok_recv, relay_send, relay_recv, curv_send, curv_recv):
    planes = n // 2
    z, y, x, c = spot()
    zeta = mirrored(z, c, planes)
    hub = lax.rem(zeta, 2) == 0
    spoke = lax.rem(zeta, 2) == 1
    mate = z + 1 - 2 * lax.rem(z, 2)
    y_peer = device(z, 1 - y, x, c)
    x_peer = device(z, y, 1 - x, c)
    core_peer = device(z, y, x, 1 - c)
    z_peer = device(mate, y, x, c)
    row = [device(lax.rem(z + i, planes), y, x, c) for i in range(1, planes)]
    cuts = cut_count(slots)
    size = slots // cuts
    own = (w_ref, p_ref)
    held = (held_w, held_p)
    me = 2 * z + y

    def own_load(which):
        here = held[which].at[pl.ds(me * slots, slots)]
        return pltpu.make_async_copy(own[which], here, in_sem.at[which])

    def token_load():
        return pltpu.make_async_copy(tokens_ref, normed, in_sem.at[2])

    stores = [
        pltpu.make_async_copy(here, there, out_sem.at[i])
        for i, (here, there) in enumerate((
            (normed_t_ref, normed_t_out), (proj_ref, proj_out), (wo_ref, wo_out),
            (po_ref, po_out), (curv_part, curv_out),
        ))
    ]

    @pl.when(hub)
    def _():
        token_load().start()
        for which in range(2):
            own_load(which).start()

    greet(row + [core_peer, y_peer, x_peer])
    tok_cuts = tok_send.shape[0]
    half = normed.shape[0] // 2
    tok_rows = half // tok_cuts
    width = normed.shape[1]
    part = width // 8

    def at(zeta_at):
        return mirrored(zeta_at, c, planes)

    def spread(which, d, j):
        return held[which].at[pl.ds(d * slots + j * size, size)]

    def move(src, which, d, j, peer, sem):
        return pltpu.make_async_remote_copy(
            src_ref=src,
            dst_ref=spread(which, d, j),
            send_sem=sem,
            recv_sem=recv.at[d, which * cuts + j],
            device_id=peer,
            device_id_type=pl.DeviceIdType.MESH,
        )

    def own_chunk(which, j):
        return own[which].at[pl.ds(j * size, size)]

    def arrive(which, d, j):
        move(spread(which, d, j), which, d, j, core_peer, send_y.at[0, 0]).wait_recv()

    other_hub = device(at(2 - zeta), y, x, c)
    near_hub = device(at(2), y, x, c)
    end_hub = device(at(0), y, x, c)

    def token_copy(i, rows_half, peer, s_sem, r_sem, src):
        rows = pl.ds(rows_half * half + i * tok_rows, tok_rows)
        return pltpu.make_async_remote_copy(
            src_ref=src.at[rows],
            dst_ref=normed.at[rows],
            send_sem=s_sem.at[i],
            recv_sem=r_sem.at[i],
            device_id=peer,
            device_id_type=pl.DeviceIdType.MESH,
        )

    def curv_copy(i):
        first = shard_columns(x, lax.rem(mate, 2), width)[i]
        return pltpu.make_async_remote_copy(
            src_ref=curv_ref.at[:, pl.ds(pl.multiple_of(first, part), part)],
            dst_ref=curv_part.at[i],
            send_sem=curv_send.at[i],
            recv_sem=curv_recv.at[i],
            device_id=z_peer,
            device_id_type=pl.DeviceIdType.MESH,
        )

    def curv_local(i):
        first = shard_columns(x, lax.rem(z, 2), width)[i]
        return pltpu.make_async_copy(
            curv_ref.at[:, pl.ds(pl.multiple_of(first, part), part)],
            curv_part.at[i],
            curv_recv.at[i],
        )

    def to_z(which, j):
        k = which * cuts + j
        return move(own_chunk(which, j), which, me, j, other_hub, send_z.at[0, k])

    def to_y(which, j):
        k = which * cuts + j
        return move(own_chunk(which, j), which, me, j, y_peer, send_y.at[0, k])

    def to_core(which, j):
        k = which * cuts + j
        return move(own_chunk(which, j), which, me, j, core_peer, send_core.at[0, k])

    def spoke_own(which, j):
        src = own_chunk(which, j)
        k = which * cuts + j
        return (
            move(src, which, me, j, near_hub, send_z.at[0, k]),
            move(src, which, me, j, end_hub, send_z.at[1, k]),
        )

    lead = min(6, 2 * cuts)
    every = [(which, j) for which in range(2) for j in range(cuts)]

    @pl.when(hub)
    def _():
        for k in range(lead):
            to_y(*every[k]).start()
        for k in range(max(len(every), tok_cuts)):
            if k < len(every):
                to_z(*every[k]).start()
            if k < tok_cuts:
                token_copy(k, x, z_peer, tok_send, tok_recv, tokens_ref).start()
        for i in range(2):
            curv_copy(i).start()
            curv_local(i).start()

    @pl.when(spoke)
    def _():
        for one in every:
            for copy in spoke_own(*one):
                copy.start()

    def pass_row(k):
        which, j = every[k]
        to_core(which, j).start()
        for r in range(1, planes):
            d = 2 * at(lax.rem(zeta + r, planes)) + y
            arrive(which, d, j)
            src = spread(which, d, j)
            move(src, which, d, j, y_peer, send_y.at[r, k]).start()
            move(src, which, d, j, core_peer, send_core.at[r, k]).start()
            if r == 1 and k + lead < len(every):
                to_y(*every[k + lead]).start()

    def pass_across(k):
        which, j = every[k]
        for r in range(planes):
            d = 2 * at(lax.rem(zeta + r, planes)) + 1 - y
            arrive(which, d, j)
            move(spread(which, d, j), which, d, j, core_peer, send_core.at[planes + r, k]).start()

    def forward(which, j):
        k = which * cuts + j
        pass_row(k)
        if k not in (0, cuts):
            pass_across(k - 1)
        if k in (cuts - 1, 2 * cuts - 1):
            pass_across(k)

    def step(which, j):
        @pl.when(hub)
        def _():
            forward(which, j)

        @pl.when(spoke)
        def _():
            for d in range(n):
                arrive(which, d, j)

    def normalize():
        rows = 32

        def some(i, carry):
            here = pl.ds(pl.multiple_of(i * rows, rows), rows)
            values = normed[here, :].astype(jnp.float32)
            factor = lax.rsqrt(jnp.mean(values * values, axis=-1, keepdims=True) + EPS)
            normed[here, :] = (values * factor * gain_ref[...]).astype(jnp.bfloat16)
            return carry

        lax.fori_loop(0, normed.shape[0] // rows, some, 0)

    length = normed.shape[0]
    mid = width // 2

    def transpose():
        edge = held_w.shape[-1]

        def some(i, carry):
            here = pl.ds(pl.multiple_of(i * edge, edge), edge)
            mine = pl.ds(pl.multiple_of(c * mid + i * edge, edge), edge)
            other = pl.ds(pl.multiple_of((1 - c) * mid + i * edge, edge), edge)
            normed_t_ref[here, :length] = normed[:, mine].T
            turned[here, :] = normed[:, other].T
            return carry

        lax.fori_loop(0, mid // edge, some, 0)

    swap = pltpu.make_async_remote_copy(
        src_ref=turned,
        dst_ref=normed_t_ref.at[:, pl.ds(length, length)],
        send_sem=swap_send.at[0],
        recv_sem=swap_recv.at[0],
        device_id=core_peer,
        device_id_type=pl.DeviceIdType.MESH,
    )

    def project(result_ref):
        rows = 256

        def some(i, carry):
            here = pl.ds(pl.multiple_of(i * rows, rows), rows)
            result_ref[here, :] = jnp.dot(
                normed[here, :], matrix[...], preferred_element_type=jnp.float32
            )
            return carry

        lax.fori_loop(0, normed.shape[0] // rows, some, 0)

    def unpack_qkv(which):
        rows, cols = grid_qkv
        edge = held_w.shape[-1]

        def qkv_row(i, carry):
            for col in range(cols):
                matrix[pl.ds(pl.multiple_of(i * edge, edge), edge), col * edge:(col + 1) * edge] = (
                    held[which][slot_ref[i * cols + col]]
                )
            return carry

        lax.fori_loop(0, rows, qkv_row, 0)

    def unpack_out(which, out_ref):
        rows, cols = grid_qkv
        out_rows, out_cols = grid_out
        edge = held_w.shape[-1]

        def out_col(i, carry):
            for r in range(out_rows):
                out_ref[r * edge:(r + 1) * edge, pl.ds(pl.multiple_of(i * edge, edge), edge)] = (
                    held[which][slot_ref[rows * cols + r * out_cols + i]]
                )
            return carry

        lax.fori_loop(0, out_cols, out_col, 0)

    def keep_own(which):
        @pl.when(hub)
        def _():
            own_load(which).wait()

    @pl.when(hub)
    def _():
        token_load().wait()

    @pl.when(spoke)
    def _():
        for i in range(tok_cuts):
            token_copy(i, x, z_peer, tok_send, tok_recv, normed).wait_recv()
            token_copy(i, x, x_peer, relay_send, relay_recv, normed).start()
        for i in range(tok_cuts):
            token_copy(i, 1 - x, x_peer, relay_send, relay_recv, normed).wait_recv()
        for i in range(tok_cuts):
            token_copy(i, x, x_peer, relay_send, relay_recv, normed).wait_send()

    normalize()
    for j in range(cuts):
        step(0, j)
        if j == 0:
            transpose()
            swap.start()
    keep_own(0)
    def first_proj():
        project(proj_ref)
        stores[1].start()

    def first_out():
        unpack_out(0, wo_ref)
        stores[2].start()

    todo = [lambda: unpack_qkv(0), first_proj, first_out]
    for j in range(cuts):
        step(1, j)
        if j < cuts - 1 and todo:
            todo.pop(0)()
    while todo:
        todo.pop(0)()
    keep_own(1)
    unpack_out(1, po_ref)
    stores[3].start()

    @pl.when(hub)
    def _():
        for i in range(2):
            curv_local(i).wait()

    @pl.when(spoke)
    def _():
        for i in range(2):
            curv_copy(i).wait_recv()

    stores[4].start()
    swap.wait_recv()
    stores[0].start()
    unpack_qkv(1)
    project(d_proj_ref)

    @pl.when(hub)
    def _():
        for i in range(tok_cuts):
            token_copy(i, x, z_peer, tok_send, tok_recv, tokens_ref).wait_send()
        for i in range(2):
            curv_copy(i).wait_send()
        for k, (which, j) in enumerate(every):
            to_z(which, j).wait_send()
            to_y(which, j).wait_send()
            to_core(which, j).wait_send()
            src = spread(which, me, j)
            for r in range(1, planes):
                move(src, which, me, j, y_peer, send_y.at[r, k]).wait_send()
            for r in range(1, n):
                move(src, which, me, j, core_peer, send_core.at[r, k]).wait_send()

    @pl.when(spoke)
    def _():
        for one in every:
            for copy in spoke_own(*one):
                copy.wait_send()

    swap.wait_send()
    for store in stores:
        store.wait()


def gather_grid(slot_of, weights, probes, tokens, gain, curvature, n, grid_qkv, grid_out):
    slots, edge, _ = weights.shape
    cuts = cut_count(slots)
    length, width = tokens.shape
    proj = jax.ShapeDtypeStruct((length, grid_qkv[1] * edge), jnp.float32)
    turned = jax.ShapeDtypeStruct((width // 2, 2 * length), jnp.bfloat16)
    out = jax.ShapeDtypeStruct((grid_out[0] * edge, grid_out[1] * edge), jnp.bfloat16)
    shard = (2, length, width // 8)
    vmem = pl.BlockSpec(memory_space=pltpu.VMEM)
    anywhere = pl.BlockSpec(memory_space=pl.ANY)
    dma = pltpu.SemaphoreType.DMA
    return pl.pallas_call(
        functools.partial(gather_grid_kernel, n, slots, grid_qkv, grid_out),
        out_shape=(proj, proj, out, out, turned, jax.ShapeDtypeStruct(shard, jnp.bfloat16)),
        in_specs=[pl.BlockSpec(memory_space=pltpu.SMEM)] + [anywhere] * 3 + [vmem, anywhere],
        out_specs=(anywhere, vmem) + (anywhere,) * 4,
        scratch_shapes=[
            pltpu.VMEM((n * slots, edge, edge), jnp.bfloat16),
            pltpu.VMEM((n * slots, edge, edge), jnp.bfloat16),
            pltpu.VMEM((grid_qkv[0] * edge, grid_qkv[1] * edge), jnp.bfloat16),
            pltpu.VMEM((length, width), jnp.bfloat16),
            pltpu.VMEM(out.shape, out.dtype),
            pltpu.VMEM(out.shape, out.dtype),
            pltpu.VMEM(turned.shape, turned.dtype),
            pltpu.VMEM(proj.shape, proj.dtype),
            pltpu.VMEM(shard, jnp.bfloat16),
            pltpu.VMEM((width // 2, length), jnp.bfloat16),
            dma((1,)),
            dma((1,)),
            dma((3,)),
            dma((5,)),
            dma((n // 2, 2 * cuts)),
            dma((n, 2 * cuts)),
            dma((2, 2 * cuts)),
            dma((n, 2 * cuts)),
            dma((4,)),
            dma((4,)),
            dma((4,)),
            dma((4,)),
            dma((2,)),
            dma((2,)),
        ],
        compiler_params=pltpu.CompilerParams(
            collective_id=3, has_side_effects=True, vmem_limit_bytes=GRID_VMEM_BYTES
        ),
    )(slot_of, weights, probes, tokens, gain, curvature)


def turn_tables(length, head_dim):
    half_dim = head_dim // 2
    frequency = np.exp(-np.log(THETA) * 2.0 * np.arange(half_dim) / head_dim).astype(np.float32)
    angles = np.arange(length, dtype=np.float32)[:, None] * frequency[None, :]
    cosine, sine = np.cos(angles), np.sin(angles)
    return (
        jnp.asarray(np.concatenate([cosine, cosine], axis=1), jnp.float32),
        jnp.asarray(np.concatenate([-sine, sine], axis=1), jnp.float32),
    )


def turn(values, cosine, sine):
    return values * cosine + pltpu.roll(values, values.shape[1] // 2, 1) * sine


def attend(heads, proj_ref, d_proj_ref, cos_ref, sin_ref, mixed_ref, d_mixed_ref, mixed_t_ref,
           probs_ref, rot_ref, d_rot):
    length = proj_ref.shape[0]
    hd = cos_ref.shape[1]
    key_at = heads * hd
    val_at = key_at + hd
    scale = hd ** -0.5

    def spin(source, target):
        def some(h, carry):
            here = pl.ds(pl.multiple_of(h * hd, hd), hd)
            target[:, here] = turn(source[:, here], cos_ref[...], sin_ref[...]).astype(jnp.bfloat16)
            return carry

        lax.fori_loop(0, heads + 1, some, 0)
        target[:, val_at:] = source[:, val_at:].astype(jnp.bfloat16)

    spin(proj_ref, rot_ref)
    spin(d_proj_ref, d_rot)
    tile = hd

    def head(h, carry):
        here = pl.ds(pl.multiple_of(h * hd, hd), hd)
        for i in range(length // tile):
            rows = slice(i * tile, (i + 1) * tile)
            span = (i + 1) * tile
            q, dq = rot_ref[rows, here], d_rot[rows, here]
            k, dk = rot_ref[:span, key_at:val_at], d_rot[:span, key_at:val_at]
            v, dv = rot_ref[:span, val_at:], d_rot[:span, val_at:]
            contract = (((1,), (1,)), ((), ()))
            scores = lax.dot_general(q, k, contract, preferred_element_type=jnp.float32) * scale
            slopes = lax.dot_general(
                jnp.concatenate([dq, q], axis=1),
                jnp.concatenate([k, dk], axis=1),
                contract,
                preferred_element_type=jnp.float32,
            ) * scale
            at_row = i * tile + lax.broadcasted_iota(jnp.int32, (tile, span), 0)
            at_col = lax.broadcasted_iota(jnp.int32, (tile, span), 1)
            seen = at_row >= at_col
            scores = jnp.where(seen, scores, NEGATIVE)
            slopes = jnp.where(seen, slopes, 0.0)
            raised = jnp.exp(scores - jnp.max(scores, axis=1, keepdims=True))
            probs = raised / jnp.sum(raised, axis=1, keepdims=True)
            d_probs = probs * (slopes - jnp.sum(probs * slopes, axis=1, keepdims=True))
            probs = probs.astype(jnp.bfloat16)
            d_probs = d_probs.astype(jnp.bfloat16)
            probs_ref[h, rows, :span] = probs
            if span < length:
                probs_ref[h, rows, span:] = jnp.zeros((tile, length - span), jnp.bfloat16)
            mixed = jnp.dot(probs, v, preferred_element_type=jnp.float32).astype(jnp.bfloat16)
            mixed_ref[rows, here] = mixed
            mixed_t_ref[here, rows] = mixed.T
            d_mixed_ref[rows, here] = (
                jnp.dot(d_probs, v, preferred_element_type=jnp.float32)
                + jnp.dot(probs, dv, preferred_element_type=jnp.float32)
            ).astype(jnp.bfloat16)
        return carry

    lax.fori_loop(0, heads, head, 0)


def attend_back(heads, back_ref, probs_ref, rot_ref, cos_ref, sin_ref, out_ref, slope_ref):
    length = back_ref.shape[0]
    hd = cos_ref.shape[1]
    key_at = heads * hd
    val_at = key_at + hd
    scale = hd ** -0.5
    tile = hd

    def unturn(values):
        rounded = values.astype(jnp.bfloat16).astype(jnp.float32)
        return turn(rounded, cos_ref[...], -sin_ref[...]).astype(jnp.bfloat16)

    def head(h, totals):
        here = pl.ds(pl.multiple_of(h * hd, hd), hd)
        key_total, val_total = totals
        for i in range(length // tile):
            rows = slice(i * tile, (i + 1) * tile)
            span = (i + 1) * tile
            back = back_ref[rows, here]
            d_probs = lax.dot_general(
                back, rot_ref[:span, val_at:], (((1,), (1,)), ((), ())),
                preferred_element_type=jnp.float32,
            ).astype(jnp.bfloat16).astype(jnp.float32)
            probs = probs_ref[h, rows, :span].astype(jnp.float32)
            slopes = probs * (d_probs - jnp.sum(probs * d_probs, axis=1, keepdims=True)) * scale
            slope_ref[rows, :span] = slopes.astype(jnp.bfloat16)
            if span < length:
                slope_ref[rows, span:] = jnp.zeros((tile, length - span), jnp.bfloat16)
        slopes = slope_ref[...]
        d_query = jnp.dot(slopes, rot_ref[:, key_at:val_at], preferred_element_type=jnp.float32)
        out_ref[:, here] = unturn(d_query)
        first = (((0,), (0,)), ((), ()))
        key_total = key_total + lax.dot_general(
            rot_ref[:, here], slopes, first, preferred_element_type=jnp.float32
        )
        val_total = val_total + lax.dot_general(
            back_ref[:, here], probs_ref[h], first, preferred_element_type=jnp.float32
        )
        return key_total, val_total

    zero = jnp.zeros((hd, length), jnp.float32)
    key_total, val_total = lax.fori_loop(0, heads, head, (zero, zero))
    out_ref[:, key_at:val_at] = unturn(key_total.T)
    out_ref[:, val_at:] = val_total.T.astype(jnp.bfloat16)


def square_kernel(heads, proj_ref, d_proj_ref, w_out, p_out, curv_ref, cos_ref, sin_ref,
                  weighted_out, back_proj_ref, mixed_t_out, mixed_t, theirs, w_ref, p_ref, mixed_ref, d_mixed_ref,
                  probs, rot, d_rot, slope, back_ref, terms, near_x, near_z, pair_a, pair_b, far_z,
                  far_x, full, load_sem, store_sem, swap_send, swap_recv, send_sem,
                  recv_sem):
    z, y, x, c = spot()
    side = lax.rem(z, 2)
    x_peer = device(z, y, 1 - x, c)
    z_peer = device(z + 1 - 2 * side, y, x, c)
    loads = [
        pltpu.make_async_copy(w_out, w_ref, load_sem.at[0]),
        pltpu.make_async_copy(p_out, p_ref, load_sem.at[1]),
    ]
    for load in loads:
        load.start()
    core_peer = device(z, y, x, 1 - c)
    greet([x_peer, z_peer, core_peer])
    attend(
        heads, proj_ref, d_proj_ref, cos_ref, sin_ref, mixed_ref, d_mixed_ref, mixed_t, probs, rot,
        d_rot,
    )
    length, width = terms.shape
    chunks = recv_sem.shape[1]

    def swap(i, here, there):
        return pltpu.make_async_remote_copy(
            src_ref=here,
            dst_ref=there,
            send_sem=swap_send.at[i],
            recv_sem=swap_recv.at[i],
            device_id=core_peer,
            device_id_type=pl.DeviceIdType.MESH,
        )

    swap_mixed = swap(
        chunks, mixed_t.at[:, pl.ds(0, length)], mixed_t.at[:, pl.ds(length, length)]
    )
    swap_mixed.start()
    for load in loads:
        load.wait()
    quarter, part = width // 4, width // 8
    rows = length // chunks

    def block(i):
        return pl.ds(i * rows, rows)

    def cols(first, count):
        return pl.ds(pl.multiple_of(first, count), count)

    keep_a, give_a = cols(x * quarter, quarter), cols((1 - x) * quarter, quarter)
    keep_b = cols(width // 2 + side * quarter, quarter)
    give_b = cols(width // 2 + (1 - side) * quarter, quarter)
    first_a, first_b = shard_columns(x, side, width)
    own_a, own_b = cols(first_a, part), cols(first_b, part)

    def copy(kind, i, here, there, target):
        return pltpu.make_async_remote_copy(
            src_ref=here,
            dst_ref=there,
            send_sem=send_sem.at[kind, i],
            recv_sem=recv_sem.at[kind, i],
            device_id=target,
            device_id_type=pl.DeviceIdType.MESH,
        )

    def stage(i):
        b = block(i)
        return (
            copy(0, i, terms.at[b, give_a], near_x.at[b], x_peer),
            copy(1, i, terms.at[b, give_b], near_z.at[b], z_peer),
            copy(2, i, pair_a.at[b, cols((1 - side) * part, part)], far_z.at[b], z_peer),
            copy(3, i, pair_b.at[b, cols((1 - x) * part, part)], far_x.at[b], x_peer),
            copy(4, i, full.at[b, own_a], full.at[b, own_a], z_peer),
            copy(5, i, full.at[b, own_b], full.at[b, own_b], x_peer),
            copy(6, i, full.at[b, keep_a], full.at[b, keep_a], x_peer),
            copy(7, i, full.at[b, keep_b], full.at[b, keep_b], z_peer),
        )

    def incoming(kind, i, there):
        copy(kind, i, there, there, x_peer).wait_recv()

    def terms_of(i):
        tile = width // 4

        def columns(j, carry):
            here = pl.ds(pl.multiple_of(j * tile, tile), tile)
            terms[block(i), here] = (
                jnp.dot(d_mixed_ref[block(i), :], w_ref[:, here], preferred_element_type=jnp.float32)
                + jnp.dot(mixed_ref[block(i), :], p_ref[:, here], preferred_element_type=jnp.float32)
            ).astype(jnp.bfloat16)
            return carry

        lax.fori_loop(0, 4, columns, 0)

    plans = [stage(i) for i in range(chunks)]

    def pair_up(i):
        b = block(i)
        for kind, pair, keep, near in ((0, pair_a, keep_a, near_x), (1, pair_b, keep_b, near_z)):
            incoming(kind, i, near.at[b])
            pair[b] = (
                terms[b, keep].astype(jnp.float32) + near[b].astype(jnp.float32)
            ).astype(jnp.bfloat16)
            plans[i][2 + kind].start()

    def weigh(i):
        b = block(i)
        for kind, pair, mine, far, own_cols in (
            (0, pair_a, side, far_z, own_a), (1, pair_b, x, far_x, own_b)
        ):
            incoming(2 + kind, i, far.at[b])
            total = pair[b, cols(mine * part, part)].astype(jnp.float32) + far[b].astype(jnp.float32)
            full[b, own_cols] = (curv_ref[kind, b].astype(jnp.float32) * total).astype(jnp.bfloat16)
            plans[i][4 + kind].start()

    def widen(i):
        b = block(i)
        other_a, other_b = shard_columns(x, 1 - side, width)[0], shard_columns(1 - x, side, width)[1]
        incoming(4, i, full.at[b, cols(other_a, part)])
        plans[i][6].start()
        incoming(5, i, full.at[b, cols(other_b, part)])
        plans[i][7].start()

    mid = width // 2

    def store(i):
        b = block(i)
        return pltpu.make_async_copy(
            full.at[b, cols(c * mid, mid)], weighted_out.at[b], store_sem.at[i]
        )

    def store_theirs(i):
        there = weighted_out.at[pl.ds(length + i * rows, rows)]
        return pltpu.make_async_copy(theirs.at[block(i)], there, store_sem.at[chunks + i])

    def swap_weighted(i):
        b = block(i)
        return swap(i, full.at[b, cols((1 - c) * mid, mid)], theirs.at[b])

    def finish(i):
        b = block(i)
        incoming(6, i, full.at[b, give_a])
        incoming(7, i, full.at[b, give_b])
        store(i).start()
        swap_weighted(i).start()
        back_ref[b, :] = lax.dot_general(
            full[b, :], w_ref[...], (((1,), (1,)), ((), ())), preferred_element_type=jnp.float32
        ).astype(jnp.bfloat16)

    for i in range(chunks + 3):
        if i < chunks:
            terms_of(i)
            plans[i][0].start()
            plans[i][1].start()
        if 0 <= i - 1 < chunks:
            pair_up(i - 1)
        if 0 <= i - 2 < chunks:
            weigh(i - 2)
        if 0 <= i - 3 < chunks:
            widen(i - 3)
    for i in range(chunks):
        finish(i)
    swap_mixed.wait_recv()
    store_mixed = pltpu.make_async_copy(mixed_t, mixed_t_out, store_sem.at[2 * chunks])
    store_mixed.start()
    for i in range(chunks):
        swap_weighted(i).wait_recv()
        store_theirs(i).start()
    attend_back(heads, back_ref, probs, rot, cos_ref, sin_ref, back_proj_ref, slope)
    store_mixed.wait()
    for i in range(chunks):
        store(i).wait()
        store_theirs(i).wait()
        swap_weighted(i).wait_send()
    swap_mixed.wait_send()
    for plan in plans:
        for one in plan:
            one.wait_send()


def square_exchange(projected, d_projected, w_out, p_out, curvature, cosine, sine, heads):
    length, inputs = projected.shape
    inner, width = w_out.shape
    chunks = 4
    half = jnp.bfloat16
    vmem = pl.BlockSpec(memory_space=pltpu.VMEM)
    anywhere = pl.BlockSpec(memory_space=pl.ANY)
    quarter = pltpu.VMEM((length, width // 4), half)
    part = pltpu.VMEM((length, width // 8), half)
    whole = pltpu.VMEM((length, width), half)
    narrow = pltpu.VMEM((length, inner), half)
    return pl.pallas_call(
        functools.partial(square_kernel, heads),
        out_shape=(
            jax.ShapeDtypeStruct((2 * length, width // 2), half),
            jax.ShapeDtypeStruct((length, inputs), half),
            jax.ShapeDtypeStruct((inner, 2 * length), half),
        ),
        in_specs=[vmem] * 2 + [anywhere] * 2 + [vmem] * 3,
        out_specs=(anywhere, vmem, anywhere),
        scratch_shapes=[
            pltpu.VMEM((inner, 2 * length), half),
            pltpu.VMEM((length, width // 2), half),
            pltpu.VMEM((inner, width), half),
            pltpu.VMEM((inner, width), half),
            narrow,
            narrow,
            pltpu.VMEM((heads, length, length), half),
            pltpu.VMEM((length, inputs), half),
            pltpu.VMEM((length, inputs), half),
            pltpu.VMEM((length, length), half),
            narrow,
            whole, quarter, quarter, quarter, quarter, part, part, whole,
            pltpu.SemaphoreType.DMA((2,)),
            pltpu.SemaphoreType.DMA((2 * chunks + 1,)),
            pltpu.SemaphoreType.DMA((chunks + 1,)),
            pltpu.SemaphoreType.DMA((chunks + 1,)),
            pltpu.SemaphoreType.DMA((8, chunks)),
            pltpu.SemaphoreType.DMA((8, chunks)),
        ],
        compiler_params=pltpu.CompilerParams(
            collective_id=4, has_side_effects=True, vmem_limit_bytes=GRID_VMEM_BYTES
        ),
    )(projected, d_projected, w_out, p_out, curvature, cosine, sine)


def reduce_grid_kernel(n, slots, scale, grid_qkv, grid_out, pick_ref, normed_t_in, d_proj_in,
                       mixed_t_ref, weighted_ref, out_ref, d_proj_ref, swap_sem,
                       normed_t_ref, load_sem, grads, begin, across, onward,
                       landed, core_send, core_recv, y_send, y_recv, z_send, z_recv):
    planes = n // 2
    z, y, x, c = spot()
    zeta = mirrored(z, c, planes)
    hub = lax.rem(zeta, 2) == 0
    spoke = lax.rem(zeta, 2) == 1
    late = lax.div(zeta, 2)
    y_peer = device(z, 1 - y, x, c)
    core_peer = device(z, y, x, 1 - c)
    row = [device(lax.rem(z + i, planes), y, x, c) for i in range(1, planes)]
    load = pltpu.make_async_copy(normed_t_in, normed_t_ref, load_sem.at[0])
    load.start()
    own_rows = d_proj_in.shape[0]
    d_proj_ref[:own_rows] = d_proj_in[...]
    greet(row + [core_peer, y_peer])
    swap = pltpu.make_async_remote_copy(
        src_ref=d_proj_in,
        dst_ref=d_proj_ref.at[pl.ds(own_rows, own_rows)],
        send_sem=swap_sem.at[0],
        recv_sem=swap_sem.at[1],
        device_id=core_peer,
        device_id_type=pl.DeviceIdType.MESH,
    )
    swap.start()
    cuts = cut_count(slots)
    size = slots // cuts
    rows, cols = grid_qkv
    out_rows, out_cols = grid_out
    total = rows * cols + out_rows * out_cols
    edge = out_ref.shape[-1]
    legs = core_send.shape[0] - out_rows
    leg_rows = rows // 2 // legs
    group = 2
    giver = 1 - lax.rem(z, 2)

    def core_copy(i):
        if i < out_rows:
            count = out_cols // 2
            here = pl.ds(rows * cols + i * out_cols + giver * count, count)
        else:
            count = leg_rows * cols
            here = pl.ds((giver * legs + i - out_rows) * count, count)
        return pltpu.make_async_remote_copy(
            src_ref=grads.at[here],
            dst_ref=grads.at[here],
            send_sem=core_send.at[i],
            recv_sem=core_recv.at[i],
            device_id=core_peer,
            device_id_type=pl.DeviceIdType.MESH,
        )

    def out_columns(i, carry):
        width = group * edge
        right = weighted_ref[:, pl.ds(pl.multiple_of(i * width, width), width)]
        block = jnp.dot(
            mixed_t_ref[...], right, preferred_element_type=jnp.float32
        ).astype(jnp.bfloat16)
        for r in range(out_rows):
            for k in range(group):
                at = rows * cols + r * out_cols + c * (out_cols // 2) + i * group + k
                grads[at] = block[r * edge:(r + 1) * edge, k * edge:(k + 1) * edge]
        return carry

    def qkv_rows(i, carry):
        width = group * edge
        left = normed_t_ref[pl.ds(pl.multiple_of(i * width, width), width), :]
        block = jnp.dot(
            left, d_proj_ref[...], preferred_element_type=jnp.float32
        ).astype(jnp.bfloat16)
        for r in range(group):
            for k in range(cols):
                grads[(c * (rows // 2) + i * group + r) * cols + k] = block[
                    r * edge:(r + 1) * edge, k * edge:(k + 1) * edge
                ]
        return carry

    def hand_over(i):
        @pl.when(spoke)
        def _():
            core_copy(i).start()

    grads[total] = jnp.zeros((edge, edge), grads.dtype)
    lax.fori_loop(0, out_cols // 2 // group, out_columns, 0)
    for i in range(out_rows):
        hand_over(i)
    load.wait()
    swap.wait()
    for i in range(legs):
        steps = leg_rows // group
        lax.fori_loop(i * steps, (i + 1) * steps, qkv_rows, 0)
        hand_over(out_rows + i)

    def owner(i, at_y):
        first = (3, 2, 1, 0)[i]
        second = (0, 1, 3, 2)[i]
        o = (1 - late) * first + late * second
        return 2 * mirrored(o, c, planes) + at_y

    def block_sum(index):
        return grads[index].astype(jnp.float32)

    def y_copy(i, j):
        here = pl.ds(i * slots + j * size, size)
        return pltpu.make_async_remote_copy(
            src_ref=begin.at[here],
            dst_ref=across.at[here],
            send_sem=y_send.at[i, j],
            recv_sem=y_recv.at[i, j],
            device_id=y_peer,
            device_id_type=pl.DeviceIdType.MESH,
        )

    def z_copy(i, j):
        goal = (1 - late) * (2, 2, 1)[i] + late * (0, 1, 3)[i]
        buffer = (0, 1, 0)[i]
        return pltpu.make_async_remote_copy(
            src_ref=onward.at[i, pl.ds(j * size, size)],
            dst_ref=landed.at[buffer, pl.ds(j * size, size)],
            send_sem=z_send.at[i, j],
            recv_sem=z_recv.at[buffer, j],
            device_id=device(mirrored(goal, c, planes), y, x, c),
            device_id_type=pl.DeviceIdType.MESH,
        )

    def z_wait(buffer, j):
        here = landed.at[buffer, pl.ds(j * size, size)]
        pltpu.make_async_remote_copy(
            src_ref=here,
            dst_ref=here,
            send_sem=z_send.at[0, j],
            recv_sem=z_recv.at[buffer, j],
            device_id=core_peer,
            device_id_type=pl.DeviceIdType.MESH,
        ).wait_recv()

    def each(j, body):
        def some(t, carry):
            body(j * size + t)
            return carry

        lax.fori_loop(0, size, some, 0)

    @pl.when(hub)
    def _():
        for i in range(out_rows + legs):
            core_copy(i).wait_recv()
        def start(i, j):
            base = owner(i, 1 - y) * slots

            def fill(t):
                begin[i * slots + t] = grads[pick_ref[base + t]]

            each(j, fill)
            y_copy(i, j).start()

        def go(i, j):
            base = owner(i, y) * slots

            def value(t):
                return block_sum(pick_ref[base + t]) + across[i * slots + t].astype(jnp.float32)

            def pass_on(t):
                onward[i, t] = value(t).astype(jnp.bfloat16)

            def join_on(t):
                onward[i, t] = (value(t) + landed[0, t].astype(jnp.float32)).astype(jnp.bfloat16)

            def last(t):
                out_ref[t] = (value(t) + landed[late, t].astype(jnp.float32)) * scale

            y_copy(i, j).wait_recv()
            if i < 2:
                each(j, pass_on)
                z_copy(i, j).start()
            elif i == 2:

                @pl.when(late == 0)
                def _():
                    each(j, pass_on)

                @pl.when(late == 1)
                def _():
                    z_wait(0, j)
                    each(j, join_on)

                z_copy(i, j).start()
            else:
                z_wait(late, j)
                each(j, last)

        for i in range(planes + 1):

            def turn_round(j, carry, i=i):
                if i < planes:
                    start(i, j)
                if i > 0:
                    go(i - 1, j)
                return carry

            lax.fori_loop(0, cuts, turn_round, 0)

        def close(j, carry):
            for i in range(planes):
                y_copy(i, j).wait_send()
            for i in range(3):
                z_copy(i, j).wait_send()
            return carry

        lax.fori_loop(0, cuts, close, 0)

    @pl.when(spoke)
    def _():
        @pl.when(zeta == 1)
        def _():
            def go(j, carry):
                z_wait(0, j)
                z_wait(1, j)

                def last(t):
                    out_ref[t] = (
                        landed[0, t].astype(jnp.float32) + landed[1, t].astype(jnp.float32)
                    ) * scale

                each(j, last)
                return carry

            lax.fori_loop(0, cuts, go, 0)

        @pl.when(zeta == 3)
        def _():
            def go(j, carry):
                z_wait(0, j)

                def last(t):
                    out_ref[t] = landed[0, t].astype(jnp.float32) * scale

                each(j, last)
                return carry

            lax.fori_loop(0, cuts, go, 0)

        for i in range(out_rows + legs):
            core_copy(i).wait_send()


def reduce_grid(picked, normed_t, d_proj, mixed_t, weighted, n, scale, grid_qkv, grid_out):
    slots = picked.shape[0] // n
    edge = BLK
    total_blocks = grid_qkv[0] * grid_qkv[1] + grid_out[0] * grid_out[1]
    cuts = cut_count(slots)
    legs = 4
    vmem = pl.BlockSpec(memory_space=pltpu.VMEM)
    dma = pltpu.SemaphoreType.DMA
    return pl.pallas_call(
        functools.partial(reduce_grid_kernel, n, slots, scale, grid_qkv, grid_out),
        out_shape=jax.ShapeDtypeStruct((slots, edge, edge), jnp.float32),
        in_specs=[pl.BlockSpec(memory_space=pltpu.SMEM), pl.BlockSpec(memory_space=pl.ANY)]
        + [vmem] * 3,
        out_specs=vmem,
        scratch_shapes=[
            pltpu.VMEM((2 * d_proj.shape[0], d_proj.shape[1]), d_proj.dtype),
            dma((2,)),
            pltpu.VMEM(normed_t.shape, normed_t.dtype),
            dma((1,)),
            pltpu.VMEM((total_blocks + 1, edge, edge), jnp.bfloat16),
            pltpu.VMEM((n // 2 * slots, edge, edge), jnp.bfloat16),
            pltpu.VMEM((n // 2 * slots, edge, edge), jnp.bfloat16),
            pltpu.VMEM((3, slots, edge, edge), jnp.bfloat16),
            pltpu.VMEM((2, slots, edge, edge), jnp.bfloat16),
            dma((grid_out[0] + legs,)),
            dma((grid_out[0] + legs,)),
            dma((n // 2, cuts)),
            dma((n // 2, cuts)),
            dma((3, cuts)),
            dma((2, cuts)),
        ],
        compiler_params=pltpu.CompilerParams(
            collective_id=5, has_side_effects=True, vmem_limit_bytes=GRID_VMEM_BYTES
        ),
    )(picked, normed_t, d_proj, mixed_t, weighted)


def local_grid(tokens, norm_gain, curvature, weight_slots, probe_slots, block_counts):
    n_columns = lax.axis_size("seq")
    n_owners = lax.axis_size("fsdp")
    q_heads = HQ // n_columns
    kv_heads = HK // n_columns
    row_blocks = D // BLK
    qkv_cols = (q_heads + 2 * kv_heads) * HD // BLK
    out_rows = q_heads * HD // BLK
    grid_qkv, grid_out = (row_blocks, qkv_cols), (out_rows, row_blocks)
    total_blocks = row_blocks * qkv_cols + out_rows * row_blocks
    slots = weight_slots.shape[1]
    length = tokens.shape[1]
    z, _, _, c = spot()
    theirs = lax.ppermute(block_counts, "seq", [(i, i ^ 1) for i in range(n_columns)])
    counts = jnp.where(lax.rem(z, 2) == c, block_counts, theirs)[0]
    range_ends = jnp.cumsum(counts)
    starts = range_ends - counts
    owner_ids = jnp.arange(n_owners, dtype=jnp.int32)
    block_ids = jnp.arange(total_blocks, dtype=jnp.int32)
    owners = jnp.sum((range_ends[None, :] <= block_ids[:, None]).astype(jnp.int32), axis=1)
    first_block = jnp.sum(
        jnp.where(owners[:, None] == owner_ids[None, :], starts[None, :], 0), axis=1
    )
    slot_of = (owners * slots + block_ids - first_block).astype(jnp.int32)
    projected, d_projected, w_out, p_out, normed_t, curv_part = gather_grid(
        slot_of,
        weight_slots[0],
        probe_slots[0],
        tokens[0],
        norm_gain[None, :],
        curvature[0],
        n_owners,
        grid_qkv,
        grid_out,
    )
    cosine, sine = turn_tables(length, HD)
    weighted, back_projected, mixed_t = square_exchange(
        projected, d_projected, w_out, p_out, curv_part, cosine, sine, q_heads
    )
    slot_index = jnp.arange(n_owners * slots, dtype=jnp.int32)
    place = slot_index % slots
    owner_hot = (slot_index // slots)[:, None] == owner_ids[None, :]
    owner_first = jnp.sum(jnp.where(owner_hot, starts[None, :], 0), axis=1)
    own_count = jnp.sum(jnp.where(owner_hot, counts[None, :], 0), axis=1)
    picked = jnp.where(place < own_count, owner_first + place, total_blocks).astype(jnp.int32)
    scaled = reduce_grid(
        picked,
        normed_t,
        back_projected,
        mixed_t,
        weighted,
        n_owners,
        (length * n_owners) ** -0.5,
        grid_qkv,
        grid_out,
    )
    return scaled.reshape(1, slots, BLK, BLK)


def solution(mesh):
    in_specs = (
        P("fsdp", None, None),
        P(),
        P("fsdp", None, None),
        P("seq", "fsdp", None, None),
        P("seq", "fsdp", None, None),
        P("seq", None),
    )
    out_specs = P("seq", "fsdp", None, None)
    body = local_grid if mesh.shape["fsdp"] == 8 and mesh.shape["seq"] == 4 else local
    return jax.shard_map(body, mesh=mesh, in_specs=in_specs, out_specs=out_specs, check_vma=False)
```

```python
import functools

import jax
import jax.numpy as jnp
import numpy as np
from jax import lax
from jax.experimental import pallas as pl
from jax.experimental.pallas import tpu as pltpu
from jax.sharding import PartitionSpec as P

D = 4096
HQ = 16
HK = 4
HD = 128
BLK = 128


THETA = 500000.0
EPS = 1e-05
NEGATIVE = -1e30


def rotary(length, head_dim):
    half_dim = head_dim // 2
    frequency = jnp.exp(-jnp.log(THETA) * 2.0 * jnp.arange(half_dim, dtype=jnp.float32) / head_dim)
    angles = jnp.arange(length, dtype=jnp.float32)[:, None] * frequency[None, :]
    return (jnp.cos(angles)[:, None, :], jnp.sin(angles)[:, None, :])


def rotate(field_in, cosine, sine):
    half_dim = field_in.shape[-1] // 2
    first_half = field_in[..., :half_dim]
    second = field_in[..., half_dim:]
    return jnp.concatenate(
        [first_half * cosine - second * sine, second * cosine + first_half * sine], axis=-1
    )


VMEM_BYTES = 62 * 1024 * 1024
GRID_VMEM_BYTES = 67043328


def attention(projected, cosine, sine, q_heads, kv_heads):
    length = projected.shape[0]
    head_dim = projected.shape[1] // (q_heads + 2 * kv_heads)
    q_end = q_heads * head_dim
    k_end = q_end + kv_heads * head_dim
    queries = rotate(projected[:, :q_end].reshape(length, q_heads, head_dim), cosine, sine).astype(
        jnp.bfloat16
    )
    key_rows = rotate(
        projected[:, q_end:k_end].reshape(length, kv_heads, head_dim), cosine, sine
    ).astype(jnp.bfloat16)
    values = projected[:, k_end:].reshape(length, kv_heads, head_dim).astype(jnp.bfloat16)
    queries = queries.reshape(length, kv_heads, q_heads // kv_heads, head_dim)
    scores = jnp.einsum(
        "qkgd,skd->kgqs", queries, key_rows, preferred_element_type=jnp.float32
    ) * head_dim ** (-0.5)
    causal = jnp.arange(length)[:, None] >= jnp.arange(length)[None, :]
    scores = jnp.where(causal, scores, NEGATIVE)
    attn_probs = jax.nn.softmax(scores, axis=-1).astype(jnp.bfloat16)
    mixed_heads = jnp.einsum(
        "kgqs,skd->qkgd", attn_probs, values, preferred_element_type=jnp.float32
    )
    return mixed_heads.reshape(length, q_heads * head_dim).astype(jnp.bfloat16)


def ring_position(index, n):
    odd = lax.rem(index, 2)
    half = lax.div(index, 2)
    return (1 - odd) * half + odd * (n - 1 - half)


def ring_index(position, n):
    back = lax.div(position, n // 2)
    return (1 - back) * 2 * position + back * (2 * (n - 1 - position) + 1)


def pieces(slots):
    half = slots // 2
    out = []
    for direction, first, count in ((0, 0, half), (1, half, slots - half)):
        cuts = 5 if count % 5 == 0 else 1
        size = count // cuts
        out.append([(first + i * size, size) for i in range(cuts)])
    return out


def enter(neighbours, axis="fsdp"):
    barrier = pltpu.get_barrier_semaphore()
    for neighbour in neighbours:
        pl.semaphore_signal(
            barrier, inc=1, device_id={axis: neighbour}, device_id_type=pl.DeviceIdType.MESH
        )
    pl.semaphore_wait(barrier, len(neighbours))


def gather_kernel(n, slots, grid_qkv, grid_out, slot_ref, w_ref, p_ref, tokens_ref, gain_ref,
                  proj_ref, d_proj_ref, wo_ref, po_ref, normed_t_ref, held_w, held_p, matrix,
                  normed, send_sem, recv_sem):
    me = lax.axis_index("fsdp")
    pos = ring_position(me, n)
    right = ring_index(lax.rem(pos + 1, n), n)
    left = ring_index(lax.rem(pos + n - 1, n), n)
    towards = (right, left)
    enter((left, right))
    parts = pieces(slots)
    arrays = ((w_ref, held_w), (p_ref, held_p))

    def copy(which, step, direction, j):
        own, held = arrays[which]
        first, size = parts[direction][j]
        shift = n - step if direction == 0 else step
        origin = ring_index(lax.rem(pos + shift, n), n)
        there = held.at[pl.ds(origin * slots + first, size)]
        here = own.at[pl.ds(first, size)] if step == 0 else there
        return pltpu.make_async_remote_copy(
            src_ref=here,
            dst_ref=there,
            send_sem=send_sem.at[which, step, direction, j],
            recv_sem=recv_sem.at[which, step, direction, j],
            device_id={"fsdp": towards[direction]},
            device_id_type=pl.DeviceIdType.MESH,
        )

    def arrival(which, step, direction, j):
        first, size = parts[direction][j]
        own, held = arrays[which]
        shift = n - step - 1 if direction == 0 else step + 1
        origin = ring_index(lax.rem(pos + shift, n), n)
        there = held.at[pl.ds(origin * slots + first, size)]
        pltpu.make_async_remote_copy(
            src_ref=there,
            dst_ref=there,
            send_sem=send_sem.at[which, step, direction, j],
            recv_sem=recv_sem.at[which, step, direction, j],
            device_id={"fsdp": towards[direction]},
            device_id_type=pl.DeviceIdType.MESH,
        ).wait_recv()

    def each():
        for j in range(max(len(parts[0]), len(parts[1]))):
            for direction in range(2):
                if j < len(parts[direction]):
                    yield direction, j

    def normalize():
        rows = 32

        def some(i, carry):
            here = pl.ds(pl.multiple_of(i * rows, rows), rows)
            values = tokens_ref[here, :].astype(jnp.float32)
            factor = lax.rsqrt(jnp.mean(values * values, axis=-1, keepdims=True) + EPS)
            normed[here, :] = (values * factor * gain_ref[...]).astype(jnp.bfloat16)
            return carry

        lax.fori_loop(0, normed.shape[0] // rows, some, 0)

    def transpose():
        edge = held_w.shape[-1]

        def some(i, carry):
            here = pl.ds(pl.multiple_of(i * edge, edge), edge)
            normed_t_ref[here, :] = normed[:, here].T
            return carry

        lax.fori_loop(0, normed.shape[1] // edge, some, 0)

    def project(result_ref):
        rows = 256

        def some(i, carry):
            here = pl.ds(pl.multiple_of(i * rows, rows), rows)
            result_ref[here, :] = jnp.dot(
                normed[here, :], matrix[...], preferred_element_type=jnp.float32
            )
            return carry

        lax.fori_loop(0, normed.shape[0] // rows, some, 0)

    def unpack(which, qkv_ref, out_ref):
        own, held = arrays[which]
        rows, cols = grid_qkv
        edge = held.shape[-1]

        def qkv_row(i, carry):
            for c in range(cols):
                qkv_ref[pl.ds(pl.multiple_of(i * edge, edge), edge), c * edge:(c + 1) * edge] = (
                    held[slot_ref[i * cols + c]]
                )
            return carry

        lax.fori_loop(0, rows, qkv_row, 0)
        out_rows, out_cols = grid_out

        def out_col(i, carry):
            for r in range(out_rows):
                out_ref[r * edge:(r + 1) * edge, pl.ds(pl.multiple_of(i * edge, edge), edge)] = (
                    held[slot_ref[rows * cols + r * out_cols + i]]
                )
            return carry

        lax.fori_loop(0, out_cols, out_col, 0)

    def finish(which, qkv_ref, out_ref):
        own, held = arrays[which]
        for direction, j in each():
            arrival(which, n - 2, direction, j)
        held[pl.ds(me * slots, slots)] = own[...]
        unpack(which, qkv_ref, out_ref)

    sent = []
    for which in range(2):
        for step in range(n - 1):
            for direction, j in each():
                if step > 0:
                    arrival(which, step - 1, direction, j)
                one = copy(which, step, direction, j)
                one.start()
                sent.append(one)
            if which == 0 and step == 0:
                normalize()
            if which == 0 and step == 1:
                transpose()
            if which == 1 and step == 0:
                finish(0, matrix, wo_ref)
            if which == 1 and step == 1:
                project(proj_ref)
    finish(1, matrix, po_ref)
    project(d_proj_ref)
    for one in sent:
        one.wait_send()


def gather_weights(slot_of, weights, probes, tokens, gain, n, grid_qkv, grid_out):
    slots, edge, _ = weights.shape
    cuts = max(len(part) for part in pieces(slots))
    length, width = tokens.shape
    proj = jax.ShapeDtypeStruct((length, grid_qkv[1] * edge), jnp.float32)
    turned = jax.ShapeDtypeStruct((width, length), jnp.bfloat16)
    out = jax.ShapeDtypeStruct((grid_out[0] * edge, grid_out[1] * edge), jnp.bfloat16)
    vmem = pl.BlockSpec(memory_space=pltpu.VMEM)
    return pl.pallas_call(
        functools.partial(gather_kernel, n, slots, grid_qkv, grid_out),
        out_shape=(proj, proj, out, out, turned),
        in_specs=[pl.BlockSpec(memory_space=pltpu.SMEM)] + [vmem] * 4,
        out_specs=(vmem,) * 5,
        scratch_shapes=[
            pltpu.VMEM((n * slots, edge, edge), jnp.bfloat16),
            pltpu.VMEM((n * slots, edge, edge), jnp.bfloat16),
            pltpu.VMEM((grid_qkv[0] * edge, grid_qkv[1] * edge), jnp.bfloat16),
            pltpu.VMEM((length, width), jnp.bfloat16),
            pltpu.SemaphoreType.DMA((2, n - 1, 2, cuts)),
            pltpu.SemaphoreType.DMA((2, n - 1, 2, cuts)),
        ],
        compiler_params=pltpu.CompilerParams(
            collective_id=0, has_side_effects=True, vmem_limit_bytes=VMEM_BYTES
        ),
    )(slot_of, weights, probes, tokens, gain)


def gradient_blocks(grid_qkv, grid_out, normed_t_ref, d_proj_ref, mixed_t_ref, weighted_ref,
                    out_ref):
    edge = out_ref.shape[-1]
    rows, cols = grid_qkv
    out_rows, out_cols = grid_out
    group = 2

    out_ref[rows * cols + out_rows * out_cols] = jnp.zeros((edge, edge), out_ref.dtype)

    def qkv_rows(i, carry):
        width = group * edge
        left = normed_t_ref[pl.ds(pl.multiple_of(i * width, width), width), :]
        block = jnp.dot(
            left, d_proj_ref[...], preferred_element_type=jnp.float32
        ).astype(jnp.bfloat16)
        for r in range(group):
            for c in range(cols):
                out_ref[(i * group + r) * cols + c] = block[
                    r * edge:(r + 1) * edge, c * edge:(c + 1) * edge
                ]
        return carry

    lax.fori_loop(0, rows // group, qkv_rows, 0)

    def out_columns(i, carry):
        width = group * edge
        right = weighted_ref[:, pl.ds(pl.multiple_of(i * width, width), width)]
        block = jnp.dot(
            mixed_t_ref[...], right, preferred_element_type=jnp.float32
        ).astype(jnp.bfloat16)
        for r in range(out_rows):
            for c in range(group):
                out_ref[rows * cols + r * out_cols + i * group + c] = block[
                    r * edge:(r + 1) * edge, c * edge:(c + 1) * edge
                ]
        return carry

    lax.fori_loop(0, out_cols // group, out_columns, 0)


def reduce_kernel(n, slots, scale, grid_qkv, grid_out, pick_ref, normed_t_ref, d_proj_ref,
                  mixed_t_ref, weighted_ref, out_ref, grads, begin, held, send_sem, recv_sem):
    me = lax.axis_index("fsdp")
    pos = ring_position(me, n)
    right = ring_index(lax.rem(pos + 1, n), n)
    left = ring_index(lax.rem(pos + n - 1, n), n)
    towards = (right, left)
    enter((left, right))
    parts = pieces(slots)
    gradient_blocks(
        grid_qkv, grid_out, normed_t_ref, d_proj_ref, mixed_t_ref, weighted_ref, grads
    )

    def own(step, direction, j):
        shift = n - 1 - step if direction == 0 else 1 + step
        target = ring_index(lax.rem(pos + shift, n), n)
        return target * slots

    def each_block(direction, j, body):
        first, size = parts[direction][j]

        def some(i, carry):
            body(first + i)
            return carry

        lax.fori_loop(0, size, some, 0)

    def copy(step, direction, j):
        first, size = parts[direction][j]
        here = begin.at[pl.ds(first, size)] if step == 0 else held.at[step - 1, pl.ds(first, size)]
        return pltpu.make_async_remote_copy(
            src_ref=here,
            dst_ref=held.at[step, pl.ds(first, size)],
            send_sem=send_sem.at[step, direction, j],
            recv_sem=recv_sem.at[step, direction, j],
            device_id={"fsdp": towards[direction]},
            device_id_type=pl.DeviceIdType.MESH,
        )

    def each():
        for j in range(max(len(parts[0]), len(parts[1]))):
            for direction in range(2):
                if j < len(parts[direction]):
                    yield direction, j

    sent = {}
    for step in range(n - 1):
        for direction, j in each():
            first, size = parts[direction][j]
            base = own(step, direction, j)
            if step > 0:
                sent[step - 1, direction, j].wait_recv()

                def add(t, step=step, base=base):
                    held[step - 1, t] = (
                        held[step - 1, t].astype(jnp.float32)
                        + grads[pick_ref[base + t]].astype(jnp.float32)
                    ).astype(jnp.bfloat16)

                each_block(direction, j, add)
            else:

                def fill(t, base=base):
                    begin[t] = grads[pick_ref[base + t]]

                each_block(direction, j, fill)
            one = copy(step, direction, j)
            one.start()
            sent[step, direction, j] = one
    for direction, j in each():
        first, size = parts[direction][j]
        sent[n - 2, direction, j].wait_recv()
        base = own(n - 1, direction, j)

        def last(t, base=base):
            out_ref[t] = (
                held[n - 2, t].astype(jnp.float32) + grads[pick_ref[base + t]].astype(jnp.float32)
            ) * scale

        each_block(direction, j, last)
    for one in sent.values():
        one.wait_send()


def reduce_slots(picked, normed_t, d_proj, mixed_t, weighted, n, scale, grid_qkv, grid_out):
    slots = picked.shape[0] // n
    edge = BLK
    total_blocks = grid_qkv[0] * grid_qkv[1] + grid_out[0] * grid_out[1]
    cuts = max(len(part) for part in pieces(slots))
    vmem = pl.BlockSpec(memory_space=pltpu.VMEM)
    return pl.pallas_call(
        functools.partial(reduce_kernel, n, slots, scale, grid_qkv, grid_out),
        out_shape=jax.ShapeDtypeStruct((slots, edge, edge), jnp.float32),
        in_specs=[pl.BlockSpec(memory_space=pltpu.SMEM)] + [vmem] * 4,
        out_specs=vmem,
        scratch_shapes=[
            pltpu.VMEM((total_blocks + 1, edge, edge), jnp.bfloat16),
            pltpu.VMEM((slots, edge, edge), jnp.bfloat16),
            pltpu.VMEM((n - 1, slots, edge, edge), jnp.bfloat16),
            pltpu.SemaphoreType.DMA((n - 1, 2, cuts)),
            pltpu.SemaphoreType.DMA((n - 1, 2, cuts)),
        ],
        compiler_params=pltpu.CompilerParams(
            collective_id=1, has_side_effects=True, vmem_limit_bytes=VMEM_BYTES
        ),
    )(picked, normed_t, d_proj, mixed_t, weighted)


def exchange_kernel(mixed_ref, d_mixed_ref, w_ref, p_ref, curv_ref, weighted_ref, back_ref,
                    terms, near, pair, far, share, rest, send_sem, recv_sem):
    me = lax.axis_index("seq")
    side = lax.rem(me, 2)
    core = me + 1 - 2 * side
    across = me + 2 - 4 * lax.rem(lax.div(me, 2), 2)
    enter((core, across), "seq")
    length, width = terms.shape
    half = width // 2
    chunks = recv_sem.shape[1]
    rows = length // chunks
    mine = pl.ds(pl.multiple_of(side * half, half), half)
    other = pl.ds(pl.multiple_of((1 - side) * half, half), half)

    def block(i):
        return pl.ds(i * rows, rows)

    def copy(stage, i, here, there, target):
        return pltpu.make_async_remote_copy(
            src_ref=here,
            dst_ref=there,
            send_sem=send_sem.at[stage, i],
            recv_sem=recv_sem.at[stage, i],
            device_id={"seq": target},
            device_id_type=pl.DeviceIdType.MESH,
        )

    def terms_of(i):
        tile = width // 4

        def columns(j, carry):
            cols = pl.ds(pl.multiple_of(j * tile, tile), tile)
            terms[block(i), cols] = (
                jnp.dot(d_mixed_ref[block(i), :], w_ref[:, cols], preferred_element_type=jnp.float32)
                + jnp.dot(mixed_ref[block(i), :], p_ref[:, cols], preferred_element_type=jnp.float32)
            ).astype(jnp.bfloat16)
            return carry

        lax.fori_loop(0, 4, columns, 0)

    first = [copy(0, i, terms.at[block(i), other], near.at[block(i)], core) for i in range(chunks)]
    second = [copy(1, i, pair.at[block(i)], far.at[block(i)], across) for i in range(chunks)]
    third = [copy(2, i, share.at[block(i)], rest.at[block(i)], core) for i in range(chunks)]

    def send_pair(i):
        first[i].wait_recv()
        pair[block(i)] = (
            terms[block(i), mine].astype(jnp.float32) + near[block(i)].astype(jnp.float32)
        ).astype(jnp.bfloat16)
        second[i].start()

    def send_share(i):
        second[i].wait_recv()
        total = pair[block(i)].astype(jnp.float32) + far[block(i)].astype(jnp.float32)
        share[block(i)] = (curv_ref[block(i), mine].astype(jnp.float32) * total).astype(
            jnp.bfloat16
        )
        third[i].start()

    def finish(i):
        weighted_ref[block(i), mine] = share[block(i)]
        third[i].wait_recv()
        weighted_ref[block(i), other] = rest[block(i)]
        back_ref[block(i), :] = lax.dot_general(
            weighted_ref[block(i), :],
            w_ref[...],
            (((1,), (1,)), ((), ())),
            preferred_element_type=jnp.float32,
        ).astype(jnp.bfloat16)

    for i in range(chunks):
        terms_of(i)
        first[i].start()
        if i > 0:
            send_pair(i - 1)
    send_pair(chunks - 1)
    for i in range(chunks):
        send_share(i)
        if i > 0:
            finish(i - 1)
    finish(chunks - 1)
    for one in first + second + third:
        one.wait_send()


def exchange(mixed, d_mixed, w_out, p_out, curvature):
    length, width = curvature.shape
    chunks = 4
    vmem = pl.BlockSpec(memory_space=pltpu.VMEM)
    half = pltpu.VMEM((length, width // 2), jnp.bfloat16)
    return pl.pallas_call(
        exchange_kernel,
        out_shape=(
            jax.ShapeDtypeStruct((length, width), jnp.bfloat16),
            jax.ShapeDtypeStruct(mixed.shape, jnp.bfloat16),
        ),
        in_specs=[vmem] * 5,
        out_specs=(vmem, vmem),
        scratch_shapes=[
            pltpu.VMEM((length, width), jnp.bfloat16),
            half,
            half,
            half,
            half,
            half,
            pltpu.SemaphoreType.DMA((3, chunks)),
            pltpu.SemaphoreType.DMA((3, chunks)),
        ],
        compiler_params=pltpu.CompilerParams(
            collective_id=2, has_side_effects=True, vmem_limit_bytes=VMEM_BYTES
        ),
    )(mixed, d_mixed, w_out, p_out, curvature)


def local(tokens, norm_gain, curvature, weight_slots, probe_slots, block_counts):
    n_columns = lax.axis_size("seq")
    n_owners = lax.axis_size("fsdp")
    q_heads = HQ // n_columns
    kv_heads = HK // n_columns
    row_blocks = D // BLK
    qkv_cols = (q_heads + 2 * kv_heads) * HD // BLK
    out_rows = q_heads * HD // BLK
    grid_qkv, grid_out = (row_blocks, qkv_cols), (out_rows, row_blocks)
    total_blocks = row_blocks * qkv_cols + out_rows * row_blocks
    slots = weight_slots.shape[1]
    length = tokens.shape[1]
    counts = block_counts[0]
    range_ends = jnp.cumsum(counts)
    starts = range_ends - counts
    owner_ids = jnp.arange(n_owners, dtype=jnp.int32)
    block_ids = jnp.arange(total_blocks, dtype=jnp.int32)
    owners = jnp.sum((range_ends[None, :] <= block_ids[:, None]).astype(jnp.int32), axis=1)
    first_block = jnp.sum(
        jnp.where(owners[:, None] == owner_ids[None, :], starts[None, :], 0), axis=1
    )
    slot_of = (owners * slots + block_ids - first_block).astype(jnp.int32)
    projected, d_projected, w_out, p_out, normed_t = gather_weights(
        slot_of,
        weight_slots[0],
        probe_slots[0],
        tokens[0],
        norm_gain[None, :],
        n_owners,
        grid_qkv,
        grid_out,
    )
    cosine, sine = rotary(length, HD)

    def inner(projected):
        return attention(projected, cosine, sine, q_heads, kv_heads)

    mixed, d_mixed = jax.jvp(inner, (projected,), (d_projected,))
    weighted, back_mixed = exchange(mixed, d_mixed, w_out, p_out, curvature[0])
    mixed_again, pullback = jax.vjp(inner, projected)
    (back_projected,) = pullback(back_mixed)
    slot_index = jnp.arange(n_owners * slots, dtype=jnp.int32)
    place = slot_index % slots
    owner_hot = (slot_index // slots)[:, None] == owner_ids[None, :]
    owner_first = jnp.sum(jnp.where(owner_hot, starts[None, :], 0), axis=1)
    own_count = jnp.sum(jnp.where(owner_hot, counts[None, :], 0), axis=1)
    picked = jnp.where(place < own_count, owner_first + place, total_blocks).astype(jnp.int32)
    scaled = reduce_slots(
        picked,
        normed_t,
        back_projected.astype(jnp.bfloat16),
        mixed_again.T,
        weighted,
        n_owners,
        (length * n_owners) ** -0.5,
        grid_qkv,
        grid_out,
    )
    return scaled.reshape(1, slots, BLK, BLK)


def spot():
    f = lax.axis_index("fsdp")
    s = lax.axis_index("seq")
    return lax.div(f, 2), lax.rem(f, 2), lax.div(s, 2), lax.rem(s, 2)


def device(z, y, x, c):
    return {"fsdp": 2 * z + y, "seq": 2 * x + c}


def mirrored(z, c, planes):
    return z + c * (planes - 1 - 2 * z)


def greet(peers):
    barrier = pltpu.get_barrier_semaphore()
    for peer in peers:
        pl.semaphore_signal(barrier, inc=1, device_id=peer, device_id_type=pl.DeviceIdType.MESH)
    pl.semaphore_wait(barrier, len(peers))


def shard_columns(x, j, width):
    return x * (width // 4) + j * (width // 8), width // 2 + j * (width // 4) + x * (width // 8)


def cut_count(slots):
    return 5 if slots % 5 == 0 else 1


def gather_grid_kernel(n, slots, grid_qkv, grid_out, slot_ref, w_ref, p_ref, tokens_ref, gain_ref,
                       curv_ref, proj_out, d_proj_ref, wo_out, po_out, normed_t_out, curv_out,
                       held_w, held_p, matrix, normed, wo_ref, po_ref, normed_t_ref, proj_ref,
                       curv_part, turned, swap_send, swap_recv, in_sem, out_sem, send_y, send_core, send_z, recv, tok_send,
                       tok_recv, relay_send, relay_recv, curv_send, curv_recv):
    planes = n // 2
    z, y, x, c = spot()
    zeta = mirrored(z, c, planes)
    hub = lax.rem(zeta, 2) == 0
    spoke = lax.rem(zeta, 2) == 1
    mate = z + 1 - 2 * lax.rem(z, 2)
    y_peer = device(z, 1 - y, x, c)
    x_peer = device(z, y, 1 - x, c)
    core_peer = device(z, y, x, 1 - c)
    z_peer = device(mate, y, x, c)
    row = [device(lax.rem(z + i, planes), y, x, c) for i in range(1, planes)]
    cuts = cut_count(slots)
    size = slots // cuts
    own = (w_ref, p_ref)
    held = (held_w, held_p)
    me = 2 * z + y

    def own_load(which):
        here = held[which].at[pl.ds(me * slots, slots)]
        return pltpu.make_async_copy(own[which], here, in_sem.at[which])

    def token_load():
        return pltpu.make_async_copy(tokens_ref, normed, in_sem.at[2])

    stores = [
        pltpu.make_async_copy(here, there, out_sem.at[i])
        for i, (here, there) in enumerate((
            (normed_t_ref, normed_t_out), (proj_ref, proj_out), (wo_ref, wo_out),
            (po_ref, po_out), (curv_part, curv_out),
        ))
    ]

    @pl.when(hub)
    def _():
        token_load().start()
        for which in range(2):
            own_load(which).start()

    greet(row + [core_peer, y_peer, x_peer])
    tok_cuts = tok_send.shape[0]
    half = normed.shape[0] // 2
    tok_rows = half // tok_cuts
    width = normed.shape[1]
    part = width // 8

    def at(zeta_at):
        return mirrored(zeta_at, c, planes)

    def spread(which, d, j):
        return held[which].at[pl.ds(d * slots + j * size, size)]

    def move(src, which, d, j, peer, sem):
        return pltpu.make_async_remote_copy(
            src_ref=src,
            dst_ref=spread(which, d, j),
            send_sem=sem,
            recv_sem=recv.at[d, which * cuts + j],
            device_id=peer,
            device_id_type=pl.DeviceIdType.MESH,
        )

    def own_chunk(which, j):
        return own[which].at[pl.ds(j * size, size)]

    def arrive(which, d, j):
        move(spread(which, d, j), which, d, j, core_peer, send_y.at[0, 0]).wait_recv()

    other_hub = device(at(2 - zeta), y, x, c)
    near_hub = device(at(2), y, x, c)
    end_hub = device(at(0), y, x, c)

    def token_copy(i, rows_half, peer, s_sem, r_sem, src):
        rows = pl.ds(rows_half * half + i * tok_rows, tok_rows)
        return pltpu.make_async_remote_copy(
            src_ref=src.at[rows],
            dst_ref=normed.at[rows],
            send_sem=s_sem.at[i],
            recv_sem=r_sem.at[i],
            device_id=peer,
            device_id_type=pl.DeviceIdType.MESH,
        )

    def curv_copy(i):
        first = shard_columns(x, lax.rem(mate, 2), width)[i]
        return pltpu.make_async_remote_copy(
            src_ref=curv_ref.at[:, pl.ds(pl.multiple_of(first, part), part)],
            dst_ref=curv_part.at[i],
            send_sem=curv_send.at[i],
            recv_sem=curv_recv.at[i],
            device_id=z_peer,
            device_id_type=pl.DeviceIdType.MESH,
        )

    def curv_local(i):
        first = shard_columns(x, lax.rem(z, 2), width)[i]
        return pltpu.make_async_copy(
            curv_ref.at[:, pl.ds(pl.multiple_of(first, part), part)],
            curv_part.at[i],
            curv_recv.at[i],
        )

    def to_z(which, j):
        k = which * cuts + j
        return move(own_chunk(which, j), which, me, j, other_hub, send_z.at[0, k])

    def to_y(which, j):
        k = which * cuts + j
        return move(own_chunk(which, j), which, me, j, y_peer, send_y.at[0, k])

    def to_core(which, j):
        k = which * cuts + j
        return move(own_chunk(which, j), which, me, j, core_peer, send_core.at[0, k])

    def spoke_own(which, j):
        src = own_chunk(which, j)
        k = which * cuts + j
        return (
            move(src, which, me, j, near_hub, send_z.at[0, k]),
            move(src, which, me, j, end_hub, send_z.at[1, k]),
        )

    lead = min(6, 2 * cuts)
    every = [(which, j) for which in range(2) for j in range(cuts)]

    @pl.when(hub)
    def _():
        for k in range(lead):
            to_y(*every[k]).start()
        for k in range(max(len(every), tok_cuts)):
            if k < len(every):
                to_z(*every[k]).start()
            if k < tok_cuts:
                token_copy(k, x, z_peer, tok_send, tok_recv, tokens_ref).start()
        for i in range(2):
            curv_copy(i).start()
            curv_local(i).start()

    @pl.when(spoke)
    def _():
        for one in every:
            for copy in spoke_own(*one):
                copy.start()

    def pass_row(k):
        which, j = every[k]
        to_core(which, j).start()
        for r in range(1, planes):
            d = 2 * at(lax.rem(zeta + r, planes)) + y
            arrive(which, d, j)
            src = spread(which, d, j)
            move(src, which, d, j, y_peer, send_y.at[r, k]).start()
            move(src, which, d, j, core_peer, send_core.at[r, k]).start()
            if r == 1 and k + lead < len(every):
                to_y(*every[k + lead]).start()

    def pass_across(k):
        which, j = every[k]
        for r in range(planes):
            d = 2 * at(lax.rem(zeta + r, planes)) + 1 - y
            arrive(which, d, j)
            move(spread(which, d, j), which, d, j, core_peer, send_core.at[planes + r, k]).start()

    def forward(which, j):
        k = which * cuts + j
        pass_row(k)
        if k not in (0, cuts):
            pass_across(k - 1)
        if k in (cuts - 1, 2 * cuts - 1):
            pass_across(k)

    def step(which, j):
        @pl.when(hub)
        def _():
            forward(which, j)

        @pl.when(spoke)
        def _():
            for d in range(n):
                arrive(which, d, j)

    def normalize():
        rows = 32

        def some(i, carry):
            here = pl.ds(pl.multiple_of(i * rows, rows), rows)
            values = normed[here, :].astype(jnp.float32)
            factor = lax.rsqrt(jnp.mean(values * values, axis=-1, keepdims=True) + EPS)
            normed[here, :] = (values * factor * gain_ref[...]).astype(jnp.bfloat16)
            return carry

        lax.fori_loop(0, normed.shape[0] // rows, some, 0)

    length = normed.shape[0]
    mid = width // 2

    def transpose():
        edge = held_w.shape[-1]

        def some(i, carry):
            here = pl.ds(pl.multiple_of(i * edge, edge), edge)
            mine = pl.ds(pl.multiple_of(c * mid + i * edge, edge), edge)
            other = pl.ds(pl.multiple_of((1 - c) * mid + i * edge, edge), edge)
            normed_t_ref[here, :length] = normed[:, mine].T
            turned[here, :] = normed[:, other].T
            return carry

        lax.fori_loop(0, mid // edge, some, 0)

    swap = pltpu.make_async_remote_copy(
        src_ref=turned,
        dst_ref=normed_t_ref.at[:, pl.ds(length, length)],
        send_sem=swap_send.at[0],
        recv_sem=swap_recv.at[0],
        device_id=core_peer,
        device_id_type=pl.DeviceIdType.MESH,
    )

    def project(result_ref):
        rows = 256

        def some(i, carry):
            here = pl.ds(pl.multiple_of(i * rows, rows), rows)
            result_ref[here, :] = jnp.dot(
                normed[here, :], matrix[...], preferred_element_type=jnp.float32
            )
            return carry

        lax.fori_loop(0, normed.shape[0] // rows, some, 0)

    def unpack_qkv(which):
        rows, cols = grid_qkv
        edge = held_w.shape[-1]

        def qkv_row(i, carry):
            for col in range(cols):
                matrix[pl.ds(pl.multiple_of(i * edge, edge), edge), col * edge:(col + 1) * edge] = (
                    held[which][slot_ref[i * cols + col]]
                )
            return carry

        lax.fori_loop(0, rows, qkv_row, 0)

    def unpack_out(which, out_ref):
        rows, cols = grid_qkv
        out_rows, out_cols = grid_out
        edge = held_w.shape[-1]

        def out_col(i, carry):
            for r in range(out_rows):
                out_ref[r * edge:(r + 1) * edge, pl.ds(pl.multiple_of(i * edge, edge), edge)] = (
                    held[which][slot_ref[rows * cols + r * out_cols + i]]
                )
            return carry

        lax.fori_loop(0, out_cols, out_col, 0)

    def keep_own(which):
        @pl.when(hub)
        def _():
            own_load(which).wait()

    @pl.when(hub)
    def _():
        token_load().wait()

    @pl.when(spoke)
    def _():
        for i in range(tok_cuts):
            token_copy(i, x, z_peer, tok_send, tok_recv, normed).wait_recv()
            token_copy(i, x, x_peer, relay_send, relay_recv, normed).start()
        for i in range(tok_cuts):
            token_copy(i, 1 - x, x_peer, relay_send, relay_recv, normed).wait_recv()
        for i in range(tok_cuts):
            token_copy(i, x, x_peer, relay_send, relay_recv, normed).wait_send()

    normalize()
    for j in range(cuts):
        step(0, j)
        if j == 0:
            transpose()
            swap.start()
    keep_own(0)
    def first_proj():
        project(proj_ref)
        stores[1].start()

    def first_out():
        unpack_out(0, wo_ref)
        stores[2].start()

    todo = [lambda: unpack_qkv(0), first_proj, first_out]
    for j in range(cuts):
        step(1, j)
        if j < cuts - 1 and todo:
            todo.pop(0)()
    while todo:
        todo.pop(0)()
    keep_own(1)
    unpack_out(1, po_ref)
    stores[3].start()

    @pl.when(hub)
    def _():
        for i in range(2):
            curv_local(i).wait()

    @pl.when(spoke)
    def _():
        for i in range(2):
            curv_copy(i).wait_recv()

    stores[4].start()
    swap.wait_recv()
    stores[0].start()
    unpack_qkv(1)
    project(d_proj_ref)

    @pl.when(hub)
    def _():
        for i in range(tok_cuts):
            token_copy(i, x, z_peer, tok_send, tok_recv, tokens_ref).wait_send()
        for i in range(2):
            curv_copy(i).wait_send()
        for k, (which, j) in enumerate(every):
            to_z(which, j).wait_send()
            to_y(which, j).wait_send()
            to_core(which, j).wait_send()
            src = spread(which, me, j)
            for r in range(1, planes):
                move(src, which, me, j, y_peer, send_y.at[r, k]).wait_send()
            for r in range(1, n):
                move(src, which, me, j, core_peer, send_core.at[r, k]).wait_send()

    @pl.when(spoke)
    def _():
        for one in every:
            for copy in spoke_own(*one):
                copy.wait_send()

    swap.wait_send()
    for store in stores:
        store.wait()


def gather_grid(slot_of, weights, probes, tokens, gain, curvature, n, grid_qkv, grid_out):
    slots, edge, _ = weights.shape
    cuts = cut_count(slots)
    length, width = tokens.shape
    proj = jax.ShapeDtypeStruct((length, grid_qkv[1] * edge), jnp.float32)
    turned = jax.ShapeDtypeStruct((width // 2, 2 * length), jnp.bfloat16)
    out = jax.ShapeDtypeStruct((grid_out[0] * edge, grid_out[1] * edge), jnp.bfloat16)
    shard = (2, length, width // 8)
    vmem = pl.BlockSpec(memory_space=pltpu.VMEM)
    anywhere = pl.BlockSpec(memory_space=pl.ANY)
    dma = pltpu.SemaphoreType.DMA
    return pl.pallas_call(
        functools.partial(gather_grid_kernel, n, slots, grid_qkv, grid_out),
        out_shape=(proj, proj, out, out, turned, jax.ShapeDtypeStruct(shard, jnp.bfloat16)),
        in_specs=[pl.BlockSpec(memory_space=pltpu.SMEM)] + [anywhere] * 3 + [vmem, anywhere],
        out_specs=(anywhere, vmem) + (anywhere,) * 4,
        scratch_shapes=[
            pltpu.VMEM((n * slots, edge, edge), jnp.bfloat16),
            pltpu.VMEM((n * slots, edge, edge), jnp.bfloat16),
            pltpu.VMEM((grid_qkv[0] * edge, grid_qkv[1] * edge), jnp.bfloat16),
            pltpu.VMEM((length, width), jnp.bfloat16),
            pltpu.VMEM(out.shape, out.dtype),
            pltpu.VMEM(out.shape, out.dtype),
            pltpu.VMEM(turned.shape, turned.dtype),
            pltpu.VMEM(proj.shape, proj.dtype),
            pltpu.VMEM(shard, jnp.bfloat16),
            pltpu.VMEM((width // 2, length), jnp.bfloat16),
            dma((1,)),
            dma((1,)),
            dma((3,)),
            dma((5,)),
            dma((n // 2, 2 * cuts)),
            dma((n, 2 * cuts)),
            dma((2, 2 * cuts)),
            dma((n, 2 * cuts)),
            dma((4,)),
            dma((4,)),
            dma((4,)),
            dma((4,)),
            dma((2,)),
            dma((2,)),
        ],
        compiler_params=pltpu.CompilerParams(
            collective_id=3, has_side_effects=True, vmem_limit_bytes=GRID_VMEM_BYTES
        ),
    )(slot_of, weights, probes, tokens, gain, curvature)


def turn_tables(length, head_dim):
    half_dim = head_dim // 2
    frequency = np.exp(-np.log(THETA) * 2.0 * np.arange(half_dim) / head_dim).astype(np.float32)
    angles = np.arange(length, dtype=np.float32)[:, None] * frequency[None, :]
    cosine, sine = np.cos(angles), np.sin(angles)
    return (
        jnp.asarray(np.concatenate([cosine, cosine], axis=1), jnp.float32),
        jnp.asarray(np.concatenate([-sine, sine], axis=1), jnp.float32),
    )


def turn(values, cosine, sine):
    return values * cosine + pltpu.roll(values, values.shape[1] // 2, 1) * sine


def spin(heads, hd, source, target, cos_ref, sin_ref):
    val_at = (heads + 1) * hd

    def some(h, carry):
        here = pl.ds(pl.multiple_of(h * hd, hd), hd)
        target[:, here] = turn(source[:, here], cos_ref[...], sin_ref[...]).astype(jnp.bfloat16)
        return carry

    lax.fori_loop(0, heads + 1, some, 0)
    target[:, val_at:] = source[:, val_at:].astype(jnp.bfloat16)


def attend(heads, hd, first, tile, mixed_ref, d_mixed_ref, mixed_t_ref, probs_ref, rot_ref, d_rot):
    length = rot_ref.shape[0]
    key_at = heads * hd
    val_at = key_at + hd
    scale = hd ** -0.5
    rows = slice(first, first + tile)
    span = first + tile

    def head(h, carry):
        here = pl.ds(pl.multiple_of(h * hd, hd), hd)
        q, dq = rot_ref[rows, here], d_rot[rows, here]
        k, dk = rot_ref[:span, key_at:val_at], d_rot[:span, key_at:val_at]
        v, dv = rot_ref[:span, val_at:], d_rot[:span, val_at:]
        contract = (((1,), (1,)), ((), ()))
        scores = lax.dot_general(q, k, contract, preferred_element_type=jnp.float32) * scale
        slopes = lax.dot_general(
            jnp.concatenate([dq, q], axis=1),
            jnp.concatenate([k, dk], axis=1),
            contract,
            preferred_element_type=jnp.float32,
        ) * scale
        at_row = first + lax.broadcasted_iota(jnp.int32, (tile, span), 0)
        at_col = lax.broadcasted_iota(jnp.int32, (tile, span), 1)
        seen = at_row >= at_col
        scores = jnp.where(seen, scores, NEGATIVE)
        slopes = jnp.where(seen, slopes, 0.0)
        raised = jnp.exp(scores - jnp.max(scores, axis=1, keepdims=True))
        probs = raised / jnp.sum(raised, axis=1, keepdims=True)
        d_probs = probs * (slopes - jnp.sum(probs * slopes, axis=1, keepdims=True))
        probs = probs.astype(jnp.bfloat16)
        d_probs = d_probs.astype(jnp.bfloat16)
        probs_ref[h, rows, :span] = probs
        if span < length:
            probs_ref[h, rows, span:] = jnp.zeros((tile, length - span), jnp.bfloat16)
        mixed = jnp.dot(probs, v, preferred_element_type=jnp.float32).astype(jnp.bfloat16)
        mixed_ref[rows, here] = mixed
        mixed_t_ref[here, rows] = mixed.T
        d_mixed_ref[rows, here] = (
            jnp.dot(d_probs, v, preferred_element_type=jnp.float32)
            + jnp.dot(probs, dv, preferred_element_type=jnp.float32)
        ).astype(jnp.bfloat16)
        return carry

    lax.fori_loop(0, heads, head, 0)


def attend_back(heads, back_ref, probs_ref, rot_ref, cos_ref, sin_ref, out_ref, slope_ref):
    length = back_ref.shape[0]
    hd = cos_ref.shape[1]
    key_at = heads * hd
    val_at = key_at + hd
    scale = hd ** -0.5
    tile = hd

    def unturn(values):
        rounded = values.astype(jnp.bfloat16).astype(jnp.float32)
        return turn(rounded, cos_ref[...], -sin_ref[...]).astype(jnp.bfloat16)

    def head(h, totals):
        here = pl.ds(pl.multiple_of(h * hd, hd), hd)
        key_total, val_total = totals
        for i in range(length // tile):
            rows = slice(i * tile, (i + 1) * tile)
            span = (i + 1) * tile
            back = back_ref[rows, here]
            d_probs = lax.dot_general(
                back, rot_ref[:span, val_at:], (((1,), (1,)), ((), ())),
                preferred_element_type=jnp.float32,
            ).astype(jnp.bfloat16).astype(jnp.float32)
            probs = probs_ref[h, rows, :span].astype(jnp.float32)
            slopes = probs * (d_probs - jnp.sum(probs * d_probs, axis=1, keepdims=True)) * scale
            slope_ref[rows, :span] = slopes.astype(jnp.bfloat16)
            if span < length:
                slope_ref[rows, span:] = jnp.zeros((tile, length - span), jnp.bfloat16)
        slopes = slope_ref[...]
        d_query = jnp.dot(slopes, rot_ref[:, key_at:val_at], preferred_element_type=jnp.float32)
        out_ref[:, here] = unturn(d_query)
        first = (((0,), (0,)), ((), ()))
        key_total = key_total + lax.dot_general(
            rot_ref[:, here], slopes, first, preferred_element_type=jnp.float32
        )
        val_total = val_total + lax.dot_general(
            back_ref[:, here], probs_ref[h], first, preferred_element_type=jnp.float32
        )
        return key_total, val_total

    zero = jnp.zeros((hd, length), jnp.float32)
    key_total, val_total = lax.fori_loop(0, heads, head, (zero, zero))
    out_ref[:, key_at:val_at] = unturn(key_total.T)
    out_ref[:, val_at:] = val_total.T.astype(jnp.bfloat16)


def square_kernel(heads, proj_ref, d_proj_ref, w_out, p_out, curv_ref, cos_ref, sin_ref,
                  weighted_out, back_proj_ref, mixed_t_out, mixed_t, theirs, w_ref, p_ref, mixed_ref, d_mixed_ref,
                  probs, rot, d_rot, slope, back_ref, terms, near_x, near_z, pair_a, pair_b, far_z,
                  far_x, full, load_sem, store_sem, swap_send, swap_recv, send_sem,
                  recv_sem):
    z, y, x, c = spot()
    side = lax.rem(z, 2)
    x_peer = device(z, y, 1 - x, c)
    z_peer = device(z + 1 - 2 * side, y, x, c)
    loads = [
        pltpu.make_async_copy(w_out, w_ref, load_sem.at[0]),
        pltpu.make_async_copy(p_out, p_ref, load_sem.at[1]),
    ]
    for load in loads:
        load.start()
    core_peer = device(z, y, x, 1 - c)
    greet([x_peer, z_peer, core_peer])
    hd = cos_ref.shape[1]
    spin(heads, hd, proj_ref, rot, cos_ref, sin_ref)
    spin(heads, hd, d_proj_ref, d_rot, cos_ref, sin_ref)
    length, width = terms.shape
    chunks = recv_sem.shape[1]

    def swap(i, here, there):
        return pltpu.make_async_remote_copy(
            src_ref=here,
            dst_ref=there,
            send_sem=swap_send.at[i],
            recv_sem=swap_recv.at[i],
            device_id=core_peer,
            device_id_type=pl.DeviceIdType.MESH,
        )

    swap_mixed = swap(
        chunks, mixed_t.at[:, pl.ds(0, length)], mixed_t.at[:, pl.ds(length, length)]
    )
    rows = length // chunks
    tile = min(hd, length)
    tiles = length // tile
    per = chunks // tiles
    quarter, part = width // 4, width // 8

    def block(i):
        return pl.ds(i * rows, rows)

    def cols(first, count):
        return pl.ds(pl.multiple_of(first, count), count)

    keep_a, give_a = cols(x * quarter, quarter), cols((1 - x) * quarter, quarter)
    keep_b = cols(width // 2 + side * quarter, quarter)
    give_b = cols(width // 2 + (1 - side) * quarter, quarter)
    first_a, first_b = shard_columns(x, side, width)
    own_a, own_b = cols(first_a, part), cols(first_b, part)

    def copy(kind, i, here, there, target):
        return pltpu.make_async_remote_copy(
            src_ref=here,
            dst_ref=there,
            send_sem=send_sem.at[kind, i],
            recv_sem=recv_sem.at[kind, i],
            device_id=target,
            device_id_type=pl.DeviceIdType.MESH,
        )

    def stage(i):
        b = block(i)
        return (
            copy(0, i, terms.at[b, give_a], near_x.at[b], x_peer),
            copy(1, i, terms.at[b, give_b], near_z.at[b], z_peer),
            copy(2, i, pair_a.at[b, cols((1 - side) * part, part)], far_z.at[b], z_peer),
            copy(3, i, pair_b.at[b, cols((1 - x) * part, part)], far_x.at[b], x_peer),
            copy(4, i, full.at[b, own_a], full.at[b, own_a], z_peer),
            copy(5, i, full.at[b, own_b], full.at[b, own_b], x_peer),
            copy(6, i, full.at[b, keep_a], full.at[b, keep_a], x_peer),
            copy(7, i, full.at[b, keep_b], full.at[b, keep_b], z_peer),
        )

    def incoming(kind, i, there):
        copy(kind, i, there, there, x_peer).wait_recv()

    def group(i):
        return pl.ds(i * tile, tile)

    def terms_of(i):
        attend(
            heads, hd, i * tile, tile, mixed_ref, d_mixed_ref, mixed_t, probs, rot, d_rot
        )
        if i == 0:
            for load in loads:
                load.wait()
        if i == tiles - 1:
            swap_mixed.start()
        b = group(i)

        def columns(j, carry):
            here = pl.ds(pl.multiple_of(j * quarter, quarter), quarter)
            terms[b, here] = (
                jnp.dot(d_mixed_ref[b, :], w_ref[:, here], preferred_element_type=jnp.float32)
                + jnp.dot(mixed_ref[b, :], p_ref[:, here], preferred_element_type=jnp.float32)
            ).astype(jnp.bfloat16)
            return carry

        lax.fori_loop(0, 4, columns, 0)

    plans = [stage(i) for i in range(chunks)]

    def pair_up(i):
        b = block(i)
        for kind, pair, keep, near in ((0, pair_a, keep_a, near_x), (1, pair_b, keep_b, near_z)):
            incoming(kind, i, near.at[b])
            pair[b] = (
                terms[b, keep].astype(jnp.float32) + near[b].astype(jnp.float32)
            ).astype(jnp.bfloat16)
            plans[i][2 + kind].start()

    def weigh(i):
        b = block(i)
        for kind, pair, mine, far, own_cols in (
            (0, pair_a, side, far_z, own_a), (1, pair_b, x, far_x, own_b)
        ):
            incoming(2 + kind, i, far.at[b])
            total = pair[b, cols(mine * part, part)].astype(jnp.float32) + far[b].astype(jnp.float32)
            full[b, own_cols] = (curv_ref[kind, b].astype(jnp.float32) * total).astype(jnp.bfloat16)
            plans[i][4 + kind].start()

    def widen(i):
        b = block(i)
        other_a, other_b = shard_columns(x, 1 - side, width)[0], shard_columns(1 - x, side, width)[1]
        incoming(4, i, full.at[b, cols(other_a, part)])
        plans[i][6].start()
        incoming(5, i, full.at[b, cols(other_b, part)])
        plans[i][7].start()

    mid = width // 2

    def store(i):
        b = block(i)
        return pltpu.make_async_copy(
            full.at[b, cols(c * mid, mid)], weighted_out.at[b], store_sem.at[i]
        )

    def store_theirs(i):
        there = weighted_out.at[pl.ds(length + i * rows, rows)]
        return pltpu.make_async_copy(theirs.at[block(i)], there, store_sem.at[chunks + i])

    def swap_weighted(i):
        b = block(i)
        return swap(i, full.at[b, cols((1 - c) * mid, mid)], theirs.at[b])

    def finish(i):
        b = block(i)
        incoming(6, i, full.at[b, give_a])
        incoming(7, i, full.at[b, give_b])
        store(i).start()
        swap_weighted(i).start()
        if i % per == per - 1:
            g = group(i // per)
            back_ref[g, :] = lax.dot_general(
                full[g, :], w_ref[...], (((1,), (1,)), ((), ())), preferred_element_type=jnp.float32
            ).astype(jnp.bfloat16)

    for i in range(chunks + 3):
        if i < chunks:
            if i % per == 0:
                terms_of(i // per)
            plans[i][0].start()
            plans[i][1].start()
        if 0 <= i - 1 < chunks:
            pair_up(i - 1)
        if 0 <= i - 2 < chunks:
            weigh(i - 2)
        if 0 <= i - 3 < chunks:
            widen(i - 3)
    for i in range(chunks):
        finish(i)
    swap_mixed.wait_recv()
    store_mixed = pltpu.make_async_copy(mixed_t, mixed_t_out, store_sem.at[2 * chunks])
    store_mixed.start()
    for i in range(chunks):
        swap_weighted(i).wait_recv()
        store_theirs(i).start()
    attend_back(heads, back_ref, probs, rot, cos_ref, sin_ref, back_proj_ref, slope)
    store_mixed.wait()
    for i in range(chunks):
        store(i).wait()
        store_theirs(i).wait()
        swap_weighted(i).wait_send()
    swap_mixed.wait_send()
    for plan in plans:
        for one in plan:
            one.wait_send()


def square_exchange(projected, d_projected, w_out, p_out, curvature, cosine, sine, heads):
    length, inputs = projected.shape
    inner, width = w_out.shape
    chunks = 4
    half = jnp.bfloat16
    vmem = pl.BlockSpec(memory_space=pltpu.VMEM)
    anywhere = pl.BlockSpec(memory_space=pl.ANY)
    quarter = pltpu.VMEM((length, width // 4), half)
    part = pltpu.VMEM((length, width // 8), half)
    whole = pltpu.VMEM((length, width), half)
    narrow = pltpu.VMEM((length, inner), half)
    return pl.pallas_call(
        functools.partial(square_kernel, heads),
        out_shape=(
            jax.ShapeDtypeStruct((2 * length, width // 2), half),
            jax.ShapeDtypeStruct((length, inputs), half),
            jax.ShapeDtypeStruct((inner, 2 * length), half),
        ),
        in_specs=[vmem] * 2 + [anywhere] * 2 + [vmem] * 3,
        out_specs=(anywhere, vmem, anywhere),
        scratch_shapes=[
            pltpu.VMEM((inner, 2 * length), half),
            pltpu.VMEM((length, width // 2), half),
            pltpu.VMEM((inner, width), half),
            pltpu.VMEM((inner, width), half),
            narrow,
            narrow,
            pltpu.VMEM((heads, length, length), half),
            pltpu.VMEM((length, inputs), half),
            pltpu.VMEM((length, inputs), half),
            pltpu.VMEM((length, length), half),
            narrow,
            whole, quarter, quarter, quarter, quarter, part, part, whole,
            pltpu.SemaphoreType.DMA((2,)),
            pltpu.SemaphoreType.DMA((2 * chunks + 1,)),
            pltpu.SemaphoreType.DMA((chunks + 1,)),
            pltpu.SemaphoreType.DMA((chunks + 1,)),
            pltpu.SemaphoreType.DMA((8, chunks)),
            pltpu.SemaphoreType.DMA((8, chunks)),
        ],
        compiler_params=pltpu.CompilerParams(
            collective_id=4, has_side_effects=True, vmem_limit_bytes=GRID_VMEM_BYTES
        ),
    )(projected, d_projected, w_out, p_out, curvature, cosine, sine)


def reduce_grid_kernel(n, slots, grid_qkv, grid_out, pick_ref, normed_t_in, d_proj_in,
                       mixed_t_ref, weighted_ref, out_ref, d_proj_ref, swap_sem,
                       normed_t_ref, load_sem, grads, begin, across, onward,
                       landed, core_send, core_recv, y_send, y_recv, z_send, z_recv):
    planes = n // 2
    z, y, x, c = spot()
    zeta = mirrored(z, c, planes)
    hub = lax.rem(zeta, 2) == 0
    spoke = lax.rem(zeta, 2) == 1
    late = lax.div(zeta, 2)
    y_peer = device(z, 1 - y, x, c)
    core_peer = device(z, y, x, 1 - c)
    row = [device(lax.rem(z + i, planes), y, x, c) for i in range(1, planes)]
    load = pltpu.make_async_copy(normed_t_in, normed_t_ref, load_sem.at[0])
    load.start()
    own_rows = d_proj_in.shape[0]
    d_proj_ref[:own_rows] = d_proj_in[...]
    greet(row + [core_peer, y_peer])
    swap = pltpu.make_async_remote_copy(
        src_ref=d_proj_in,
        dst_ref=d_proj_ref.at[pl.ds(own_rows, own_rows)],
        send_sem=swap_sem.at[0],
        recv_sem=swap_sem.at[1],
        device_id=core_peer,
        device_id_type=pl.DeviceIdType.MESH,
    )
    swap.start()
    cuts = cut_count(slots)
    size = slots // cuts
    rows, cols = grid_qkv
    out_rows, out_cols = grid_out
    total = rows * cols + out_rows * out_cols
    edge = out_ref.shape[-1]
    legs = core_send.shape[0] - out_rows
    leg_rows = rows // 2 // legs
    group = 2
    giver = 1 - lax.rem(z, 2)

    def core_copy(i):
        if i < out_rows:
            count = out_cols // 2
            here = pl.ds(rows * cols + i * out_cols + giver * count, count)
        else:
            count = leg_rows * cols
            here = pl.ds((giver * legs + i - out_rows) * count, count)
        return pltpu.make_async_remote_copy(
            src_ref=grads.at[here],
            dst_ref=grads.at[here],
            send_sem=core_send.at[i],
            recv_sem=core_recv.at[i],
            device_id=core_peer,
            device_id_type=pl.DeviceIdType.MESH,
        )

    def out_columns(i, carry):
        width = group * edge
        right = weighted_ref[:, pl.ds(pl.multiple_of(i * width, width), width)]
        block = jnp.dot(
            mixed_t_ref[...], right, preferred_element_type=jnp.float32
        ).astype(jnp.bfloat16)
        for r in range(out_rows):
            for k in range(group):
                at = rows * cols + r * out_cols + c * (out_cols // 2) + i * group + k
                grads[at] = block[r * edge:(r + 1) * edge, k * edge:(k + 1) * edge]
        return carry

    def qkv_rows(i, carry):
        width = group * edge
        left = normed_t_ref[pl.ds(pl.multiple_of(i * width, width), width), :]
        block = jnp.dot(
            left, d_proj_ref[...], preferred_element_type=jnp.float32
        ).astype(jnp.bfloat16)
        for r in range(group):
            for k in range(cols):
                grads[(c * (rows // 2) + i * group + r) * cols + k] = block[
                    r * edge:(r + 1) * edge, k * edge:(k + 1) * edge
                ]
        return carry

    def hand_over(i):
        @pl.when(spoke)
        def _():
            core_copy(i).start()

    grads[total] = jnp.zeros((edge, edge), grads.dtype)
    lax.fori_loop(0, out_cols // 2 // group, out_columns, 0)
    for i in range(out_rows):
        hand_over(i)
    load.wait()
    swap.wait()
    for i in range(legs):
        steps = leg_rows // group
        lax.fori_loop(i * steps, (i + 1) * steps, qkv_rows, 0)
        hand_over(out_rows + i)

    def owner(i, at_y):
        first = (3, 2, 1, 0)[i]
        second = (0, 1, 3, 2)[i]
        o = (1 - late) * first + late * second
        return 2 * mirrored(o, c, planes) + at_y

    def block_sum(index):
        return grads[index].astype(jnp.float32)

    def y_copy(i, j):
        here = pl.ds(i * slots + j * size, size)
        return pltpu.make_async_remote_copy(
            src_ref=begin.at[here],
            dst_ref=across.at[here],
            send_sem=y_send.at[i, j],
            recv_sem=y_recv.at[i, j],
            device_id=y_peer,
            device_id_type=pl.DeviceIdType.MESH,
        )

    def z_copy(i, j):
        goal = (1 - late) * (2, 2, 1)[i] + late * (0, 1, 3)[i]
        buffer = (0, 1, 0)[i]
        return pltpu.make_async_remote_copy(
            src_ref=onward.at[i, pl.ds(j * size, size)],
            dst_ref=landed.at[buffer, pl.ds(j * size, size)],
            send_sem=z_send.at[i, j],
            recv_sem=z_recv.at[buffer, j],
            device_id=device(mirrored(goal, c, planes), y, x, c),
            device_id_type=pl.DeviceIdType.MESH,
        )

    def z_wait(buffer, j):
        here = landed.at[buffer, pl.ds(j * size, size)]
        pltpu.make_async_remote_copy(
            src_ref=here,
            dst_ref=here,
            send_sem=z_send.at[0, j],
            recv_sem=z_recv.at[buffer, j],
            device_id=core_peer,
            device_id_type=pl.DeviceIdType.MESH,
        ).wait_recv()

    def each(j, body):
        def some(t, carry):
            body(j * size + t)
            return carry

        lax.fori_loop(0, size, some, 0)

    @pl.when(hub)
    def _():
        for i in range(out_rows + legs):
            core_copy(i).wait_recv()
        def start(i, j):
            base = owner(i, 1 - y) * slots

            def fill(t):
                begin[i * slots + t] = grads[pick_ref[base + t]]

            each(j, fill)
            y_copy(i, j).start()

        def go(i, j):
            base = owner(i, y) * slots

            def value(t):
                return block_sum(pick_ref[base + t]) + across[i * slots + t].astype(jnp.float32)

            def pass_on(t):
                onward[i, t] = value(t).astype(jnp.bfloat16)

            def join_on(t):
                onward[i, t] = (value(t) + landed[0, t].astype(jnp.float32)).astype(jnp.bfloat16)

            def last(t):
                out_ref[t] = (value(t) + landed[late, t].astype(jnp.float32)).astype(jnp.bfloat16)

            y_copy(i, j).wait_recv()
            if i < 2:
                each(j, pass_on)
                z_copy(i, j).start()
            elif i == 2:

                @pl.when(late == 0)
                def _():
                    each(j, pass_on)

                @pl.when(late == 1)
                def _():
                    z_wait(0, j)
                    each(j, join_on)

                z_copy(i, j).start()
            else:
                z_wait(late, j)
                each(j, last)

        for i in range(planes + 1):

            def turn_round(j, carry, i=i):
                if i < planes:
                    start(i, j)
                if i > 0:
                    go(i - 1, j)
                return carry

            lax.fori_loop(0, cuts, turn_round, 0)

        def close(j, carry):
            for i in range(planes):
                y_copy(i, j).wait_send()
            for i in range(3):
                z_copy(i, j).wait_send()
            return carry

        lax.fori_loop(0, cuts, close, 0)

    @pl.when(spoke)
    def _():
        @pl.when(zeta == 1)
        def _():
            def go(j, carry):
                z_wait(0, j)
                z_wait(1, j)

                def last(t):
                    out_ref[t] = (
                        landed[0, t].astype(jnp.float32) + landed[1, t].astype(jnp.float32)
                    ).astype(jnp.bfloat16)

                each(j, last)
                return carry

            lax.fori_loop(0, cuts, go, 0)

        @pl.when(zeta == 3)
        def _():
            def go(j, carry):
                z_wait(0, j)

                def last(t):
                    out_ref[t] = landed[0, t]

                each(j, last)
                return carry

            lax.fori_loop(0, cuts, go, 0)

        for i in range(out_rows + legs):
            core_copy(i).wait_send()


def reduce_grid(picked, normed_t, d_proj, mixed_t, weighted, n, grid_qkv, grid_out):
    slots = picked.shape[0] // n
    edge = BLK
    total_blocks = grid_qkv[0] * grid_qkv[1] + grid_out[0] * grid_out[1]
    cuts = cut_count(slots)
    legs = 4
    vmem = pl.BlockSpec(memory_space=pltpu.VMEM)
    dma = pltpu.SemaphoreType.DMA
    return pl.pallas_call(
        functools.partial(reduce_grid_kernel, n, slots, grid_qkv, grid_out),
        out_shape=jax.ShapeDtypeStruct((slots, edge, edge), jnp.bfloat16),
        in_specs=[pl.BlockSpec(memory_space=pltpu.SMEM), pl.BlockSpec(memory_space=pl.ANY)]
        + [vmem] * 3,
        out_specs=vmem,
        scratch_shapes=[
            pltpu.VMEM((2 * d_proj.shape[0], d_proj.shape[1]), d_proj.dtype),
            dma((2,)),
            pltpu.VMEM(normed_t.shape, normed_t.dtype),
            dma((1,)),
            pltpu.VMEM((total_blocks + 1, edge, edge), jnp.bfloat16),
            pltpu.VMEM((n // 2 * slots, edge, edge), jnp.bfloat16),
            pltpu.VMEM((n // 2 * slots, edge, edge), jnp.bfloat16),
            pltpu.VMEM((3, slots, edge, edge), jnp.bfloat16),
            pltpu.VMEM((2, slots, edge, edge), jnp.bfloat16),
            dma((grid_out[0] + legs,)),
            dma((grid_out[0] + legs,)),
            dma((n // 2, cuts)),
            dma((n // 2, cuts)),
            dma((3, cuts)),
            dma((2, cuts)),
        ],
        compiler_params=pltpu.CompilerParams(
            collective_id=5, has_side_effects=True, vmem_limit_bytes=GRID_VMEM_BYTES
        ),
    )(picked, normed_t, d_proj, mixed_t, weighted)


def local_grid(tokens, norm_gain, curvature, weight_slots, probe_slots, block_counts):
    n_columns = lax.axis_size("seq")
    n_owners = lax.axis_size("fsdp")
    q_heads = HQ // n_columns
    kv_heads = HK // n_columns
    row_blocks = D // BLK
    qkv_cols = (q_heads + 2 * kv_heads) * HD // BLK
    out_rows = q_heads * HD // BLK
    grid_qkv, grid_out = (row_blocks, qkv_cols), (out_rows, row_blocks)
    total_blocks = row_blocks * qkv_cols + out_rows * row_blocks
    slots = weight_slots.shape[1]
    length = tokens.shape[1]
    z, _, _, c = spot()
    theirs = lax.ppermute(block_counts, "seq", [(i, i ^ 1) for i in range(n_columns)])
    counts = jnp.where(lax.rem(z, 2) == c, block_counts, theirs)[0]
    range_ends = jnp.cumsum(counts)
    starts = range_ends - counts
    owner_ids = jnp.arange(n_owners, dtype=jnp.int32)
    block_ids = jnp.arange(total_blocks, dtype=jnp.int32)
    owners = jnp.sum((range_ends[None, :] <= block_ids[:, None]).astype(jnp.int32), axis=1)
    first_block = jnp.sum(
        jnp.where(owners[:, None] == owner_ids[None, :], starts[None, :], 0), axis=1
    )
    slot_of = (owners * slots + block_ids - first_block).astype(jnp.int32)
    projected, d_projected, w_out, p_out, normed_t, curv_part = gather_grid(
        slot_of,
        weight_slots[0],
        probe_slots[0],
        tokens[0],
        norm_gain[None, :],
        curvature[0],
        n_owners,
        grid_qkv,
        grid_out,
    )
    cosine, sine = turn_tables(length, HD)
    weighted, back_projected, mixed_t = square_exchange(
        projected, d_projected, w_out, p_out, curv_part, cosine, sine, q_heads
    )
    slot_index = jnp.arange(n_owners * slots, dtype=jnp.int32)
    place = slot_index % slots
    owner_hot = (slot_index // slots)[:, None] == owner_ids[None, :]
    owner_first = jnp.sum(jnp.where(owner_hot, starts[None, :], 0), axis=1)
    own_count = jnp.sum(jnp.where(owner_hot, counts[None, :], 0), axis=1)
    picked = jnp.where(place < own_count, owner_first + place, total_blocks).astype(jnp.int32)
    summed = reduce_grid(
        picked,
        normed_t,
        back_projected,
        mixed_t,
        weighted,
        n_owners,
        grid_qkv,
        grid_out,
    )
    scale = (length * n_owners) ** -0.5
    return summed.astype(jnp.float32).reshape(1, slots, BLK, BLK) * scale


def solution(mesh):
    in_specs = (
        P("fsdp", None, None),
        P(),
        P("fsdp", None, None),
        P("seq", "fsdp", None, None),
        P("seq", "fsdp", None, None),
        P("seq", None),
    )
    out_specs = P("seq", "fsdp", None, None)
    body = local_grid if mesh.shape["fsdp"] == 8 and mesh.shape["seq"] == 4 else local
    return jax.shard_map(body, mesh=mesh, in_specs=in_specs, out_specs=out_specs, check_vma=False)
```

```python
import functools

import jax
import jax.numpy as jnp
import numpy as np
from jax import lax
from jax.experimental import pallas as pl
from jax.experimental.pallas import tpu as pltpu
from jax.sharding import PartitionSpec as P

D = 4096
HQ = 16
HK = 4
HD = 128
BLK = 128


THETA = 500000.0
EPS = 1e-05
NEGATIVE = -1e30


def rotary(length, head_dim):
    half_dim = head_dim // 2
    frequency = jnp.exp(-jnp.log(THETA) * 2.0 * jnp.arange(half_dim, dtype=jnp.float32) / head_dim)
    angles = jnp.arange(length, dtype=jnp.float32)[:, None] * frequency[None, :]
    return (jnp.cos(angles)[:, None, :], jnp.sin(angles)[:, None, :])


def rotate(field_in, cosine, sine):
    half_dim = field_in.shape[-1] // 2
    first_half = field_in[..., :half_dim]
    second = field_in[..., half_dim:]
    return jnp.concatenate(
        [first_half * cosine - second * sine, second * cosine + first_half * sine], axis=-1
    )


VMEM_BYTES = 62 * 1024 * 1024
GRID_VMEM_BYTES = 67043328


def attention(projected, cosine, sine, q_heads, kv_heads):
    length = projected.shape[0]
    head_dim = projected.shape[1] // (q_heads + 2 * kv_heads)
    q_end = q_heads * head_dim
    k_end = q_end + kv_heads * head_dim
    queries = rotate(projected[:, :q_end].reshape(length, q_heads, head_dim), cosine, sine).astype(
        jnp.bfloat16
    )
    key_rows = rotate(
        projected[:, q_end:k_end].reshape(length, kv_heads, head_dim), cosine, sine
    ).astype(jnp.bfloat16)
    values = projected[:, k_end:].reshape(length, kv_heads, head_dim).astype(jnp.bfloat16)
    queries = queries.reshape(length, kv_heads, q_heads // kv_heads, head_dim)
    scores = jnp.einsum(
        "qkgd,skd->kgqs", queries, key_rows, preferred_element_type=jnp.float32
    ) * head_dim ** (-0.5)
    causal = jnp.arange(length)[:, None] >= jnp.arange(length)[None, :]
    scores = jnp.where(causal, scores, NEGATIVE)
    attn_probs = jax.nn.softmax(scores, axis=-1).astype(jnp.bfloat16)
    mixed_heads = jnp.einsum(
        "kgqs,skd->qkgd", attn_probs, values, preferred_element_type=jnp.float32
    )
    return mixed_heads.reshape(length, q_heads * head_dim).astype(jnp.bfloat16)


def ring_position(index, n):
    odd = lax.rem(index, 2)
    half = lax.div(index, 2)
    return (1 - odd) * half + odd * (n - 1 - half)


def ring_index(position, n):
    back = lax.div(position, n // 2)
    return (1 - back) * 2 * position + back * (2 * (n - 1 - position) + 1)


def pieces(slots):
    half = slots // 2
    out = []
    for direction, first, count in ((0, 0, half), (1, half, slots - half)):
        cuts = 5 if count % 5 == 0 else 1
        size = count // cuts
        out.append([(first + i * size, size) for i in range(cuts)])
    return out


def enter(neighbours, axis="fsdp"):
    barrier = pltpu.get_barrier_semaphore()
    for neighbour in neighbours:
        pl.semaphore_signal(
            barrier, inc=1, device_id={axis: neighbour}, device_id_type=pl.DeviceIdType.MESH
        )
    pl.semaphore_wait(barrier, len(neighbours))


def gather_kernel(n, slots, grid_qkv, grid_out, slot_ref, w_ref, p_ref, tokens_ref, gain_ref,
                  proj_ref, d_proj_ref, wo_ref, po_ref, normed_t_ref, held_w, held_p, matrix,
                  normed, send_sem, recv_sem):
    me = lax.axis_index("fsdp")
    pos = ring_position(me, n)
    right = ring_index(lax.rem(pos + 1, n), n)
    left = ring_index(lax.rem(pos + n - 1, n), n)
    towards = (right, left)
    enter((left, right))
    parts = pieces(slots)
    arrays = ((w_ref, held_w), (p_ref, held_p))

    def copy(which, step, direction, j):
        own, held = arrays[which]
        first, size = parts[direction][j]
        shift = n - step if direction == 0 else step
        origin = ring_index(lax.rem(pos + shift, n), n)
        there = held.at[pl.ds(origin * slots + first, size)]
        here = own.at[pl.ds(first, size)] if step == 0 else there
        return pltpu.make_async_remote_copy(
            src_ref=here,
            dst_ref=there,
            send_sem=send_sem.at[which, step, direction, j],
            recv_sem=recv_sem.at[which, step, direction, j],
            device_id={"fsdp": towards[direction]},
            device_id_type=pl.DeviceIdType.MESH,
        )

    def arrival(which, step, direction, j):
        first, size = parts[direction][j]
        own, held = arrays[which]
        shift = n - step - 1 if direction == 0 else step + 1
        origin = ring_index(lax.rem(pos + shift, n), n)
        there = held.at[pl.ds(origin * slots + first, size)]
        pltpu.make_async_remote_copy(
            src_ref=there,
            dst_ref=there,
            send_sem=send_sem.at[which, step, direction, j],
            recv_sem=recv_sem.at[which, step, direction, j],
            device_id={"fsdp": towards[direction]},
            device_id_type=pl.DeviceIdType.MESH,
        ).wait_recv()

    def each():
        for j in range(max(len(parts[0]), len(parts[1]))):
            for direction in range(2):
                if j < len(parts[direction]):
                    yield direction, j

    def normalize():
        rows = 32

        def some(i, carry):
            here = pl.ds(pl.multiple_of(i * rows, rows), rows)
            values = tokens_ref[here, :].astype(jnp.float32)
            factor = lax.rsqrt(jnp.mean(values * values, axis=-1, keepdims=True) + EPS)
            normed[here, :] = (values * factor * gain_ref[...]).astype(jnp.bfloat16)
            return carry

        lax.fori_loop(0, normed.shape[0] // rows, some, 0)

    def transpose():
        edge = held_w.shape[-1]

        def some(i, carry):
            here = pl.ds(pl.multiple_of(i * edge, edge), edge)
            normed_t_ref[here, :] = normed[:, here].T
            return carry

        lax.fori_loop(0, normed.shape[1] // edge, some, 0)

    def project(result_ref):
        rows = 256

        def some(i, carry):
            here = pl.ds(pl.multiple_of(i * rows, rows), rows)
            result_ref[here, :] = jnp.dot(
                normed[here, :], matrix[...], preferred_element_type=jnp.float32
            )
            return carry

        lax.fori_loop(0, normed.shape[0] // rows, some, 0)

    def unpack(which, qkv_ref, out_ref):
        own, held = arrays[which]
        rows, cols = grid_qkv
        edge = held.shape[-1]

        def qkv_row(i, carry):
            for c in range(cols):
                qkv_ref[pl.ds(pl.multiple_of(i * edge, edge), edge), c * edge:(c + 1) * edge] = (
                    held[slot_ref[i * cols + c]]
                )
            return carry

        lax.fori_loop(0, rows, qkv_row, 0)
        out_rows, out_cols = grid_out

        def out_col(i, carry):
            for r in range(out_rows):
                out_ref[r * edge:(r + 1) * edge, pl.ds(pl.multiple_of(i * edge, edge), edge)] = (
                    held[slot_ref[rows * cols + r * out_cols + i]]
                )
            return carry

        lax.fori_loop(0, out_cols, out_col, 0)

    def finish(which, qkv_ref, out_ref):
        own, held = arrays[which]
        for direction, j in each():
            arrival(which, n - 2, direction, j)
        held[pl.ds(me * slots, slots)] = own[...]
        unpack(which, qkv_ref, out_ref)

    sent = []
    for which in range(2):
        for step in range(n - 1):
            for direction, j in each():
                if step > 0:
                    arrival(which, step - 1, direction, j)
                one = copy(which, step, direction, j)
                one.start()
                sent.append(one)
            if which == 0 and step == 0:
                normalize()
            if which == 0 and step == 1:
                transpose()
            if which == 1 and step == 0:
                finish(0, matrix, wo_ref)
            if which == 1 and step == 1:
                project(proj_ref)
    finish(1, matrix, po_ref)
    project(d_proj_ref)
    for one in sent:
        one.wait_send()


def gather_weights(slot_of, weights, probes, tokens, gain, n, grid_qkv, grid_out):
    slots, edge, _ = weights.shape
    cuts = max(len(part) for part in pieces(slots))
    length, width = tokens.shape
    proj = jax.ShapeDtypeStruct((length, grid_qkv[1] * edge), jnp.float32)
    turned = jax.ShapeDtypeStruct((width, length), jnp.bfloat16)
    out = jax.ShapeDtypeStruct((grid_out[0] * edge, grid_out[1] * edge), jnp.bfloat16)
    vmem = pl.BlockSpec(memory_space=pltpu.VMEM)
    return pl.pallas_call(
        functools.partial(gather_kernel, n, slots, grid_qkv, grid_out),
        out_shape=(proj, proj, out, out, turned),
        in_specs=[pl.BlockSpec(memory_space=pltpu.SMEM)] + [vmem] * 4,
        out_specs=(vmem,) * 5,
        scratch_shapes=[
            pltpu.VMEM((n * slots, edge, edge), jnp.bfloat16),
            pltpu.VMEM((n * slots, edge, edge), jnp.bfloat16),
            pltpu.VMEM((grid_qkv[0] * edge, grid_qkv[1] * edge), jnp.bfloat16),
            pltpu.VMEM((length, width), jnp.bfloat16),
            pltpu.SemaphoreType.DMA((2, n - 1, 2, cuts)),
            pltpu.SemaphoreType.DMA((2, n - 1, 2, cuts)),
        ],
        compiler_params=pltpu.CompilerParams(
            collective_id=0, has_side_effects=True, vmem_limit_bytes=VMEM_BYTES
        ),
    )(slot_of, weights, probes, tokens, gain)


def gradient_blocks(grid_qkv, grid_out, normed_t_ref, d_proj_ref, mixed_t_ref, weighted_ref,
                    out_ref):
    edge = out_ref.shape[-1]
    rows, cols = grid_qkv
    out_rows, out_cols = grid_out
    group = 2

    out_ref[rows * cols + out_rows * out_cols] = jnp.zeros((edge, edge), out_ref.dtype)

    def qkv_rows(i, carry):
        width = group * edge
        left = normed_t_ref[pl.ds(pl.multiple_of(i * width, width), width), :]
        block = jnp.dot(
            left, d_proj_ref[...], preferred_element_type=jnp.float32
        ).astype(jnp.bfloat16)
        for r in range(group):
            for c in range(cols):
                out_ref[(i * group + r) * cols + c] = block[
                    r * edge:(r + 1) * edge, c * edge:(c + 1) * edge
                ]
        return carry

    lax.fori_loop(0, rows // group, qkv_rows, 0)

    def out_columns(i, carry):
        width = group * edge
        right = weighted_ref[:, pl.ds(pl.multiple_of(i * width, width), width)]
        block = jnp.dot(
            mixed_t_ref[...], right, preferred_element_type=jnp.float32
        ).astype(jnp.bfloat16)
        for r in range(out_rows):
            for c in range(group):
                out_ref[rows * cols + r * out_cols + i * group + c] = block[
                    r * edge:(r + 1) * edge, c * edge:(c + 1) * edge
                ]
        return carry

    lax.fori_loop(0, out_cols // group, out_columns, 0)


def reduce_kernel(n, slots, scale, grid_qkv, grid_out, pick_ref, normed_t_ref, d_proj_ref,
                  mixed_t_ref, weighted_ref, out_ref, grads, begin, held, send_sem, recv_sem):
    me = lax.axis_index("fsdp")
    pos = ring_position(me, n)
    right = ring_index(lax.rem(pos + 1, n), n)
    left = ring_index(lax.rem(pos + n - 1, n), n)
    towards = (right, left)
    enter((left, right))
    parts = pieces(slots)
    gradient_blocks(
        grid_qkv, grid_out, normed_t_ref, d_proj_ref, mixed_t_ref, weighted_ref, grads
    )

    def own(step, direction, j):
        shift = n - 1 - step if direction == 0 else 1 + step
        target = ring_index(lax.rem(pos + shift, n), n)
        return target * slots

    def each_block(direction, j, body):
        first, size = parts[direction][j]

        def some(i, carry):
            body(first + i)
            return carry

        lax.fori_loop(0, size, some, 0)

    def copy(step, direction, j):
        first, size = parts[direction][j]
        here = begin.at[pl.ds(first, size)] if step == 0 else held.at[step - 1, pl.ds(first, size)]
        return pltpu.make_async_remote_copy(
            src_ref=here,
            dst_ref=held.at[step, pl.ds(first, size)],
            send_sem=send_sem.at[step, direction, j],
            recv_sem=recv_sem.at[step, direction, j],
            device_id={"fsdp": towards[direction]},
            device_id_type=pl.DeviceIdType.MESH,
        )

    def each():
        for j in range(max(len(parts[0]), len(parts[1]))):
            for direction in range(2):
                if j < len(parts[direction]):
                    yield direction, j

    sent = {}
    for step in range(n - 1):
        for direction, j in each():
            first, size = parts[direction][j]
            base = own(step, direction, j)
            if step > 0:
                sent[step - 1, direction, j].wait_recv()

                def add(t, step=step, base=base):
                    held[step - 1, t] = (
                        held[step - 1, t].astype(jnp.float32)
                        + grads[pick_ref[base + t]].astype(jnp.float32)
                    ).astype(jnp.bfloat16)

                each_block(direction, j, add)
            else:

                def fill(t, base=base):
                    begin[t] = grads[pick_ref[base + t]]

                each_block(direction, j, fill)
            one = copy(step, direction, j)
            one.start()
            sent[step, direction, j] = one
    for direction, j in each():
        first, size = parts[direction][j]
        sent[n - 2, direction, j].wait_recv()
        base = own(n - 1, direction, j)

        def last(t, base=base):
            out_ref[t] = (
                held[n - 2, t].astype(jnp.float32) + grads[pick_ref[base + t]].astype(jnp.float32)
            ) * scale

        each_block(direction, j, last)
    for one in sent.values():
        one.wait_send()


def reduce_slots(picked, normed_t, d_proj, mixed_t, weighted, n, scale, grid_qkv, grid_out):
    slots = picked.shape[0] // n
    edge = BLK
    total_blocks = grid_qkv[0] * grid_qkv[1] + grid_out[0] * grid_out[1]
    cuts = max(len(part) for part in pieces(slots))
    vmem = pl.BlockSpec(memory_space=pltpu.VMEM)
    return pl.pallas_call(
        functools.partial(reduce_kernel, n, slots, scale, grid_qkv, grid_out),
        out_shape=jax.ShapeDtypeStruct((slots, edge, edge), jnp.float32),
        in_specs=[pl.BlockSpec(memory_space=pltpu.SMEM)] + [vmem] * 4,
        out_specs=vmem,
        scratch_shapes=[
            pltpu.VMEM((total_blocks + 1, edge, edge), jnp.bfloat16),
            pltpu.VMEM((slots, edge, edge), jnp.bfloat16),
            pltpu.VMEM((n - 1, slots, edge, edge), jnp.bfloat16),
            pltpu.SemaphoreType.DMA((n - 1, 2, cuts)),
            pltpu.SemaphoreType.DMA((n - 1, 2, cuts)),
        ],
        compiler_params=pltpu.CompilerParams(
            collective_id=1, has_side_effects=True, vmem_limit_bytes=VMEM_BYTES
        ),
    )(picked, normed_t, d_proj, mixed_t, weighted)


def exchange_kernel(mixed_ref, d_mixed_ref, w_ref, p_ref, curv_ref, weighted_ref, back_ref,
                    terms, near, pair, far, share, rest, send_sem, recv_sem):
    me = lax.axis_index("seq")
    side = lax.rem(me, 2)
    core = me + 1 - 2 * side
    across = me + 2 - 4 * lax.rem(lax.div(me, 2), 2)
    enter((core, across), "seq")
    length, width = terms.shape
    half = width // 2
    chunks = recv_sem.shape[1]
    rows = length // chunks
    mine = pl.ds(pl.multiple_of(side * half, half), half)
    other = pl.ds(pl.multiple_of((1 - side) * half, half), half)

    def block(i):
        return pl.ds(i * rows, rows)

    def copy(stage, i, here, there, target):
        return pltpu.make_async_remote_copy(
            src_ref=here,
            dst_ref=there,
            send_sem=send_sem.at[stage, i],
            recv_sem=recv_sem.at[stage, i],
            device_id={"seq": target},
            device_id_type=pl.DeviceIdType.MESH,
        )

    def terms_of(i):
        tile = width // 4

        def columns(j, carry):
            cols = pl.ds(pl.multiple_of(j * tile, tile), tile)
            terms[block(i), cols] = (
                jnp.dot(d_mixed_ref[block(i), :], w_ref[:, cols], preferred_element_type=jnp.float32)
                + jnp.dot(mixed_ref[block(i), :], p_ref[:, cols], preferred_element_type=jnp.float32)
            ).astype(jnp.bfloat16)
            return carry

        lax.fori_loop(0, 4, columns, 0)

    first = [copy(0, i, terms.at[block(i), other], near.at[block(i)], core) for i in range(chunks)]
    second = [copy(1, i, pair.at[block(i)], far.at[block(i)], across) for i in range(chunks)]
    third = [copy(2, i, share.at[block(i)], rest.at[block(i)], core) for i in range(chunks)]

    def send_pair(i):
        first[i].wait_recv()
        pair[block(i)] = (
            terms[block(i), mine].astype(jnp.float32) + near[block(i)].astype(jnp.float32)
        ).astype(jnp.bfloat16)
        second[i].start()

    def send_share(i):
        second[i].wait_recv()
        total = pair[block(i)].astype(jnp.float32) + far[block(i)].astype(jnp.float32)
        share[block(i)] = (curv_ref[block(i), mine].astype(jnp.float32) * total).astype(
            jnp.bfloat16
        )
        third[i].start()

    def finish(i):
        weighted_ref[block(i), mine] = share[block(i)]
        third[i].wait_recv()
        weighted_ref[block(i), other] = rest[block(i)]
        back_ref[block(i), :] = lax.dot_general(
            weighted_ref[block(i), :],
            w_ref[...],
            (((1,), (1,)), ((), ())),
            preferred_element_type=jnp.float32,
        ).astype(jnp.bfloat16)

    for i in range(chunks):
        terms_of(i)
        first[i].start()
        if i > 0:
            send_pair(i - 1)
    send_pair(chunks - 1)
    for i in range(chunks):
        send_share(i)
        if i > 0:
            finish(i - 1)
    finish(chunks - 1)
    for one in first + second + third:
        one.wait_send()


def exchange(mixed, d_mixed, w_out, p_out, curvature):
    length, width = curvature.shape
    chunks = 4
    vmem = pl.BlockSpec(memory_space=pltpu.VMEM)
    half = pltpu.VMEM((length, width // 2), jnp.bfloat16)
    return pl.pallas_call(
        exchange_kernel,
        out_shape=(
            jax.ShapeDtypeStruct((length, width), jnp.bfloat16),
            jax.ShapeDtypeStruct(mixed.shape, jnp.bfloat16),
        ),
        in_specs=[vmem] * 5,
        out_specs=(vmem, vmem),
        scratch_shapes=[
            pltpu.VMEM((length, width), jnp.bfloat16),
            half,
            half,
            half,
            half,
            half,
            pltpu.SemaphoreType.DMA((3, chunks)),
            pltpu.SemaphoreType.DMA((3, chunks)),
        ],
        compiler_params=pltpu.CompilerParams(
            collective_id=2, has_side_effects=True, vmem_limit_bytes=VMEM_BYTES
        ),
    )(mixed, d_mixed, w_out, p_out, curvature)


def local(tokens, norm_gain, curvature, weight_slots, probe_slots, block_counts):
    n_columns = lax.axis_size("seq")
    n_owners = lax.axis_size("fsdp")
    q_heads = HQ // n_columns
    kv_heads = HK // n_columns
    row_blocks = D // BLK
    qkv_cols = (q_heads + 2 * kv_heads) * HD // BLK
    out_rows = q_heads * HD // BLK
    grid_qkv, grid_out = (row_blocks, qkv_cols), (out_rows, row_blocks)
    total_blocks = row_blocks * qkv_cols + out_rows * row_blocks
    slots = weight_slots.shape[1]
    length = tokens.shape[1]
    counts = block_counts[0]
    range_ends = jnp.cumsum(counts)
    starts = range_ends - counts
    owner_ids = jnp.arange(n_owners, dtype=jnp.int32)
    block_ids = jnp.arange(total_blocks, dtype=jnp.int32)
    owners = jnp.sum((range_ends[None, :] <= block_ids[:, None]).astype(jnp.int32), axis=1)
    first_block = jnp.sum(
        jnp.where(owners[:, None] == owner_ids[None, :], starts[None, :], 0), axis=1
    )
    slot_of = (owners * slots + block_ids - first_block).astype(jnp.int32)
    projected, d_projected, w_out, p_out, normed_t = gather_weights(
        slot_of,
        weight_slots[0],
        probe_slots[0],
        tokens[0],
        norm_gain[None, :],
        n_owners,
        grid_qkv,
        grid_out,
    )
    cosine, sine = rotary(length, HD)

    def inner(projected):
        return attention(projected, cosine, sine, q_heads, kv_heads)

    mixed, d_mixed = jax.jvp(inner, (projected,), (d_projected,))
    weighted, back_mixed = exchange(mixed, d_mixed, w_out, p_out, curvature[0])
    mixed_again, pullback = jax.vjp(inner, projected)
    (back_projected,) = pullback(back_mixed)
    slot_index = jnp.arange(n_owners * slots, dtype=jnp.int32)
    place = slot_index % slots
    owner_hot = (slot_index // slots)[:, None] == owner_ids[None, :]
    owner_first = jnp.sum(jnp.where(owner_hot, starts[None, :], 0), axis=1)
    own_count = jnp.sum(jnp.where(owner_hot, counts[None, :], 0), axis=1)
    picked = jnp.where(place < own_count, owner_first + place, total_blocks).astype(jnp.int32)
    scaled = reduce_slots(
        picked,
        normed_t,
        back_projected.astype(jnp.bfloat16),
        mixed_again.T,
        weighted,
        n_owners,
        (length * n_owners) ** -0.5,
        grid_qkv,
        grid_out,
    )
    return scaled.reshape(1, slots, BLK, BLK)


def spot():
    f = lax.axis_index("fsdp")
    s = lax.axis_index("seq")
    return lax.div(f, 2), lax.rem(f, 2), lax.div(s, 2), lax.rem(s, 2)


def device(z, y, x, c):
    return {"fsdp": 2 * z + y, "seq": 2 * x + c}


def mirrored(z, c, planes):
    return z + c * (planes - 1 - 2 * z)


def greet(peers):
    barrier = pltpu.get_barrier_semaphore()
    for peer in peers:
        pl.semaphore_signal(barrier, inc=1, device_id=peer, device_id_type=pl.DeviceIdType.MESH)
    pl.semaphore_wait(barrier, len(peers))


def shard_columns(x, j, width):
    return x * (width // 4) + j * (width // 8), width // 2 + j * (width // 4) + x * (width // 8)


def cut_count(slots, finer=1):
    for cuts in (5 * finer, 5):
        if slots % cuts == 0:
            return cuts
    return 1


def gather_grid_kernel(n, slots, grid_qkv, grid_out, slot_ref, w_ref, p_ref, tokens_ref, gain_ref,
                       curv_ref, proj_out, d_proj_ref, wo_out, po_out, normed_t_out, curv_out,
                       held_w, held_p, matrix, normed, wo_ref, po_ref, normed_t_ref, proj_ref,
                       curv_part, turned, swap_send, swap_recv, in_sem, out_sem, send_y, send_core, send_z, recv, tok_send,
                       tok_recv, relay_send, relay_recv, curv_send, curv_recv):
    planes = n // 2
    z, y, x, c = spot()
    zeta = mirrored(z, c, planes)
    hub = lax.rem(zeta, 2) == 0
    spoke = lax.rem(zeta, 2) == 1
    mate = z + 1 - 2 * lax.rem(z, 2)
    y_peer = device(z, 1 - y, x, c)
    x_peer = device(z, y, 1 - x, c)
    core_peer = device(z, y, x, 1 - c)
    z_peer = device(mate, y, x, c)
    row = [device(lax.rem(z + i, planes), y, x, c) for i in range(1, planes)]
    cuts = cut_count(slots)
    size = slots // cuts
    own = (w_ref, p_ref)
    held = (held_w, held_p)
    me = 2 * z + y

    def own_load(which):
        here = held[which].at[pl.ds(me * slots, slots)]
        return pltpu.make_async_copy(own[which], here, in_sem.at[which])

    def token_load():
        return pltpu.make_async_copy(tokens_ref, normed, in_sem.at[2])

    stores = [
        pltpu.make_async_copy(here, there, out_sem.at[i])
        for i, (here, there) in enumerate((
            (normed_t_ref, normed_t_out), (proj_ref, proj_out), (wo_ref, wo_out),
            (po_ref, po_out), (curv_part, curv_out),
        ))
    ]

    @pl.when(hub)
    def _():
        token_load().start()
        for which in range(2):
            own_load(which).start()

    greet(row + [core_peer, y_peer, x_peer])
    tok_cuts = tok_send.shape[0]
    half = normed.shape[0] // 2
    tok_rows = half // tok_cuts
    width = normed.shape[1]
    part = width // 8

    def at(zeta_at):
        return mirrored(zeta_at, c, planes)

    def spread(which, d, j):
        return held[which].at[pl.ds(d * slots + j * size, size)]

    def move(src, which, d, j, peer, sem):
        return pltpu.make_async_remote_copy(
            src_ref=src,
            dst_ref=spread(which, d, j),
            send_sem=sem,
            recv_sem=recv.at[d, which * cuts + j],
            device_id=peer,
            device_id_type=pl.DeviceIdType.MESH,
        )

    def own_chunk(which, j):
        return own[which].at[pl.ds(j * size, size)]

    def arrive(which, d, j):
        move(spread(which, d, j), which, d, j, core_peer, send_y.at[0, 0]).wait_recv()

    other_hub = device(at(2 - zeta), y, x, c)
    near_hub = device(at(2), y, x, c)
    end_hub = device(at(0), y, x, c)

    def token_copy(i, rows_half, peer, s_sem, r_sem, src):
        rows = pl.ds(rows_half * half + i * tok_rows, tok_rows)
        return pltpu.make_async_remote_copy(
            src_ref=src.at[rows],
            dst_ref=normed.at[rows],
            send_sem=s_sem.at[i],
            recv_sem=r_sem.at[i],
            device_id=peer,
            device_id_type=pl.DeviceIdType.MESH,
        )

    def curv_copy(i):
        first = shard_columns(x, lax.rem(mate, 2), width)[i]
        return pltpu.make_async_remote_copy(
            src_ref=curv_ref.at[:, pl.ds(pl.multiple_of(first, part), part)],
            dst_ref=curv_part.at[i],
            send_sem=curv_send.at[i],
            recv_sem=curv_recv.at[i],
            device_id=z_peer,
            device_id_type=pl.DeviceIdType.MESH,
        )

    def curv_local(i):
        first = shard_columns(x, lax.rem(z, 2), width)[i]
        return pltpu.make_async_copy(
            curv_ref.at[:, pl.ds(pl.multiple_of(first, part), part)],
            curv_part.at[i],
            curv_recv.at[i],
        )

    def to_z(which, j):
        k = which * cuts + j
        return move(own_chunk(which, j), which, me, j, other_hub, send_z.at[0, k])

    def to_y(which, j):
        k = which * cuts + j
        return move(own_chunk(which, j), which, me, j, y_peer, send_y.at[0, k])

    def to_core(which, j):
        k = which * cuts + j
        return move(own_chunk(which, j), which, me, j, core_peer, send_core.at[0, k])

    def spoke_own(which, j):
        src = own_chunk(which, j)
        k = which * cuts + j
        return (
            move(src, which, me, j, near_hub, send_z.at[0, k]),
            move(src, which, me, j, end_hub, send_z.at[1, k]),
        )

    lead = min(6, 2 * cuts)
    every = [(which, j) for which in range(2) for j in range(cuts)]

    @pl.when(hub)
    def _():
        for k in range(lead):
            to_y(*every[k]).start()
        for k in range(max(len(every), tok_cuts)):
            if k < len(every):
                to_z(*every[k]).start()
            if k < tok_cuts:
                token_copy(k, x, z_peer, tok_send, tok_recv, tokens_ref).start()
        for i in range(2):
            curv_copy(i).start()
            curv_local(i).start()

    @pl.when(spoke)
    def _():
        for one in every:
            for copy in spoke_own(*one):
                copy.start()

    def pass_row(k):
        which, j = every[k]
        to_core(which, j).start()
        for r in range(1, planes):
            d = 2 * at(lax.rem(zeta + r, planes)) + y
            arrive(which, d, j)
            src = spread(which, d, j)
            move(src, which, d, j, y_peer, send_y.at[r, k]).start()
            move(src, which, d, j, core_peer, send_core.at[r, k]).start()
            if r == 1 and k + lead < len(every):
                to_y(*every[k + lead]).start()

    def pass_across(k):
        which, j = every[k]
        for r in range(planes):
            d = 2 * at(lax.rem(zeta + r, planes)) + 1 - y
            arrive(which, d, j)
            move(spread(which, d, j), which, d, j, core_peer, send_core.at[planes + r, k]).start()

    def forward(which, j):
        k = which * cuts + j
        pass_row(k)
        if k not in (0, cuts):
            pass_across(k - 1)
        if k in (cuts - 1, 2 * cuts - 1):
            pass_across(k)

    def step(which, j):
        @pl.when(hub)
        def _():
            forward(which, j)

        @pl.when(spoke)
        def _():
            for d in range(n):
                arrive(which, d, j)

    def normalize():
        rows = 32

        def some(i, carry):
            here = pl.ds(pl.multiple_of(i * rows, rows), rows)
            values = normed[here, :].astype(jnp.float32)
            factor = lax.rsqrt(jnp.mean(values * values, axis=-1, keepdims=True) + EPS)
            normed[here, :] = (values * factor * gain_ref[...]).astype(jnp.bfloat16)
            return carry

        lax.fori_loop(0, normed.shape[0] // rows, some, 0)

    length = normed.shape[0]
    mid = width // 2

    def transpose():
        edge = held_w.shape[-1]

        def some(i, carry):
            here = pl.ds(pl.multiple_of(i * edge, edge), edge)
            mine = pl.ds(pl.multiple_of(c * mid + i * edge, edge), edge)
            other = pl.ds(pl.multiple_of((1 - c) * mid + i * edge, edge), edge)
            normed_t_ref[here, :length] = normed[:, mine].T
            turned[here, :] = normed[:, other].T
            return carry

        lax.fori_loop(0, mid // edge, some, 0)

    swap = pltpu.make_async_remote_copy(
        src_ref=turned,
        dst_ref=normed_t_ref.at[:, pl.ds(length, length)],
        send_sem=swap_send.at[0],
        recv_sem=swap_recv.at[0],
        device_id=core_peer,
        device_id_type=pl.DeviceIdType.MESH,
    )

    def project(result_ref):
        rows = 256

        def some(i, carry):
            here = pl.ds(pl.multiple_of(i * rows, rows), rows)
            result_ref[here, :] = jnp.dot(
                normed[here, :], matrix[...], preferred_element_type=jnp.float32
            )
            return carry

        lax.fori_loop(0, normed.shape[0] // rows, some, 0)

    def unpack_qkv(which):
        rows, cols = grid_qkv
        edge = held_w.shape[-1]

        def qkv_row(i, carry):
            for col in range(cols):
                matrix[pl.ds(pl.multiple_of(i * edge, edge), edge), col * edge:(col + 1) * edge] = (
                    held[which][slot_ref[i * cols + col]]
                )
            return carry

        lax.fori_loop(0, rows, qkv_row, 0)

    def unpack_out(which, out_ref):
        rows, cols = grid_qkv
        out_rows, out_cols = grid_out
        edge = held_w.shape[-1]

        def out_col(i, carry):
            for r in range(out_rows):
                out_ref[r * edge:(r + 1) * edge, pl.ds(pl.multiple_of(i * edge, edge), edge)] = (
                    held[which][slot_ref[rows * cols + r * out_cols + i]]
                )
            return carry

        lax.fori_loop(0, out_cols, out_col, 0)

    def keep_own(which):
        @pl.when(hub)
        def _():
            own_load(which).wait()

    @pl.when(hub)
    def _():
        token_load().wait()

    @pl.when(spoke)
    def _():
        for i in range(tok_cuts):
            token_copy(i, x, z_peer, tok_send, tok_recv, normed).wait_recv()
            token_copy(i, x, x_peer, relay_send, relay_recv, normed).start()
        for i in range(tok_cuts):
            token_copy(i, 1 - x, x_peer, relay_send, relay_recv, normed).wait_recv()
        for i in range(tok_cuts):
            token_copy(i, x, x_peer, relay_send, relay_recv, normed).wait_send()

    normalize()
    for j in range(cuts):
        step(0, j)
        if j == 0:
            transpose()
            swap.start()
    keep_own(0)
    def first_proj():
        project(proj_ref)
        stores[1].start()

    def first_out():
        unpack_out(0, wo_ref)
        stores[2].start()

    todo = [lambda: unpack_qkv(0), first_proj, first_out]
    for j in range(cuts):
        step(1, j)
        if j < cuts - 1 and todo:
            todo.pop(0)()
    while todo:
        todo.pop(0)()
    keep_own(1)
    unpack_out(1, po_ref)
    stores[3].start()

    @pl.when(hub)
    def _():
        for i in range(2):
            curv_local(i).wait()

    @pl.when(spoke)
    def _():
        for i in range(2):
            curv_copy(i).wait_recv()

    stores[4].start()
    swap.wait_recv()
    stores[0].start()
    unpack_qkv(1)
    project(d_proj_ref)

    @pl.when(hub)
    def _():
        for i in range(tok_cuts):
            token_copy(i, x, z_peer, tok_send, tok_recv, tokens_ref).wait_send()
        for i in range(2):
            curv_copy(i).wait_send()
        for k, (which, j) in enumerate(every):
            to_z(which, j).wait_send()
            to_y(which, j).wait_send()
            to_core(which, j).wait_send()
            src = spread(which, me, j)
            for r in range(1, planes):
                move(src, which, me, j, y_peer, send_y.at[r, k]).wait_send()
            for r in range(1, n):
                move(src, which, me, j, core_peer, send_core.at[r, k]).wait_send()

    @pl.when(spoke)
    def _():
        for one in every:
            for copy in spoke_own(*one):
                copy.wait_send()

    swap.wait_send()
    for store in stores:
        store.wait()


def gather_grid(slot_of, weights, probes, tokens, gain, curvature, n, grid_qkv, grid_out):
    slots, edge, _ = weights.shape
    cuts = cut_count(slots)
    length, width = tokens.shape
    proj = jax.ShapeDtypeStruct((length, grid_qkv[1] * edge), jnp.float32)
    turned = jax.ShapeDtypeStruct((width // 2, 2 * length), jnp.bfloat16)
    out = jax.ShapeDtypeStruct((grid_out[0] * edge, grid_out[1] * edge), jnp.bfloat16)
    shard = (2, length, width // 8)
    vmem = pl.BlockSpec(memory_space=pltpu.VMEM)
    anywhere = pl.BlockSpec(memory_space=pl.ANY)
    dma = pltpu.SemaphoreType.DMA
    return pl.pallas_call(
        functools.partial(gather_grid_kernel, n, slots, grid_qkv, grid_out),
        out_shape=(proj, proj, out, out, turned, jax.ShapeDtypeStruct(shard, jnp.bfloat16)),
        in_specs=[pl.BlockSpec(memory_space=pltpu.SMEM)] + [anywhere] * 3 + [vmem, anywhere],
        out_specs=(anywhere, vmem) + (anywhere,) * 4,
        scratch_shapes=[
            pltpu.VMEM((n * slots, edge, edge), jnp.bfloat16),
            pltpu.VMEM((n * slots, edge, edge), jnp.bfloat16),
            pltpu.VMEM((grid_qkv[0] * edge, grid_qkv[1] * edge), jnp.bfloat16),
            pltpu.VMEM((length, width), jnp.bfloat16),
            pltpu.VMEM(out.shape, out.dtype),
            pltpu.VMEM(out.shape, out.dtype),
            pltpu.VMEM(turned.shape, turned.dtype),
            pltpu.VMEM(proj.shape, proj.dtype),
            pltpu.VMEM(shard, jnp.bfloat16),
            pltpu.VMEM((width // 2, length), jnp.bfloat16),
            dma((1,)),
            dma((1,)),
            dma((3,)),
            dma((5,)),
            dma((n // 2, 2 * cuts)),
            dma((n, 2 * cuts)),
            dma((2, 2 * cuts)),
            dma((n, 2 * cuts)),
            dma((4,)),
            dma((4,)),
            dma((4,)),
            dma((4,)),
            dma((2,)),
            dma((2,)),
        ],
        compiler_params=pltpu.CompilerParams(
            collective_id=3, has_side_effects=True, vmem_limit_bytes=GRID_VMEM_BYTES
        ),
    )(slot_of, weights, probes, tokens, gain, curvature)


def turn_tables(length, head_dim):
    half_dim = head_dim // 2
    frequency = np.exp(-np.log(THETA) * 2.0 * np.arange(half_dim) / head_dim).astype(np.float32)
    angles = np.arange(length, dtype=np.float32)[:, None] * frequency[None, :]
    cosine, sine = np.cos(angles), np.sin(angles)
    return (
        jnp.asarray(np.concatenate([cosine, cosine], axis=1), jnp.float32),
        jnp.asarray(np.concatenate([-sine, sine], axis=1), jnp.float32),
    )


def turn(values, cosine, sine):
    return values * cosine + pltpu.roll(values, values.shape[1] // 2, 1) * sine


def spin(heads, hd, source, target, cos_ref, sin_ref):
    val_at = (heads + 1) * hd

    def some(h, carry):
        here = pl.ds(pl.multiple_of(h * hd, hd), hd)
        target[:, here] = turn(source[:, here], cos_ref[...], sin_ref[...]).astype(jnp.bfloat16)
        return carry

    lax.fori_loop(0, heads + 1, some, 0)
    target[:, val_at:] = source[:, val_at:].astype(jnp.bfloat16)


def attend(heads, hd, first, tile, mixed_ref, d_mixed_ref, mixed_t_ref, probs_ref, rot_ref, d_rot):
    length = rot_ref.shape[0]
    key_at = heads * hd
    val_at = key_at + hd
    scale = hd ** -0.5
    rows = slice(first, first + tile)
    span = first + tile

    def head(h, carry):
        here = pl.ds(pl.multiple_of(h * hd, hd), hd)
        q, dq = rot_ref[rows, here], d_rot[rows, here]
        k, dk = rot_ref[:span, key_at:val_at], d_rot[:span, key_at:val_at]
        v, dv = rot_ref[:span, val_at:], d_rot[:span, val_at:]
        contract = (((1,), (1,)), ((), ()))
        scores = lax.dot_general(q, k, contract, preferred_element_type=jnp.float32) * scale
        slopes = lax.dot_general(
            jnp.concatenate([dq, q], axis=1),
            jnp.concatenate([k, dk], axis=1),
            contract,
            preferred_element_type=jnp.float32,
        ) * scale
        at_row = first + lax.broadcasted_iota(jnp.int32, (tile, span), 0)
        at_col = lax.broadcasted_iota(jnp.int32, (tile, span), 1)
        seen = at_row >= at_col
        scores = jnp.where(seen, scores, NEGATIVE)
        slopes = jnp.where(seen, slopes, 0.0)
        raised = jnp.exp(scores - jnp.max(scores, axis=1, keepdims=True))
        probs = raised / jnp.sum(raised, axis=1, keepdims=True)
        d_probs = probs * (slopes - jnp.sum(probs * slopes, axis=1, keepdims=True))
        probs = probs.astype(jnp.bfloat16)
        d_probs = d_probs.astype(jnp.bfloat16)
        probs_ref[h, rows, :span] = probs
        if span < length:
            probs_ref[h, rows, span:] = jnp.zeros((tile, length - span), jnp.bfloat16)
        mixed = jnp.dot(probs, v, preferred_element_type=jnp.float32).astype(jnp.bfloat16)
        mixed_ref[rows, here] = mixed
        mixed_t_ref[here, rows] = mixed.T
        d_mixed_ref[rows, here] = (
            jnp.dot(d_probs, v, preferred_element_type=jnp.float32)
            + jnp.dot(probs, dv, preferred_element_type=jnp.float32)
        ).astype(jnp.bfloat16)
        return carry

    lax.fori_loop(0, heads, head, 0)


def attend_back(heads, back_ref, probs_ref, rot_ref, cos_ref, sin_ref, out_ref, slope_ref):
    length = back_ref.shape[0]
    hd = cos_ref.shape[1]
    key_at = heads * hd
    val_at = key_at + hd
    scale = hd ** -0.5
    tile = hd

    def unturn(values):
        rounded = values.astype(jnp.bfloat16).astype(jnp.float32)
        return turn(rounded, cos_ref[...], -sin_ref[...]).astype(jnp.bfloat16)

    def head(h, totals):
        here = pl.ds(pl.multiple_of(h * hd, hd), hd)
        key_total, val_total = totals
        for i in range(length // tile):
            rows = slice(i * tile, (i + 1) * tile)
            span = (i + 1) * tile
            back = back_ref[rows, here]
            d_probs = lax.dot_general(
                back, rot_ref[:span, val_at:], (((1,), (1,)), ((), ())),
                preferred_element_type=jnp.float32,
            ).astype(jnp.bfloat16).astype(jnp.float32)
            probs = probs_ref[h, rows, :span].astype(jnp.float32)
            slopes = probs * (d_probs - jnp.sum(probs * d_probs, axis=1, keepdims=True)) * scale
            slope_ref[rows, :span] = slopes.astype(jnp.bfloat16)
            if span < length:
                slope_ref[rows, span:] = jnp.zeros((tile, length - span), jnp.bfloat16)
        slopes = slope_ref[...]
        d_query = jnp.dot(slopes, rot_ref[:, key_at:val_at], preferred_element_type=jnp.float32)
        out_ref[:, here] = unturn(d_query)
        first = (((0,), (0,)), ((), ()))
        key_total = key_total + lax.dot_general(
            rot_ref[:, here], slopes, first, preferred_element_type=jnp.float32
        )
        val_total = val_total + lax.dot_general(
            back_ref[:, here], probs_ref[h], first, preferred_element_type=jnp.float32
        )
        return key_total, val_total

    zero = jnp.zeros((hd, length), jnp.float32)
    key_total, val_total = lax.fori_loop(0, heads, head, (zero, zero))
    out_ref[:, key_at:val_at] = unturn(key_total.T)
    out_ref[:, val_at:] = val_total.T.astype(jnp.bfloat16)


def square_kernel(heads, proj_ref, d_proj_ref, w_out, p_out, curv_ref, cos_ref, sin_ref,
                  weighted_out, back_proj_ref, mixed_t_out, mixed_t, theirs, w_ref, p_ref, mixed_ref, d_mixed_ref,
                  probs, rot, d_rot, slope, back_ref, terms, near_x, near_z, pair_a, pair_b, far_z,
                  far_x, full, load_sem, store_sem, swap_send, swap_recv, send_sem,
                  recv_sem):
    z, y, x, c = spot()
    side = lax.rem(z, 2)
    x_peer = device(z, y, 1 - x, c)
    z_peer = device(z + 1 - 2 * side, y, x, c)
    loads = [
        pltpu.make_async_copy(w_out, w_ref, load_sem.at[0]),
        pltpu.make_async_copy(p_out, p_ref, load_sem.at[1]),
    ]
    for load in loads:
        load.start()
    core_peer = device(z, y, x, 1 - c)
    greet([x_peer, z_peer, core_peer])
    hd = cos_ref.shape[1]
    spin(heads, hd, proj_ref, rot, cos_ref, sin_ref)
    spin(heads, hd, d_proj_ref, d_rot, cos_ref, sin_ref)
    length, width = terms.shape
    chunks = recv_sem.shape[1]

    def swap(i, here, there):
        return pltpu.make_async_remote_copy(
            src_ref=here,
            dst_ref=there,
            send_sem=swap_send.at[i],
            recv_sem=swap_recv.at[i],
            device_id=core_peer,
            device_id_type=pl.DeviceIdType.MESH,
        )

    swap_mixed = swap(
        chunks, mixed_t.at[:, pl.ds(0, length)], mixed_t.at[:, pl.ds(length, length)]
    )
    rows = length // chunks
    tile = min(hd, length)
    tiles = length // tile
    per = chunks // tiles
    quarter, part = width // 4, width // 8

    def block(i):
        return pl.ds(i * rows, rows)

    def cols(first, count):
        return pl.ds(pl.multiple_of(first, count), count)

    keep_a, give_a = cols(x * quarter, quarter), cols((1 - x) * quarter, quarter)
    keep_b = cols(width // 2 + side * quarter, quarter)
    give_b = cols(width // 2 + (1 - side) * quarter, quarter)
    first_a, first_b = shard_columns(x, side, width)
    own_a, own_b = cols(first_a, part), cols(first_b, part)

    def copy(kind, i, here, there, target):
        return pltpu.make_async_remote_copy(
            src_ref=here,
            dst_ref=there,
            send_sem=send_sem.at[kind, i],
            recv_sem=recv_sem.at[kind, i],
            device_id=target,
            device_id_type=pl.DeviceIdType.MESH,
        )

    def stage(i):
        b = block(i)
        return (
            copy(0, i, terms.at[b, give_a], near_x.at[b], x_peer),
            copy(1, i, terms.at[b, give_b], near_z.at[b], z_peer),
            copy(2, i, pair_a.at[b, cols((1 - side) * part, part)], far_z.at[b], z_peer),
            copy(3, i, pair_b.at[b, cols((1 - x) * part, part)], far_x.at[b], x_peer),
            copy(4, i, full.at[b, own_a], full.at[b, own_a], z_peer),
            copy(5, i, full.at[b, own_b], full.at[b, own_b], x_peer),
            copy(6, i, full.at[b, keep_a], full.at[b, keep_a], x_peer),
            copy(7, i, full.at[b, keep_b], full.at[b, keep_b], z_peer),
        )

    def incoming(kind, i, there):
        copy(kind, i, there, there, x_peer).wait_recv()

    def group(i):
        return pl.ds(i * tile, tile)

    def terms_of(i):
        attend(
            heads, hd, i * tile, tile, mixed_ref, d_mixed_ref, mixed_t, probs, rot, d_rot
        )
        if i == 0:
            for load in loads:
                load.wait()
        if i == tiles - 1:
            swap_mixed.start()
        b = group(i)

        def columns(j, carry):
            here = pl.ds(pl.multiple_of(j * quarter, quarter), quarter)
            terms[b, here] = (
                jnp.dot(d_mixed_ref[b, :], w_ref[:, here], preferred_element_type=jnp.float32)
                + jnp.dot(mixed_ref[b, :], p_ref[:, here], preferred_element_type=jnp.float32)
            ).astype(jnp.bfloat16)
            return carry

        lax.fori_loop(0, 4, columns, 0)

    plans = [stage(i) for i in range(chunks)]

    def pair_up(i):
        b = block(i)
        for kind, pair, keep, near in ((0, pair_a, keep_a, near_x), (1, pair_b, keep_b, near_z)):
            incoming(kind, i, near.at[b])
            pair[b] = (
                terms[b, keep].astype(jnp.float32) + near[b].astype(jnp.float32)
            ).astype(jnp.bfloat16)
            plans[i][2 + kind].start()

    def weigh(i):
        b = block(i)
        for kind, pair, mine, far, own_cols in (
            (0, pair_a, side, far_z, own_a), (1, pair_b, x, far_x, own_b)
        ):
            incoming(2 + kind, i, far.at[b])
            total = pair[b, cols(mine * part, part)].astype(jnp.float32) + far[b].astype(jnp.float32)
            full[b, own_cols] = (curv_ref[kind, b].astype(jnp.float32) * total).astype(jnp.bfloat16)
            plans[i][4 + kind].start()

    def widen(i):
        b = block(i)
        other_a, other_b = shard_columns(x, 1 - side, width)[0], shard_columns(1 - x, side, width)[1]
        incoming(4, i, full.at[b, cols(other_a, part)])
        plans[i][6].start()
        incoming(5, i, full.at[b, cols(other_b, part)])
        plans[i][7].start()

    mid = width // 2

    def store(i):
        b = block(i)
        return pltpu.make_async_copy(
            full.at[b, cols(c * mid, mid)], weighted_out.at[b], store_sem.at[i]
        )

    def store_theirs(i):
        there = weighted_out.at[pl.ds(length + i * rows, rows)]
        return pltpu.make_async_copy(theirs.at[block(i)], there, store_sem.at[chunks + i])

    def swap_weighted(i):
        b = block(i)
        return swap(i, full.at[b, cols((1 - c) * mid, mid)], theirs.at[b])

    def finish(i):
        b = block(i)
        incoming(6, i, full.at[b, give_a])
        incoming(7, i, full.at[b, give_b])
        store(i).start()
        swap_weighted(i).start()
        if i % per == per - 1:
            g = group(i // per)
            back_ref[g, :] = lax.dot_general(
                full[g, :], w_ref[...], (((1,), (1,)), ((), ())), preferred_element_type=jnp.float32
            ).astype(jnp.bfloat16)

    for i in range(chunks + 3):
        if i < chunks:
            if i % per == 0:
                terms_of(i // per)
            plans[i][0].start()
            plans[i][1].start()
        if 0 <= i - 1 < chunks:
            pair_up(i - 1)
        if 0 <= i - 2 < chunks:
            weigh(i - 2)
        if 0 <= i - 3 < chunks:
            widen(i - 3)
    for i in range(chunks):
        finish(i)
    swap_mixed.wait_recv()
    store_mixed = pltpu.make_async_copy(mixed_t, mixed_t_out, store_sem.at[2 * chunks])
    store_mixed.start()
    for i in range(chunks):
        swap_weighted(i).wait_recv()
        store_theirs(i).start()
    attend_back(heads, back_ref, probs, rot, cos_ref, sin_ref, back_proj_ref, slope)
    store_mixed.wait()
    for i in range(chunks):
        store(i).wait()
        store_theirs(i).wait()
        swap_weighted(i).wait_send()
    swap_mixed.wait_send()
    for plan in plans:
        for one in plan:
            one.wait_send()


def square_exchange(projected, d_projected, w_out, p_out, curvature, cosine, sine, heads):
    length, inputs = projected.shape
    inner, width = w_out.shape
    chunks = 4
    half = jnp.bfloat16
    vmem = pl.BlockSpec(memory_space=pltpu.VMEM)
    anywhere = pl.BlockSpec(memory_space=pl.ANY)
    quarter = pltpu.VMEM((length, width // 4), half)
    part = pltpu.VMEM((length, width // 8), half)
    whole = pltpu.VMEM((length, width), half)
    narrow = pltpu.VMEM((length, inner), half)
    return pl.pallas_call(
        functools.partial(square_kernel, heads),
        out_shape=(
            jax.ShapeDtypeStruct((2 * length, width // 2), half),
            jax.ShapeDtypeStruct((length, inputs), half),
            jax.ShapeDtypeStruct((inner, 2 * length), half),
        ),
        in_specs=[vmem] * 2 + [anywhere] * 2 + [vmem] * 3,
        out_specs=(anywhere, vmem, anywhere),
        scratch_shapes=[
            pltpu.VMEM((inner, 2 * length), half),
            pltpu.VMEM((length, width // 2), half),
            pltpu.VMEM((inner, width), half),
            pltpu.VMEM((inner, width), half),
            narrow,
            narrow,
            pltpu.VMEM((heads, length, length), half),
            pltpu.VMEM((length, inputs), half),
            pltpu.VMEM((length, inputs), half),
            pltpu.VMEM((length, length), half),
            narrow,
            whole, quarter, quarter, quarter, quarter, part, part, whole,
            pltpu.SemaphoreType.DMA((2,)),
            pltpu.SemaphoreType.DMA((2 * chunks + 1,)),
            pltpu.SemaphoreType.DMA((chunks + 1,)),
            pltpu.SemaphoreType.DMA((chunks + 1,)),
            pltpu.SemaphoreType.DMA((8, chunks)),
            pltpu.SemaphoreType.DMA((8, chunks)),
        ],
        compiler_params=pltpu.CompilerParams(
            collective_id=4, has_side_effects=True, vmem_limit_bytes=GRID_VMEM_BYTES
        ),
    )(projected, d_projected, w_out, p_out, curvature, cosine, sine)


def reduce_grid_kernel(n, slots, grid_qkv, grid_out, pick_ref, normed_t_in, d_proj_in,
                       mixed_t_ref, weighted_ref, out_ref, d_proj_ref, swap_sem,
                       normed_t_ref, load_sem, grads, begin, across, onward,
                       landed, core_send, core_recv, y_send, y_recv, z_send, z_recv):
    planes = n // 2
    z, y, x, c = spot()
    zeta = mirrored(z, c, planes)
    hub = lax.rem(zeta, 2) == 0
    spoke = lax.rem(zeta, 2) == 1
    late = lax.div(zeta, 2)
    y_peer = device(z, 1 - y, x, c)
    core_peer = device(z, y, x, 1 - c)
    row = [device(lax.rem(z + i, planes), y, x, c) for i in range(1, planes)]
    load = pltpu.make_async_copy(normed_t_in, normed_t_ref, load_sem.at[0])
    load.start()
    own_rows = d_proj_in.shape[0]
    d_proj_ref[:own_rows] = d_proj_in[...]
    greet(row + [core_peer, y_peer])
    swap = pltpu.make_async_remote_copy(
        src_ref=d_proj_in,
        dst_ref=d_proj_ref.at[pl.ds(own_rows, own_rows)],
        send_sem=swap_sem.at[0],
        recv_sem=swap_sem.at[1],
        device_id=core_peer,
        device_id_type=pl.DeviceIdType.MESH,
    )
    swap.start()
    cuts = cut_count(slots, 2)
    size = slots // cuts
    rows, cols = grid_qkv
    out_rows, out_cols = grid_out
    total = rows * cols + out_rows * out_cols
    edge = out_ref.shape[-1]
    legs = core_send.shape[0] - out_rows
    leg_rows = rows // 2 // legs
    group = 4
    giver = 1 - lax.rem(z, 2)

    def core_copy(i):
        if i < out_rows:
            count = out_cols // 2
            here = pl.ds(rows * cols + i * out_cols + giver * count, count)
        else:
            count = leg_rows * cols
            here = pl.ds((giver * legs + i - out_rows) * count, count)
        return pltpu.make_async_remote_copy(
            src_ref=grads.at[here],
            dst_ref=grads.at[here],
            send_sem=core_send.at[i],
            recv_sem=core_recv.at[i],
            device_id=core_peer,
            device_id_type=pl.DeviceIdType.MESH,
        )

    def out_columns(i, carry):
        width = group * edge
        right = weighted_ref[:, pl.ds(pl.multiple_of(i * width, width), width)]
        block = jnp.dot(
            mixed_t_ref[...], right, preferred_element_type=jnp.float32
        ).astype(jnp.bfloat16)
        for r in range(out_rows):
            for k in range(group):
                at = rows * cols + r * out_cols + c * (out_cols // 2) + i * group + k
                grads[at] = block[r * edge:(r + 1) * edge, k * edge:(k + 1) * edge]
        return carry

    def qkv_rows(i, carry):
        width = group * edge
        left = normed_t_ref[pl.ds(pl.multiple_of(i * width, width), width), :]
        block = jnp.dot(
            left, d_proj_ref[...], preferred_element_type=jnp.float32
        ).astype(jnp.bfloat16)
        for r in range(group):
            for k in range(cols):
                grads[(c * (rows // 2) + i * group + r) * cols + k] = block[
                    r * edge:(r + 1) * edge, k * edge:(k + 1) * edge
                ]
        return carry

    def hand_over(i):
        @pl.when(spoke)
        def _():
            core_copy(i).start()

    grads[total] = jnp.zeros((edge, edge), grads.dtype)
    lax.fori_loop(0, out_cols // 2 // group, out_columns, 0)
    for i in range(out_rows):
        hand_over(i)
    load.wait()
    swap.wait()
    for i in range(legs):
        steps = leg_rows // group
        lax.fori_loop(i * steps, (i + 1) * steps, qkv_rows, 0)
        hand_over(out_rows + i)

    def owner(i, at_y):
        first = (3, 2, 1, 0)[i]
        second = (0, 1, 3, 2)[i]
        o = (1 - late) * first + late * second
        return 2 * mirrored(o, c, planes) + at_y

    def block_sum(index):
        return grads[index].astype(jnp.float32)

    def y_copy(i, j):
        here = pl.ds(i * slots + j * size, size)
        return pltpu.make_async_remote_copy(
            src_ref=begin.at[here],
            dst_ref=across.at[here],
            send_sem=y_send.at[i, j],
            recv_sem=y_recv.at[i, j],
            device_id=y_peer,
            device_id_type=pl.DeviceIdType.MESH,
        )

    def z_copy(i, j):
        goal = (1 - late) * (2, 2, 1)[i] + late * (0, 1, 3)[i]
        buffer = (0, 1, 0)[i]
        return pltpu.make_async_remote_copy(
            src_ref=onward.at[i, pl.ds(j * size, size)],
            dst_ref=landed.at[buffer, pl.ds(j * size, size)],
            send_sem=z_send.at[i, j],
            recv_sem=z_recv.at[buffer, j],
            device_id=device(mirrored(goal, c, planes), y, x, c),
            device_id_type=pl.DeviceIdType.MESH,
        )

    def z_wait(buffer, j):
        here = landed.at[buffer, pl.ds(j * size, size)]
        pltpu.make_async_remote_copy(
            src_ref=here,
            dst_ref=here,
            send_sem=z_send.at[0, j],
            recv_sem=z_recv.at[buffer, j],
            device_id=core_peer,
            device_id_type=pl.DeviceIdType.MESH,
        ).wait_recv()

    def each(j, body):
        def some(t, carry):
            body(j * size + t)
            return carry

        lax.fori_loop(0, size, some, 0)

    @pl.when(hub)
    def _():
        for i in range(out_rows + legs):
            core_copy(i).wait_recv()
        def start(i, j):
            base = owner(i, 1 - y) * slots

            def fill(t):
                begin[i * slots + t] = grads[pick_ref[base + t]]

            each(j, fill)
            y_copy(i, j).start()

        def go(i, j):
            base = owner(i, y) * slots

            def value(t):
                return block_sum(pick_ref[base + t]) + across[i * slots + t].astype(jnp.float32)

            def pass_on(t):
                onward[i, t] = value(t).astype(jnp.bfloat16)

            def join_on(t):
                onward[i, t] = (value(t) + landed[0, t].astype(jnp.float32)).astype(jnp.bfloat16)

            def last(t):
                out_ref[t] = (value(t) + landed[late, t].astype(jnp.float32)).astype(jnp.bfloat16)

            y_copy(i, j).wait_recv()
            if i < 2:
                each(j, pass_on)
                z_copy(i, j).start()
            elif i == 2:

                @pl.when(late == 0)
                def _():
                    each(j, pass_on)

                @pl.when(late == 1)
                def _():
                    z_wait(0, j)
                    each(j, join_on)

                z_copy(i, j).start()
            else:
                z_wait(late, j)
                each(j, last)

        for i in range(planes + 1):

            def turn_round(j, carry, i=i):
                if i < planes:
                    start(i, j)
                if i > 0:
                    go(i - 1, j)
                return carry

            lax.fori_loop(0, cuts, turn_round, 0)

        def close(j, carry):
            for i in range(planes):
                y_copy(i, j).wait_send()
            for i in range(3):
                z_copy(i, j).wait_send()
            return carry

        lax.fori_loop(0, cuts, close, 0)

    @pl.when(spoke)
    def _():
        @pl.when(zeta == 1)
        def _():
            def go(j, carry):
                z_wait(0, j)
                z_wait(1, j)

                def last(t):
                    out_ref[t] = (
                        landed[0, t].astype(jnp.float32) + landed[1, t].astype(jnp.float32)
                    ).astype(jnp.bfloat16)

                each(j, last)
                return carry

            lax.fori_loop(0, cuts, go, 0)

        @pl.when(zeta == 3)
        def _():
            def go(j, carry):
                z_wait(0, j)

                def last(t):
                    out_ref[t] = landed[0, t]

                each(j, last)
                return carry

            lax.fori_loop(0, cuts, go, 0)

        for i in range(out_rows + legs):
            core_copy(i).wait_send()


def reduce_grid(picked, normed_t, d_proj, mixed_t, weighted, n, grid_qkv, grid_out):
    slots = picked.shape[0] // n
    edge = BLK
    total_blocks = grid_qkv[0] * grid_qkv[1] + grid_out[0] * grid_out[1]
    cuts = cut_count(slots, 2)
    legs = 4
    vmem = pl.BlockSpec(memory_space=pltpu.VMEM)
    dma = pltpu.SemaphoreType.DMA
    return pl.pallas_call(
        functools.partial(reduce_grid_kernel, n, slots, grid_qkv, grid_out),
        out_shape=jax.ShapeDtypeStruct((slots, edge, edge), jnp.bfloat16),
        in_specs=[pl.BlockSpec(memory_space=pltpu.SMEM), pl.BlockSpec(memory_space=pl.ANY)]
        + [vmem] * 3,
        out_specs=vmem,
        scratch_shapes=[
            pltpu.VMEM((2 * d_proj.shape[0], d_proj.shape[1]), d_proj.dtype),
            dma((2,)),
            pltpu.VMEM(normed_t.shape, normed_t.dtype),
            dma((1,)),
            pltpu.VMEM((total_blocks + 1, edge, edge), jnp.bfloat16),
            pltpu.VMEM((n // 2 * slots, edge, edge), jnp.bfloat16),
            pltpu.VMEM((n // 2 * slots, edge, edge), jnp.bfloat16),
            pltpu.VMEM((3, slots, edge, edge), jnp.bfloat16),
            pltpu.VMEM((2, slots, edge, edge), jnp.bfloat16),
            dma((grid_out[0] + legs,)),
            dma((grid_out[0] + legs,)),
            dma((n // 2, cuts)),
            dma((n // 2, cuts)),
            dma((3, cuts)),
            dma((2, cuts)),
        ],
        compiler_params=pltpu.CompilerParams(
            collective_id=5, has_side_effects=True, vmem_limit_bytes=GRID_VMEM_BYTES
        ),
    )(picked, normed_t, d_proj, mixed_t, weighted)


def local_grid(tokens, norm_gain, curvature, weight_slots, probe_slots, block_counts):
    n_columns = lax.axis_size("seq")
    n_owners = lax.axis_size("fsdp")
    q_heads = HQ // n_columns
    kv_heads = HK // n_columns
    row_blocks = D // BLK
    qkv_cols = (q_heads + 2 * kv_heads) * HD // BLK
    out_rows = q_heads * HD // BLK
    grid_qkv, grid_out = (row_blocks, qkv_cols), (out_rows, row_blocks)
    total_blocks = row_blocks * qkv_cols + out_rows * row_blocks
    slots = weight_slots.shape[1]
    length = tokens.shape[1]
    z, _, _, c = spot()
    theirs = lax.ppermute(block_counts, "seq", [(i, i ^ 1) for i in range(n_columns)])
    counts = jnp.where(lax.rem(z, 2) == c, block_counts, theirs)[0]
    range_ends = jnp.cumsum(counts)
    starts = range_ends - counts
    owner_ids = jnp.arange(n_owners, dtype=jnp.int32)
    block_ids = jnp.arange(total_blocks, dtype=jnp.int32)
    owners = jnp.sum((range_ends[None, :] <= block_ids[:, None]).astype(jnp.int32), axis=1)
    first_block = jnp.sum(
        jnp.where(owners[:, None] == owner_ids[None, :], starts[None, :], 0), axis=1
    )
    slot_of = (owners * slots + block_ids - first_block).astype(jnp.int32)
    projected, d_projected, w_out, p_out, normed_t, curv_part = gather_grid(
        slot_of,
        weight_slots[0],
        probe_slots[0],
        tokens[0],
        norm_gain[None, :],
        curvature[0],
        n_owners,
        grid_qkv,
        grid_out,
    )
    cosine, sine = turn_tables(length, HD)
    weighted, back_projected, mixed_t = square_exchange(
        projected, d_projected, w_out, p_out, curv_part, cosine, sine, q_heads
    )
    slot_index = jnp.arange(n_owners * slots, dtype=jnp.int32)
    place = slot_index % slots
    owner_hot = (slot_index // slots)[:, None] == owner_ids[None, :]
    owner_first = jnp.sum(jnp.where(owner_hot, starts[None, :], 0), axis=1)
    own_count = jnp.sum(jnp.where(owner_hot, counts[None, :], 0), axis=1)
    picked = jnp.where(place < own_count, owner_first + place, total_blocks).astype(jnp.int32)
    summed = reduce_grid(
        picked,
        normed_t,
        back_projected,
        mixed_t,
        weighted,
        n_owners,
        grid_qkv,
        grid_out,
    )
    scale = (length * n_owners) ** -0.5
    return summed.astype(jnp.float32).reshape(1, slots, BLK, BLK) * scale


def solution(mesh):
    in_specs = (
        P("fsdp", None, None),
        P(),
        P("fsdp", None, None),
        P("seq", "fsdp", None, None),
        P("seq", "fsdp", None, None),
        P("seq", None),
    )
    out_specs = P("seq", "fsdp", None, None)
    body = local_grid if mesh.shape["fsdp"] == 8 and mesh.shape["seq"] == 4 else local
    return jax.shard_map(body, mesh=mesh, in_specs=in_specs, out_specs=out_specs, check_vma=False)
```
